32 devices in a mesh: fsdp: 8 (over z, y), tensor: 4 (over x, core).
Axes of the slice: x: 2, y: 2, z: 4, core: 2. Of those that a mesh axis runs over, the one named last changes fastest.
Arguments:
- hidden_in: bfloat16 [8192, 2048], P(('fsdp', 'tensor')), may hold values from -6 to 6
- lengths: int32 [8], P('fsdp'), may hold values from 256 to 1024, as said below
- attn_gain: float32 [2048], replicated, may hold values from 0.5 to 2
- query_weight: bfloat16 [2048, 2048], P('fsdp', 'tensor'), may hold values from -0.125 to 0.125
- key_weight: bfloat16 [2048, 1024], P('fsdp', 'tensor'), may hold values from -0.125 to 0.125
- value_weight: bfloat16 [2048, 1024], P('fsdp', 'tensor'), may hold values from -0.125 to 0.125
- output_gate: bfloat16 [2048, 2048], P('fsdp', 'tensor'), may hold values from -0.125 to 0.125
- query_gain: float32 [128], replicated, may hold values from 0.5 to 2
- key_gain: float32 [128], replicated, may hold values from 0.5 to 2
- out_weight: bfloat16 [2048, 2048], P('tensor', 'fsdp'), may hold values from -3 to 3
- mlp_gain: float32 [2048], replicated, may hold values from 0.5 to 2
- gate_weight: bfloat16 [2048, 6144], P('fsdp', 'tensor'), may hold values from -0.125 to 0.125
- up_weight: bfloat16 [2048, 6144], P('fsdp', 'tensor'), may hold values from -0.125 to 0.125
- down_weight: bfloat16 [6144, 2048], P('tensor', 'fsdp'), may hold values from -0.15625 to 0.15625
- cotangent: bfloat16 [8192, 2048], P(('fsdp', 'tensor')), may hold values from -6 to 6
Outputs:
- output: bfloat16 [8192, 2048], P(('fsdp', 'tensor'))
- grad_hidden: float32 [8192, 2048], P(('fsdp', 'tensor'))
- grad_attn_gain: float32 [2048], replicated
- grad_query_weight: float32 [2048, 2048], P('fsdp', 'tensor')
- grad_key_weight: float32 [2048, 1024], P('fsdp', 'tensor')
- grad_value_weight: float32 [2048, 1024], P('fsdp', 'tensor')
- grad_output_gate: float32 [2048, 2048], P('fsdp', 'tensor')
- grad_query_gain: float32 [128], replicated
- grad_key_gain: float32 [128], replicated
- grad_out_weight: float32 [2048, 2048], P('tensor', 'fsdp')
- grad_mlp_gain: float32 [2048], replicated
- grad_gate_weight: float32 [2048, 6144], P('fsdp', 'tensor')
- grad_up_weight: float32 [2048, 6144], P('fsdp', 'tensor')
- grad_down_weight: float32 [6144, 2048], P('tensor', 'fsdp')
The draws below stay inside these ranges and needn't reach their ends.
Inputs may be any that keep to these rules, and one draw needn't show every extreme that they name: The first lengths[s] slots of sequence s hold real tokens, the rest padding; some sequence has all 1024 and some 1024 // 4.
All inputs are finite; a program needn't handle non-finite values.
Results may differ from the reference program's by a relative error of at most 0.019.
Values may be sent and summed in bfloat16 or wider, within the bound.
A program may use at most 192 MiB of HBM per device.

```python
import math
import jax
import jax.numpy as jnp
from jax import lax

D = 2048
HQ = 16
HK = 8
HD = 128
FF = 6144
SEQ_LEN = 1024
SEQS = 8
TOKENS = 8192


def draw_lengths(key, part):
    key_lens = jax.random.fold_in(key, 11)
    key_top = jax.random.fold_in(key, 12)
    key_low = jax.random.fold_in(key, 13)
    drawn = jax.random.randint(key_lens, (SEQS,), SEQ_LEN // 4, SEQ_LEN + 1)
    longest_at = jax.random.randint(key_top, (), 0, SEQS)
    shortest_at = (longest_at + 1 + jax.random.randint(key_low, (), 0, SEQS - 1)) % SEQS
    position = jnp.arange(SEQS)
    drawn = jnp.where(position == longest_at, SEQ_LEN, drawn)
    drawn = jnp.where(position == shortest_at, SEQ_LEN // 4, drawn)
    return drawn.astype(jnp.int32)


def block_levels(key, extent, shards, least, high):
    def one(dim, parts):
        steps = jax.random.uniform(jax.random.fold_in(jax.random.fold_in(key, 6), dim), (parts,), jnp.float32, least / len(shards), high / len(shards))
        return jnp.repeat(jnp.exp(steps), extent[dim] // parts).reshape((-1,) + (1,) * (len(extent) - dim - 1))

    level = one(*shards[0])
    for cut in shards[1:]:
        level = level * one(*cut)
    return level


def bell_draw(rng, shape, spread, reach, split=(), kind=jnp.bfloat16):
    values = spread * jax.random.normal(rng, shape, jnp.float32)
    if split:
        values = values * block_levels(rng, shape, split, -0.22, 0.18)
    return jnp.clip(values, -reach, reach).astype(kind)


def setup_inputs(seed: int = 0) -> dict:
    key_list = jax.random.split(jax.random.key(seed), 16)
    hidden_in = bell_draw(key_list[0], (TOKENS, D), 1.0, 6.0, ((0, 32),))
    lengths = draw_lengths(jax.random.fold_in(key_list[15], 71), 0)
    attn_gain = jnp.clip(jnp.exp(jax.random.uniform(key_list[2], (D,), jnp.float32, math.log(0.5), math.log(2.0))), 0.5, 2.0)
    query_weight = bell_draw(key_list[3], (D, HQ * HD), D ** -0.5, 0.125, ((0, 8), (1, 4)))
    key_weight = bell_draw(key_list[4], (D, HK * HD), D ** -0.5, 0.125, ((0, 8), (1, 4)))
    value_weight = bell_draw(key_list[5], (D, HK * HD), D ** -0.5, 0.125, ((0, 8), (1, 4)))
    output_gate = bell_draw(key_list[6], (D, HQ * HD), D ** -0.5, 0.125, ((0, 8), (1, 4)))
    query_gain = jnp.clip(jnp.exp(jax.random.uniform(key_list[7], (HD,), jnp.float32, math.log(0.5), math.log(2.0))), 0.5, 2.0)
    key_gain = jnp.clip(jnp.exp(jax.random.uniform(key_list[8], (HD,), jnp.float32, math.log(0.5), math.log(2.0))), 0.5, 2.0)
    out_weight = bell_draw(key_list[9], (HQ * HD, D), (max(HD // 32, 1)) ** -0.5, 3.0, ((0, 4), (1, 8)))
    mlp_gain = jnp.clip(jnp.exp(jax.random.uniform(key_list[10], (D,), jnp.float32, math.log(0.5), math.log(2.0))), 0.5, 2.0)
    gate_weight = bell_draw(key_list[11], (D, FF), D ** -0.5, 0.125, ((0, 8), (1, 4)))
    up_weight = bell_draw(key_list[12], (D, FF), D ** -0.5, 0.125, ((0, 8), (1, 4)))
    down_weight = bell_draw(key_list[13], (FF, D), (FF // 4) ** -0.5, 0.15625, ((0, 4), (1, 8)))
    cotangent = bell_draw(key_list[14], (TOKENS, D), 1.0, 6.0, ((0, 32),))
    return dict(hidden_in=hidden_in, lengths=lengths, attn_gain=attn_gain, query_weight=query_weight, key_weight=key_weight, value_weight=value_weight, output_gate=output_gate, query_gain=query_gain, key_gain=key_gain, out_weight=out_weight, mlp_gain=mlp_gain, gate_weight=gate_weight, up_weight=up_weight, down_weight=down_weight, cotangent=cotangent)


NORM_EPSILON = 1e-06
ROPE_THETA = 1000000.0
MASKED_LOGIT = -1e+30

@jax.custom_vjp
def low(v):
    return lax.optimization_barrier(v.astype(jnp.bfloat16)).astype(jnp.float32)

@jax.custom_vjp
def low_back(v):
    return v

def low_keep(v):
    return (low(v), None)

def low_pass(kept, grad):
    return (grad,)

def back_keep(v):
    return (v, None)

def back_low(kept, grad):
    return (low(grad),)
low.defvjp(low_keep, low_pass)
low_back.defvjp(back_keep, back_low)

def matmul(first_op, second_op):
    return jnp.dot(first_op, second_op, precision=lax.Precision.HIGHEST, preferred_element_type=jnp.float32)

def rms_scale(values, gain_vec):
    return values * lax.rsqrt(lax.optimization_barrier(jnp.mean(values * values, axis=-1, keepdims=True)) + NORM_EPSILON) * gain_vec

def rotate_half(values):
    half_width = values.shape[-1] // 2
    return jnp.concatenate([-values[..., half_width:], values[..., :half_width]], axis=-1)

def rope_tables(slot_count, head_size):
    half_width = head_size // 2
    inverse = ROPE_THETA ** (-(jnp.arange(half_width, dtype=jnp.float32) * 2.0 / head_size))
    angles = jnp.arange(slot_count, dtype=jnp.float32)[:, None] * inverse[None, :]
    cosine = jnp.concatenate([jnp.cos(angles), jnp.cos(angles)], axis=-1)
    sine_table = jnp.concatenate([jnp.sin(angles), jnp.sin(angles)], axis=-1)
    return (cosine[:, None, :], sine_table[:, None, :])

def rope_apply(values, cosine, sine_table):
    return values * cosine + rotate_half(values) * sine_table

def attend_sequence(inputs):
    queries, keys_in, values_in, length = inputs
    grouped = queries.reshape(SEQ_LEN, HK, HQ // HK, HD)
    scores = low_back(jnp.einsum('qkgd,skd->kgqs', grouped, keys_in, precision=lax.Precision.HIGHEST))
    row_index = jnp.arange(SEQ_LEN)[:, None]
    col_index = jnp.arange(SEQ_LEN)[None, :]
    allowed = (col_index <= row_index) & (col_index < length)
    logits = jnp.where(allowed, scores * HD ** (-0.5), MASKED_LOGIT)
    highest = lax.optimization_barrier(jnp.max(logits, axis=-1, keepdims=True))
    weights_raw = jnp.exp(logits - highest)
    probs = low(weights_raw / lax.optimization_barrier(jnp.sum(weights_raw, axis=-1, keepdims=True)))
    attended = low_back(jnp.einsum('kgqs,skd->qkgd', probs, values_in, precision=lax.Precision.HIGHEST))
    return attended.reshape(SEQ_LEN, HQ * HD)

def layer(hidden, attn_gain, query_weight, key_weight, value_weight, output_gate, query_gain, key_gain, out_weight, mlp_gain, gate_weight, up_weight, down_weight, lengths):
    cosine, sine_table = rope_tables(SEQ_LEN, HD)
    position = jnp.arange(SEQ_LEN)
    valid_rows = (position[None, :] < lengths[:, None]).astype(jnp.float32).reshape(SEQS * SEQ_LEN, 1)
    normed_one = low(rms_scale(hidden, attn_gain))
    query_raw = low_back(matmul(normed_one, query_weight)).reshape(SEQS, SEQ_LEN, HQ, HD)
    key_raw = low_back(matmul(normed_one, key_weight)).reshape(SEQS, SEQ_LEN, HK, HD)
    value_in = low(low_back(matmul(normed_one, value_weight))).reshape(SEQS, SEQ_LEN, HK, HD)
    gate_pre = low_back(matmul(normed_one, output_gate))
    query_rot = low(rope_apply(rms_scale(query_raw, query_gain), cosine, sine_table))
    key_rot = low(rope_apply(rms_scale(key_raw, key_gain), cosine, sine_table))
    attended = lax.map(jax.checkpoint(attend_sequence), (query_rot, key_rot, value_in, lengths))
    attended = attended.reshape(SEQS * SEQ_LEN, HQ * HD)
    gated_out = low(attended * jax.nn.sigmoid(gate_pre))
    middle = hidden + low_back(matmul(gated_out, out_weight))
    normed_two = low(rms_scale(middle, mlp_gain))
    ffn_gate = low_back(matmul(normed_two, gate_weight))
    ffn_up = low_back(matmul(normed_two, up_weight))
    ffn_mid = low(ffn_gate * jax.nn.sigmoid(ffn_gate) * ffn_up)
    return (middle + low_back(matmul(ffn_mid, down_weight))) * valid_rows

def reference(hidden_in, lengths, attn_gain, query_weight, key_weight, value_weight, output_gate, query_gain, key_gain, out_weight, mlp_gain, gate_weight, up_weight, down_weight, cotangent):
    floats = tuple((array_in.astype(jnp.float32) for array_in in (hidden_in, attn_gain, query_weight, key_weight, value_weight, output_gate, query_gain, key_gain, out_weight, mlp_gain, gate_weight, up_weight, down_weight)))

    def forward(*params):
        return layer(*params, lengths)
    result, pullback = jax.vjp(forward, *floats)
    grads = pullback(cotangent.astype(jnp.float32))
    return (result.astype(jnp.bfloat16), grads[0], grads[1], grads[2], grads[3], grads[4], grads[5], grads[6], grads[7], grads[8], grads[9], grads[10], grads[11], grads[12])
```

```python
import jax
import jax.numpy as jnp
from jax import lax
from jax.sharding import PartitionSpec as P

NORM_EPSILON = 1e-06
ROPE_THETA = 1000000.0
SCORE_BLOCK = 512
MASKED_LOGIT = -1e30
F32 = jnp.float32
BF16 = jnp.bfloat16


def exchange(values, axis, size, mask):
    return lax.ppermute(values, axis, [(i, i ^ mask) for i in range(size)])


def position_mask(position, count):
    half = count // 2
    return (position // half) | ((position % half) << 1)


def gather_blocks(shard, count, axis):
    half = count // 2
    near = [shard]
    far = [exchange(shard, "fsdp", count, 1)]
    for step in range(1, half):
        near.append(exchange(shard, "fsdp", count, step << 1))
    for step in range(1, half):
        far.append(exchange(near[step], "fsdp", count, 1))
    return jnp.concatenate(near + far, axis=axis)


def scatter_blocks(near, far, count, axis):
    half = count // 2
    arrived = exchange(far.astype(BF16), "fsdp", count, 1)
    width = near.shape[axis] // half
    total = near.astype(F32) + arrived.astype(F32)
    pieces = [lax.slice_in_dim(total, i * width, (i + 1) * width, axis=axis) for i in range(half)]
    result = pieces[0]
    moved = [
        exchange(pieces[step].astype(BF16), "fsdp", count, step << 1) for step in range(1, half)
    ]
    for piece in moved:
        result = result + piece.astype(F32)
    return result


def to_relative(values, me, count):
    width = values.shape[-1] // count
    parts = [
        lax.dynamic_slice_in_dim(
            values, (me ^ position_mask(p, count)) * width, width, axis=values.ndim - 1
        )
        for p in range(count)
    ]
    return jnp.concatenate(parts, axis=-1)


def to_absolute(values, me, count):
    width = values.shape[-1] // count
    half = count // 2
    parts = []
    for block in range(count):
        mask = me ^ block
        place = (mask & 1) * half + (mask >> 1)
        parts.append(lax.dynamic_slice_in_dim(values, place * width, width, axis=values.ndim - 1))
    return jnp.concatenate(parts, axis=-1)


def row_masks(count):
    half = count // 2
    return [((p % half) << 1) | (p // half) for p in range(count)]


def rows_in(values, count):
    half = count // 2
    near = [values] + [exchange(values, "tensor", count, step << 1) for step in range(1, half)]
    far = [exchange(piece, "tensor", count, 1) for piece in near]
    return jnp.concatenate(near + far, axis=0)


def rows_out(partial, count):
    half = count // 2
    rows = partial.shape[0] // count
    blocks = [partial[p * rows : (p + 1) * rows] for p in range(count)]
    sums = [None] * half
    for step in list(range(1, half)) + [0]:
        arrived = exchange(blocks[half + step].astype(BF16), "tensor", count, 1)
        sums[step] = blocks[step].astype(F32) + arrived.astype(F32)
    result = sums[0]
    for step in range(1, half):
        result = result + exchange(sums[step].astype(BF16), "tensor", count, step << 1).astype(F32)
    return result


def sum_everywhere(values, axes):
    for axis, count in axes:
        mask = 1
        while mask < count:
            values = values + exchange(values, axis, count, mask)
            mask <<= 1
    return values


def matmul(first_op, second_op):
    return jnp.dot(first_op, second_op, preferred_element_type=F32)


def matmul_tn(first_op, second_op):
    return lax.dot_general(
        first_op, second_op, (((0,), (0,)), ((), ())), preferred_element_type=F32
    )


def matmul_nt(first_op, second_op):
    return lax.dot_general(
        first_op, second_op, (((1,), (1,)), ((), ())), preferred_element_type=F32
    )


def normalize(values):
    inv_root = lax.rsqrt(jnp.mean(values * values, axis=-1, keepdims=True) + NORM_EPSILON)
    return (values * inv_root, inv_root)


def norm_back(gradient, unit_rows, inv_root, gain_vec):
    scaled = gradient * gain_vec
    return inv_root * (scaled - unit_rows * jnp.mean(scaled * unit_rows, axis=-1, keepdims=True))


def rotate_half(values):
    half_width = values.shape[-1] // 2
    return jnp.concatenate([-values[..., half_width:], values[..., :half_width]], axis=-1)


def rotate_back(values):
    half_width = values.shape[-1] // 2
    return jnp.concatenate([values[..., half_width:], -values[..., :half_width]], axis=-1)


def rope_tables(slots, head_size):
    half_width = head_size // 2
    inverse = ROPE_THETA ** (-(jnp.arange(half_width, dtype=F32) * 2.0 / head_size))
    angles = slots.astype(F32)[:, None] * inverse[None, :]
    cosine = jnp.concatenate([jnp.cos(angles), jnp.cos(angles)], axis=-1)
    sine_table = jnp.concatenate([jnp.sin(angles), jnp.sin(angles)], axis=-1)
    return (cosine[:, None, :], sine_table[:, None, :])


def head_forward(raw_heads, gain_vec, cosine, sine_table):
    unit_rows, inv_root = normalize(raw_heads)
    normed = unit_rows * gain_vec
    turned = normed * cosine + rotate_half(normed) * sine_table
    return (turned.astype(BF16), unit_rows, inv_root)


def head_backward(gradient, unit_rows, inv_root, gain_vec, cosine, sine_table):
    normed_grad = gradient * cosine + rotate_back(gradient * sine_table)
    gain_part = jnp.sum(normed_grad * unit_rows, axis=(0, 1))
    return (norm_back(normed_grad, unit_rows, inv_root, gain_vec), gain_part)


def block_mask(row_slots, col_slots, length):
    rows, cols = row_slots[:, None], col_slots[None, :]
    return (cols <= rows) & (cols < length)


def attend_forward(queries, keys_b, values_b, slots, length, score_scale):
    seq_len, kv_heads, head_size = keys_b.shape
    head_count = queries.shape[1]
    group_size = head_count // kv_heads
    block_rows = min(SCORE_BLOCK, seq_len)
    block_count = seq_len // block_rows
    grouped = queries.reshape(block_count, block_rows, kv_heads, group_size, head_size)

    def one_block(inputs):
        qblock, row_slots = inputs
        scores = jnp.einsum("qkgd,skd->kgqs", qblock, keys_b, preferred_element_type=F32)
        allowed = block_mask(row_slots, slots, length)
        logits = jnp.where(allowed, scores * score_scale, MASKED_LOGIT)
        highest = jnp.max(logits, axis=-1, keepdims=True)
        weights_raw = jnp.exp(logits - highest)
        row_total = jnp.sum(weights_raw, axis=-1, keepdims=True)
        probabilities = (weights_raw / row_total).astype(BF16)
        result = jnp.einsum("kgqs,skd->qkgd", probabilities, values_b, preferred_element_type=F32)
        return (result, highest + jnp.log(row_total))

    outputs, log_total = lax.map(one_block, (grouped, slots.reshape(block_count, block_rows)))
    return (outputs.reshape(seq_len, head_count * head_size), log_total)


def attend_backward(queries, keys_b, values_b, grad_out, log_total, slots, length, score_scale):
    seq_len, kv_heads, head_size = keys_b.shape
    head_count = queries.shape[1]
    group_size = head_count // kv_heads
    block_rows = min(SCORE_BLOCK, seq_len)
    block_count = seq_len // block_rows
    grouped = queries.reshape(block_count, block_rows, kv_heads, group_size, head_size)
    grad_grouped = grad_out.reshape(block_count, block_rows, kv_heads, group_size, head_size)

    def one_block(carried, inputs):
        key_grad, value_grad = carried
        qblock, gblock, block_lse, row_slots = inputs
        scores = jnp.einsum("qkgd,skd->kgqs", qblock, keys_b, preferred_element_type=F32)
        allowed = block_mask(row_slots, slots, length)
        logits = jnp.where(allowed, scores * score_scale, MASKED_LOGIT)
        soft = jnp.where(allowed, jnp.exp(logits - block_lse), 0.0)
        probs_low = soft.astype(BF16)
        prob_grad = jnp.einsum("qkgd,skd->kgqs", gblock, values_b, preferred_element_type=F32)
        centre = jnp.sum(soft * prob_grad, axis=-1, keepdims=True)
        score_grad = (score_scale * soft * (prob_grad - centre)).astype(BF16)
        query_grad = jnp.einsum("kgqs,skd->qkgd", score_grad, keys_b, preferred_element_type=F32)
        key_grad = key_grad + jnp.einsum(
            "kgqs,qkgd->skd", score_grad, qblock, preferred_element_type=F32
        )
        value_grad = value_grad + jnp.einsum(
            "kgqs,qkgd->skd", probs_low, gblock, preferred_element_type=F32
        )
        return ((key_grad, value_grad), query_grad)

    zero_grad = jnp.zeros((seq_len, kv_heads, head_size), F32)
    (key_grad, value_grad), query_grads = lax.scan(
        one_block,
        (zero_grad, zero_grad),
        (grouped, grad_grouped, log_total, slots.reshape(block_count, block_rows)),
    )
    return (query_grads.reshape(seq_len, head_count, head_size), key_grad, value_grad)


def body(
    members,
    shares,
    hidden_in,
    lengths,
    attn_gain,
    query_weight,
    key_weight,
    value_weight,
    output_gate,
    query_gain,
    key_gain,
    out_weight,
    mlp_gain,
    gate_weight,
    up_weight,
    down_weight,
    cotangent,
):
    me = lax.axis_index("fsdp")
    share = lax.axis_index("tensor")
    local_rows = hidden_in.shape[0]
    length = lengths[0]
    head_size = query_gain.shape[0]
    key_width = key_weight.shape[1]
    query_width = query_weight.shape[1]
    kv_heads = key_width // head_size
    head_count = query_width // head_size
    score_scale = head_size ** (-0.5)
    steps = jnp.arange(local_rows)
    slots = jnp.concatenate([(share ^ mask) * local_rows + steps for mask in row_masks(shares)])
    valid_rows = (slots[:local_rows] < length).astype(F32)[:, None]
    seq_len = slots.shape[0]

    def relative(values):
        return to_relative(values, me, members)

    def absolute(values):
        return to_absolute(values, me, members)

    attn_gain, mlp_gain = relative(attn_gain), relative(mlp_gain)

    qkv_full = gather_blocks(
        jnp.concatenate([query_weight, key_weight, value_weight], axis=1), members, 0
    )
    gate_full = gather_blocks(output_gate, members, 0)
    out_full = gather_blocks(out_weight, members, 1)

    residual = relative(hidden_in).astype(F32)
    unit_one, root_one = normalize(residual)
    normed_one = rows_in((unit_one * attn_gain).astype(BF16), shares)
    cosine, sine_table = rope_tables(slots, head_size)
    qkv_raw = matmul(normed_one, qkv_full)
    query_raw = qkv_raw[:, :query_width].reshape(seq_len, head_count, head_size)
    key_raw = qkv_raw[:, query_width : query_width + key_width].reshape(
        seq_len, kv_heads, head_size
    )
    value_b = qkv_raw[:, query_width + key_width :].astype(BF16)
    value_b = value_b.reshape(seq_len, kv_heads, head_size)
    gate_pre = matmul(normed_one, gate_full)
    query_b, query_unit, query_root = head_forward(query_raw, query_gain, cosine, sine_table)
    key_b, key_unit, key_root = head_forward(key_raw, key_gain, cosine, sine_table)
    attended, log_total = attend_forward(query_b, key_b, value_b, slots, length, score_scale)
    gate_sig = jax.nn.sigmoid(gate_pre)
    gated_out = (attended * gate_sig).astype(BF16)
    middle = residual + rows_out(matmul(gated_out, out_full), shares)
    unit_two, root_two = normalize(middle)
    normed_two = rows_in((unit_two * mlp_gain).astype(BF16), shares)

    gate_weights = gather_blocks(gate_weight, members, 0)
    up_weights = gather_blocks(up_weight, members, 0)
    down_weights = gather_blocks(down_weight, members, 1)
    grad_rows = relative(cotangent).astype(F32) * valid_rows
    branch_full = rows_in(grad_rows.astype(BF16), shares)

    ffn_gate = matmul(normed_two, gate_weights)
    ffn_up = matmul(normed_two, up_weights)
    ffn_sig = jax.nn.sigmoid(ffn_gate)
    ffn_act = ffn_gate * ffn_sig
    ffn_mid = (ffn_act * ffn_up).astype(BF16)

    def scatter_rows(acts, grads):
        half = acts.shape[1] // 2
        far = matmul_tn(acts[:, half:], grads).astype(BF16)
        near = matmul_tn(acts[:, :half], grads)
        return scatter_blocks(near, far, members, 0)

    def scatter_cols(acts, grads):
        half = grads.shape[1] // 2
        far = matmul_tn(acts, grads[:, half:]).astype(BF16)
        near = matmul_tn(acts, grads[:, :half])
        return scatter_blocks(near, far, members, 1)

    down_shard = scatter_cols(ffn_mid, branch_full)
    mid_grad = matmul_nt(branch_full, down_weights)
    gate_grad = (mid_grad * ffn_up * ffn_sig * (1.0 + ffn_gate * (1.0 - ffn_sig))).astype(BF16)
    up_grad = (mid_grad * ffn_act).astype(BF16)
    norm_two_grad = rows_out(
        matmul_nt(gate_grad, gate_weights) + matmul_nt(up_grad, up_weights), shares
    )
    gate_shard = scatter_rows(normed_two, gate_grad)
    up_shard = scatter_rows(normed_two, up_grad)
    ffn_branch = rows_out(matmul(ffn_mid, down_weights), shares)
    output = absolute(((middle + ffn_branch) * valid_rows).astype(BF16))

    mlp_gain_part = jnp.sum(norm_two_grad * unit_two, axis=0)
    middle_grad = grad_rows + norm_back(norm_two_grad, unit_two, root_two, mlp_gain)
    attn_full_grad = rows_in(middle_grad.astype(BF16), shares)
    gated_grad = matmul_nt(attn_full_grad, out_full)
    out_shard = scatter_cols(gated_out, attn_full_grad)
    attended_grad = (gated_grad * gate_sig).astype(BF16)
    gate_pre_grad = (gated_grad * attended * gate_sig * (1.0 - gate_sig)).astype(BF16)
    gate_attn_shard = scatter_rows(normed_one, gate_pre_grad)
    query_grad, key_grad, value_grad = attend_backward(
        query_b,
        key_b,
        value_b,
        attended_grad.reshape(seq_len, head_count, head_size),
        log_total,
        slots,
        length,
        score_scale,
    )
    query_back, query_gain_part = head_backward(
        query_grad, query_unit, query_root, query_gain, cosine, sine_table
    )
    key_back, key_gain_part = head_backward(
        key_grad, key_unit, key_root, key_gain, cosine, sine_table
    )
    qkv_send = jnp.concatenate(
        [
            query_back.reshape(seq_len, query_width).astype(BF16),
            key_back.reshape(seq_len, key_width).astype(BF16),
            value_grad.reshape(seq_len, key_width).astype(BF16),
        ],
        axis=1,
    )
    qkv_shard = scatter_rows(normed_one, qkv_send)
    norm_one_grad = rows_out(
        matmul_nt(qkv_send, qkv_full) + matmul_nt(gate_pre_grad, gate_full), shares
    )
    attn_gain_part = jnp.sum(norm_one_grad * unit_one, axis=0)
    grad_hidden = absolute(
        middle_grad + norm_back(norm_one_grad, unit_one, root_one, attn_gain)
    )
    width = hidden_in.shape[1]
    gain_totals = sum_everywhere(
        jnp.concatenate(
            [absolute(attn_gain_part), absolute(mlp_gain_part), query_gain_part, key_gain_part]
        ),
        (("tensor", shares), ("fsdp", members)),
    )
    return (
        output,
        grad_hidden,
        gain_totals[:width],
        qkv_shard[:, :query_width],
        qkv_shard[:, query_width : query_width + key_width],
        qkv_shard[:, query_width + key_width :],
        gate_attn_shard,
        gain_totals[2 * width : 2 * width + head_size],
        gain_totals[2 * width + head_size :],
        out_shard,
        gain_totals[width : 2 * width],
        gate_shard,
        up_shard,
        down_shard,
    )


def solution(mesh):
    members, shares = mesh.shape["fsdp"], mesh.shape["tensor"]

    def layer(*operands):
        return body(members, shares, *operands)

    tokens = P(("fsdp", "tensor"), None)
    return jax.shard_map(
        layer,
        mesh=mesh,
        in_specs=(
            tokens,
            P("fsdp"),
            P(),
            P("fsdp", "tensor"),
            P("fsdp", "tensor"),
            P("fsdp", "tensor"),
            P("fsdp", "tensor"),
            P(),
            P(),
            P("tensor", "fsdp"),
            P(),
            P("fsdp", "tensor"),
            P("fsdp", "tensor"),
            P("tensor", "fsdp"),
            tokens,
        ),
        out_specs=(
            tokens,
            tokens,
            P(),
            P("fsdp", "tensor"),
            P("fsdp", "tensor"),
            P("fsdp", "tensor"),
            P("fsdp", "tensor"),
            P(),
            P(),
            P("tensor", "fsdp"),
            P(),
            P("fsdp", "tensor"),
            P("fsdp", "tensor"),
            P("tensor", "fsdp"),
        ),
        check_vma=False,
    )
```

```python
import functools

import jax
import jax.numpy as jnp
from jax import lax
from jax.experimental import pallas as pl
from jax.experimental.pallas import tpu as pltpu
from jax.sharding import PartitionSpec as P

NORM_EPSILON = 1e-06
ROPE_THETA = 1000000.0
MASKED_LOGIT = -1e30
F32 = jnp.float32
BF16 = jnp.bfloat16


def exchange(values, axis, size, mask):
    return lax.ppermute(values, axis, [(i, i ^ mask) for i in range(size)])


def lines(count):
    return [list(range(0, count, 2)), list(range(1, count, 2))]


def gather_line(shard, count):
    return lax.all_gather(shard, "fsdp", axis=0, tiled=True, axis_index_groups=lines(count))


def gather_pair(near, count, *before):
    far = exchange(near, "fsdp", count, 1)
    if before:
        far = hold(far, *before)
    return jnp.concatenate([near, far], axis=0)


def scatter_line(total, count):
    return lax.psum_scatter(
        total, "fsdp", scatter_dimension=0, tiled=True, axis_index_groups=lines(count)
    )


def add_low(first, second):
    return (first.astype(F32) + second.astype(F32)).astype(BF16)


def hold(value, *others):
    return lax.optimization_barrier((value,) + others)[0]


def to_pairs(values, me, count):
    blocks = values.reshape(values.shape[:-1] + (count // 2, 2, values.shape[-1] // count))
    even = blocks[..., 0, :].reshape(values.shape[:-1] + (-1,))
    odd = blocks[..., 1, :].reshape(values.shape[:-1] + (-1,))
    first = me % 2 == 0
    return jnp.concatenate([jnp.where(first, even, odd), jnp.where(first, odd, even)], axis=-1)


def to_index_order(values, me, count):
    width = values.shape[-1]
    shape = values.shape[:-1] + (count // 2, 1, width // count)
    near = values[..., : width // 2].reshape(shape)
    far = values[..., width // 2 :].reshape(shape)
    first = me % 2 == 0
    even, odd = jnp.where(first, near, far), jnp.where(first, far, near)
    return jnp.concatenate([even, odd], axis=-2).reshape(values.shape)


def row_masks(count):
    half = count // 2
    return [((p % half) << 1) | (p // half) for p in range(count)]


def place_of(mask, count):
    return (mask & 1) * (count // 2) + (mask >> 1)


def rows_in(values, count, *before):
    half = count // 2
    moved = [exchange(values, "tensor", count, step << 1) for step in range(1, half)]
    if before:
        moved = [hold(piece, *before) for piece in moved]
    near = [values] + moved
    far = [exchange(piece, "tensor", count, 1) for piece in near]
    return jnp.concatenate(near + far, axis=0)


def rows_out(near, far, count, *before):
    half = count // 2
    rows = near.shape[0] // half
    arrived = exchange(far.astype(BF16), "tensor", count, 1)

    def block(step):
        piece = slice(step * rows, (step + 1) * rows)
        return near[piece].astype(F32) + arrived[piece].astype(F32)

    moved = [
        exchange(block(step).astype(BF16), "tensor", count, step << 1) for step in range(1, half)
    ]
    result = block(0)
    for piece in moved:
        result = result + (hold(piece, *before) if before else piece).astype(F32)
    return result


def sum_everywhere(values, axes):
    for axis, count in axes:
        mask = 1
        while mask < count:
            values = values + exchange(values, axis, count, mask)
            mask <<= 1
    return values


def matmul(first_op, second_op):
    return jnp.dot(first_op, second_op, preferred_element_type=F32)


def matmul_tn(first_op, second_op):
    return lax.dot_general(
        first_op, second_op, (((0,), (0,)), ((), ())), preferred_element_type=F32
    )


def matmul_nt(first_op, second_op):
    return lax.dot_general(
        first_op, second_op, (((1,), (1,)), ((), ())), preferred_element_type=F32
    )


def normalize(values):
    inv_root = lax.rsqrt(jnp.mean(values * values, axis=-1, keepdims=True) + NORM_EPSILON)
    return (values * inv_root, inv_root)


def norm_back(gradient, unit_rows, inv_root, gain_vec):
    scaled = gradient * gain_vec
    return inv_root * (scaled - unit_rows * jnp.mean(scaled * unit_rows, axis=-1, keepdims=True))


def rope_tables(slot_count, head_size):
    half_width = head_size // 2
    inverse = ROPE_THETA ** (-(jnp.arange(half_width, dtype=F32) * 2.0 / head_size))
    angles = jnp.arange(slot_count, dtype=F32)[:, None] * inverse[None, :]
    cosine = jnp.concatenate([jnp.cos(angles), jnp.cos(angles)], axis=-1)
    signed_sine = jnp.concatenate([-jnp.sin(angles), jnp.sin(angles)], axis=-1)
    return (cosine, signed_sine)


def allowed_block(block, rows, width, length):
    row_slot = block * rows + lax.broadcasted_iota(jnp.int32, (rows, width), 0)
    col_slot = lax.broadcasted_iota(jnp.int32, (rows, width), 1)
    return (col_slot <= row_slot) & (col_slot < length)


def turn(unit_rows, gain_vec, cosine, signed_sine):
    normed = unit_rows * gain_vec
    half = normed.shape[-1] // 2
    return normed * cosine + pltpu.roll(normed, half, 1) * signed_sine


def turn_back(gradient, cosine, signed_sine):
    half = gradient.shape[-1] // 2
    return gradient * cosine - pltpu.roll(gradient, half, 1) * signed_sine


def attend_forward_kernel(
    masks,
    head_size,
    score_scale,
    share_ref,
    length_ref,
    query_ref,
    key_ref,
    value_ref,
    query_gain_ref,
    key_gain_ref,
    cosine_ref,
    sine_ref,
    attended_ref,
    log_ref,
    query_rot_ref,
    key_rot_ref,
    value_low_ref,
):
    blocks = len(masks)
    rows = query_ref.shape[0] // blocks
    group = query_ref.shape[1] // head_size
    share, length = share_ref[0], length_ref[0]
    for place, mask in enumerate(masks):
        here = pl.ds(place * rows, rows)
        there = pl.ds(pl.multiple_of((share ^ mask) * rows, rows), rows)
        cosine, signed_sine = cosine_ref[there, :], sine_ref[there, :]
        for head in range(group):
            cols = pl.ds(head * head_size, head_size)
            unit_rows, _ = normalize(query_ref[here, cols])
            turned = turn(unit_rows, query_gain_ref[...], cosine, signed_sine)
            query_rot_ref[there, cols] = turned.astype(BF16)
        unit_rows, _ = normalize(key_ref[here, :])
        turned = turn(unit_rows, key_gain_ref[...], cosine, signed_sine)
        key_rot_ref[there, :] = turned.astype(BF16)
        value_low_ref[there, :] = value_ref[here, :].astype(BF16)

    for block in range(blocks):
        width = (block + 1) * rows
        here = pl.ds(block * rows, rows)
        allowed = allowed_block(block, rows, width, length)
        back = pl.ds(pl.multiple_of(place_of(share ^ block, blocks) * rows, rows), rows)

        def one_head(head, carry, width=width, here=here, allowed=allowed, back=back):
            cols = pl.ds(pl.multiple_of(head * head_size, head_size), head_size)
            scores = matmul_nt(query_rot_ref[here, cols], key_rot_ref[:width, :])
            logits = jnp.where(allowed, scores * score_scale, MASKED_LOGIT)
            highest = jnp.max(logits, axis=-1, keepdims=True)
            weights_raw = jnp.exp(logits - highest)
            row_total = jnp.sum(weights_raw, axis=-1, keepdims=True)
            probabilities = (weights_raw * (1.0 / row_total)).astype(BF16)
            attended_ref[back, cols] = matmul(probabilities, value_low_ref[:width, :])
            log_ref[here, cols] = jnp.broadcast_to(highest + jnp.log(row_total), (rows, head_size))
            return carry

        lax.fori_loop(0, group, one_head, 0)


def attend_backward_kernel(
    masks,
    head_size,
    score_scale,
    share_ref,
    length_ref,
    grad_ref,
    query_ref,
    key_ref,
    query_rot_ref,
    key_rot_ref,
    value_low_ref,
    log_ref,
    query_gain_ref,
    key_gain_ref,
    cosine_ref,
    sine_ref,
    send_ref,
    gain_ref,
    query_grad_ref,
    key_grad_ref,
    value_grad_ref,
):
    blocks = len(masks)
    rows = query_ref.shape[0] // blocks
    group = query_ref.shape[1] // head_size
    kv_heads = pl.num_programs(0)
    kv_head = pl.program_id(0)
    share, length = share_ref[0], length_ref[0]
    key_grad_ref[...] = jnp.zeros_like(key_grad_ref)
    value_grad_ref[...] = jnp.zeros_like(value_grad_ref)

    @pl.when(kv_head == 0)
    def _():
        gain_ref[...] = jnp.zeros_like(gain_ref)

    for block in range(blocks):
        width = (block + 1) * rows
        here = pl.ds(block * rows, rows)
        allowed = allowed_block(block, rows, width, length)
        back = pl.ds(pl.multiple_of(place_of(share ^ block, blocks) * rows, rows), rows)

        def one_head(head, carry, width=width, here=here, allowed=allowed, back=back):
            cols = pl.ds(pl.multiple_of(head * head_size, head_size), head_size)
            queries, grads = query_rot_ref[here, cols], grad_ref[back, cols]
            scores = matmul_nt(queries, key_rot_ref[:width, :])
            logits = jnp.where(allowed, scores * score_scale, MASKED_LOGIT)
            soft = jnp.where(allowed, jnp.exp(logits - log_ref[here, cols][:, :1]), 0.0)
            prob_grad = matmul_nt(grads, value_low_ref[:width, :])
            centre = jnp.sum(soft * prob_grad, axis=-1, keepdims=True)
            score_grad = (score_scale * soft * (prob_grad - centre)).astype(BF16)
            query_grad_ref[here, cols] = matmul(score_grad, key_rot_ref[:width, :])
            key_grad_ref[:width, :] += matmul_tn(score_grad, queries)
            value_grad_ref[:width, :] += matmul_tn(soft.astype(BF16), grads)
            return carry

        lax.fori_loop(0, group, one_head, 0)

    key_base, value_base = kv_heads * group * head_size, kv_heads * (group + 1) * head_size
    for place, mask in enumerate(masks):
        here = pl.ds(place * rows, rows)
        there = pl.ds(pl.multiple_of((share ^ mask) * rows, rows), rows)
        cosine, signed_sine = cosine_ref[there, :], sine_ref[there, :]

        def through_norm(gradient, raw, gain_vec):
            normed_grad = turn_back(gradient, cosine, signed_sine)
            unit_rows, inv_root = normalize(raw)
            gain_part = jnp.sum(normed_grad * unit_rows, axis=0, keepdims=True)
            return norm_back(normed_grad, unit_rows, inv_root, gain_vec).astype(BF16), gain_part

        for head in range(group):
            cols = pl.ds(head * head_size, head_size)
            sent, gain_part = through_norm(
                query_grad_ref[there, cols], query_ref[here, cols], query_gain_ref[...]
            )
            offset = pl.multiple_of((kv_head * group + head) * head_size, head_size)
            send_ref[here, pl.ds(offset, head_size)] = sent
            gain_ref[0:1, :] += gain_part
        sent, gain_part = through_norm(key_grad_ref[there, :], key_ref[here, :], key_gain_ref[...])
        offset = pl.multiple_of(key_base + kv_head * head_size, head_size)
        send_ref[here, pl.ds(offset, head_size)] = sent
        gain_ref[1:2, :] += gain_part
        offset = pl.multiple_of(value_base + kv_head * head_size, head_size)
        send_ref[here, pl.ds(offset, head_size)] = value_grad_ref[there, :].astype(BF16)


def head_specs(seq_len, group, kv_heads, head_size):
    query_spec = pl.BlockSpec((seq_len, group * head_size), lambda c: (0, c))
    key_spec = pl.BlockSpec((seq_len, head_size), lambda c: (0, kv_heads * group + c))
    value_spec = pl.BlockSpec((seq_len, head_size), lambda c: (0, kv_heads * (group + 1) + c))
    one_spec = pl.BlockSpec((seq_len, head_size), lambda c: (0, c))
    gain_spec = pl.BlockSpec((1, head_size), lambda c: (0, 0))
    table_spec = pl.BlockSpec((seq_len, head_size), lambda c: (0, 0))
    scalar_spec = pl.BlockSpec(memory_space=pltpu.SMEM)
    return query_spec, key_spec, value_spec, one_spec, gain_spec, table_spec, scalar_spec


def attend_forward(qkv_raw, share, length, gains, tables, masks, sizes):
    kv_heads, group, head_size = sizes
    seq_len = qkv_raw.shape[0]
    query, key, value, one, gain, table, scalar = head_specs(seq_len, group, kv_heads, head_size)
    wide, narrow = kv_heads * group * head_size, kv_heads * head_size
    return pl.pallas_call(
        functools.partial(attend_forward_kernel, masks, head_size, head_size ** (-0.5)),
        grid=(kv_heads,),
        in_specs=[scalar, scalar, query, key, value, gain, gain, table, table],
        out_specs=[query, query, query, one, one],
        out_shape=[
            jax.ShapeDtypeStruct((seq_len, wide), F32),
            jax.ShapeDtypeStruct((seq_len, wide), F32),
            jax.ShapeDtypeStruct((seq_len, wide), BF16),
            jax.ShapeDtypeStruct((seq_len, narrow), BF16),
            jax.ShapeDtypeStruct((seq_len, narrow), BF16),
        ],
        cost_estimate=pl.CostEstimate(
            flops=seq_len,
            bytes_accessed=seq_len,
            transcendentals=0,
        ),
        name="attend_forward",
    )(share, length, qkv_raw, qkv_raw, qkv_raw, *gains, *tables)


def attend_backward(grads, qkv_raw, kept, share, length, gains, tables, masks, sizes):
    kv_heads, group, head_size = sizes
    seq_len = qkv_raw.shape[0]
    query, key, value, one, gain, table, scalar = head_specs(seq_len, group, kv_heads, head_size)
    wide = kv_heads * group * head_size
    log_total, query_rot, key_rot, value_low = kept
    return pl.pallas_call(
        functools.partial(attend_backward_kernel, masks, head_size, head_size ** (-0.5)),
        grid=(kv_heads,),
        in_specs=[scalar, scalar, query, query, key, query, one, one, query]
        + [gain, gain, table, table],
        out_specs=[
            pl.BlockSpec(qkv_raw.shape, lambda c: (0, 0)),
            pl.BlockSpec((8, head_size), lambda c: (0, 0)),
        ],
        out_shape=[
            jax.ShapeDtypeStruct(qkv_raw.shape, BF16),
            jax.ShapeDtypeStruct((8, head_size), F32),
        ],
        scratch_shapes=[
            pltpu.VMEM((seq_len, group * head_size), F32),
            pltpu.VMEM((seq_len, head_size), F32),
            pltpu.VMEM((seq_len, head_size), F32),
        ],
        cost_estimate=pl.CostEstimate(
            flops=seq_len,
            bytes_accessed=seq_len,
            transcendentals=0,
        ),
        name="attend_backward",
    )(
        share,
        length,
        grads,
        qkv_raw,
        qkv_raw,
        query_rot,
        key_rot,
        value_low,
        log_total,
        *gains,
        *tables,
    )


def body(
    members,
    shares,
    hidden_in,
    lengths,
    attn_gain,
    query_weight,
    key_weight,
    value_weight,
    output_gate,
    query_gain,
    key_gain,
    out_weight,
    mlp_gain,
    gate_weight,
    up_weight,
    down_weight,
    cotangent,
):
    me = lax.axis_index("fsdp")
    share = lax.axis_index("tensor")
    local_rows = hidden_in.shape[0]
    length = lengths[0]
    head_size = query_gain.shape[0]
    query_width = query_weight.shape[1]
    key_width = key_weight.shape[1]
    sizes = (key_width // head_size, query_width // key_width, head_size)
    masks = row_masks(shares)
    slots = share * local_rows + jnp.arange(local_rows)
    valid_rows = (slots < length).astype(F32)[:, None]
    seq_len = local_rows * shares
    share_at, length_at = share.astype(jnp.int32)[None], lengths
    gains = (query_gain[None, :], key_gain[None, :])

    def relative(values):
        return to_pairs(values, me, members)

    def absolute(values):
        return to_index_order(values, me, members)

    attn_gain, mlp_gain = relative(attn_gain), relative(mlp_gain)

    qkv_near = gather_line(
        jnp.concatenate([query_weight, key_weight, value_weight], axis=1), members
    )
    gate_out_near = gather_line(
        jnp.concatenate([output_gate, out_weight.T], axis=1), members
    )
    down_own = down_weight.T
    down_pair = exchange(down_own, "fsdp", members, 1)
    gate_near = gather_line(hold(gate_weight, qkv_near, down_pair), members)
    up_near = gather_line(hold(up_weight, gate_out_near), members)
    down_near = gather_line(hold(down_own, gate_near), members)
    down_far = gather_line(hold(down_pair, up_near), members)

    residual = relative(hidden_in).astype(F32)
    unit_one, root_one = normalize(residual)
    normed_one = rows_in((unit_one * attn_gain).astype(BF16), shares)
    grad_rows = relative(cotangent).astype(F32) * valid_rows
    tables = rope_tables(seq_len, head_size)
    qkv_full = gather_pair(qkv_near, members)
    branch_full = rows_in(hold(grad_rows.astype(BF16), qkv_full), shares)
    qkv_raw = matmul(normed_one, qkv_full)
    qkv_raw = hold(qkv_raw, gate_out_near)
    attended, *kept = attend_forward(qkv_raw, share_at, length_at, gains, tables, masks, sizes)
    gate_out_full = gather_pair(gate_out_near, members, attended)
    gate_full, out_full = gate_out_full[:, :query_width], gate_out_full[:, query_width:]
    gate_pre = matmul(hold(normed_one, attended, branch_full), gate_full)
    gate_sig = jax.nn.sigmoid(gate_pre)
    gated_out = (attended * gate_sig).astype(BF16)
    half_rows = seq_len // 2
    attn_far = matmul_nt(gated_out[half_rows:], out_full).astype(BF16)
    attn_near = matmul_nt(gated_out[:half_rows], out_full).astype(BF16)
    attn_near = hold(attn_near, gate_near)
    gate_weights = gather_pair(gate_near, members)
    middle = residual + rows_out(attn_near, attn_far, shares)
    unit_two, root_two = normalize(middle)
    normed_two = rows_in((unit_two * mlp_gain).astype(BF16), shares)
    normed_two = hold(normed_two, up_near)
    up_weights = gather_pair(up_near, members)
    ffn_gate = matmul(normed_two, gate_weights)
    ffn_gate = hold(ffn_gate, down_near)
    ffn_up = matmul(normed_two, up_weights)
    ffn_sig = jax.nn.sigmoid(ffn_gate)
    ffn_act = ffn_gate * ffn_sig
    ffn_mid = (ffn_act * ffn_up).astype(BF16)

    def weight_grads(acts, grads):
        half = acts.shape[1] // 2
        far = matmul_tn(acts[:, half:], grads).astype(BF16)
        near = matmul_tn(acts[:, :half], grads).astype(BF16)
        return near, far

    down_near_part, down_far_part = weight_grads(branch_full, ffn_mid)
    down_far_sum = scatter_line(down_far_part, members)
    down_near_sum = scatter_line(down_near_part, members)
    down_arrived = exchange(down_far_sum, "fsdp", members, 1)
    down_shard = (down_near_sum.astype(F32) + down_arrived.astype(F32)).T

    down_far = hold(down_far, down_near_part, down_far_part)
    down_weights = jnp.concatenate([down_near, down_far], axis=0)
    mid_grad = matmul(branch_full, down_weights)
    gate_grad = (mid_grad * ffn_up * ffn_sig * (1.0 + ffn_gate * (1.0 - ffn_sig))).astype(BF16)
    up_grad = (mid_grad * ffn_act).astype(BF16)

    gate_near_sum, gate_far_sum = weight_grads(normed_two, gate_grad)
    gate_arrived = exchange(gate_far_sum, "fsdp", members, 1)

    gate_back, up_back = hold((gate_grad, up_grad), gate_far_sum)

    def ffn_back(rows):
        return matmul_nt(rows(gate_back), gate_weights) + matmul_nt(rows(up_back), up_weights)

    back_far = ffn_back(lambda g: g[half_rows:]).astype(BF16)
    back_near = ffn_back(lambda g: g[:half_rows]).astype(BF16)
    up_near_sum, up_far_sum = weight_grads(normed_two, up_grad)
    gate_total = add_low(gate_near_sum, gate_arrived)
    norm_two_grad = rows_out(back_near, back_far, shares, up_far_sum, gate_total)
    up_arrived = exchange(up_far_sum, "fsdp", members, 1)

    mlp_gain_part = jnp.sum(norm_two_grad * unit_two, axis=0)
    middle_grad = grad_rows + norm_back(norm_two_grad, unit_two, root_two, mlp_gain)
    mid_late = hold(ffn_mid, norm_two_grad)
    branch_far = matmul_nt(mid_late[half_rows:], down_weights).astype(BF16)
    branch_near = matmul_nt(mid_late[:half_rows], down_weights).astype(BF16)
    attn_full_grad = rows_in(middle_grad.astype(BF16), shares, branch_near, branch_far)
    gate_shard = scatter_line(gate_total, members)

    gated_grad = matmul(attn_full_grad, out_full)
    attended_grad = hold((gated_grad * gate_sig).astype(BF16), down_far_sum)
    gate_pre_grad = (gated_grad * attended * gate_sig * (1.0 - gate_sig)).astype(BF16)
    gate_attn_near_sum, gate_attn_far_sum = weight_grads(normed_one, gate_pre_grad)
    out_near_sum, out_far_sum = weight_grads(attn_full_grad, gated_out)
    gate_out_near_sum = jnp.concatenate([gate_attn_near_sum, out_near_sum], axis=1)
    gate_out_far_sum = jnp.concatenate([gate_attn_far_sum, out_far_sum], axis=1)
    gate_out_arrived = exchange(gate_out_far_sum, "fsdp", members, 1)
    ffn_branch = rows_out(branch_near, hold(branch_far, attn_full_grad), shares)
    output = absolute(((middle + ffn_branch) * valid_rows).astype(BF16))
    qkv_send, gain_parts = attend_backward(
        attended_grad, qkv_raw, kept, share_at, length_at, gains, tables, masks, sizes
    )
    qkv_near_sum, qkv_far_sum = weight_grads(normed_one, qkv_send)
    qkv_arrived = exchange(qkv_far_sum, "fsdp", members, 1)
    one_send, one_gate = hold((qkv_send, gate_pre_grad), qkv_far_sum)

    def attn_back(rows):
        return matmul_nt(rows(one_send), qkv_full) + matmul_nt(rows(one_gate), gate_full)

    one_far = attn_back(lambda g: g[half_rows:]).astype(BF16)
    one_near = attn_back(lambda g: g[:half_rows]).astype(BF16)
    up_total = add_low(up_near_sum, hold(up_arrived, one_near, one_far, down_near_sum))
    up_shard = scatter_line(up_total, members)
    norm_one_grad = rows_out(one_near, one_far, shares)
    attn_gain_part = jnp.sum(norm_one_grad * unit_one, axis=0)
    grad_hidden = absolute(
        middle_grad + norm_back(norm_one_grad, unit_one, root_one, attn_gain)
    )
    gain_totals = sum_everywhere(
        jnp.concatenate(
            [absolute(attn_gain_part), absolute(mlp_gain_part), gain_parts[0], gain_parts[1]]
        ),
        (("tensor", shares), ("fsdp", members)),
    )
    gate_out_total = add_low(
        gate_out_near_sum, hold(gate_out_arrived, gate_shard, norm_one_grad, ffn_branch)
    )
    gate_out_shard = scatter_line(gate_out_total, members)
    qkv_total = add_low(qkv_near_sum, hold(qkv_arrived, gate_out_total, up_shard))
    qkv_shard = scatter_line(qkv_total, members)
    gate_shard = gate_shard.astype(F32)
    up_shard = up_shard.astype(F32)
    gate_out_shard = gate_out_shard.astype(F32)
    qkv_shard = hold(
        qkv_shard, gain_totals, grad_hidden, output, gate_shard, up_shard, gate_out_shard, down_shard
    ).astype(F32)
    width = hidden_in.shape[1]
    return (
        output,
        grad_hidden,
        gain_totals[:width],
        qkv_shard[:, :query_width],
        qkv_shard[:, query_width : query_width + key_width],
        qkv_shard[:, query_width + key_width :],
        gate_out_shard[:, :query_width],
        gain_totals[2 * width : 2 * width + head_size],
        gain_totals[2 * width + head_size :],
        gate_out_shard[:, query_width:].T,
        gain_totals[width : 2 * width],
        gate_shard,
        up_shard,
        down_shard,
    )


def solution(mesh):
    members, shares = mesh.shape["fsdp"], mesh.shape["tensor"]

    def layer(*operands):
        return body(members, shares, *operands)

    tokens = P(("fsdp", "tensor"), None)
    return jax.shard_map(
        layer,
        mesh=mesh,
        in_specs=(
            tokens,
            P("fsdp"),
            P(),
            P("fsdp", "tensor"),
            P("fsdp", "tensor"),
            P("fsdp", "tensor"),
            P("fsdp", "tensor"),
            P(),
            P(),
            P("tensor", "fsdp"),
            P(),
            P("fsdp", "tensor"),
            P("fsdp", "tensor"),
            P("tensor", "fsdp"),
            tokens,
        ),
        out_specs=(
            tokens,
            tokens,
            P(),
            P("fsdp", "tensor"),
            P("fsdp", "tensor"),
            P("fsdp", "tensor"),
            P("fsdp", "tensor"),
            P(),
            P(),
            P("tensor", "fsdp"),
            P(),
            P("fsdp", "tensor"),
            P("fsdp", "tensor"),
            P("tensor", "fsdp"),
        ),
        check_vma=False,
    )
```

```python
import functools

import jax
import jax.numpy as jnp
from jax import lax
from jax.experimental import pallas as pl
from jax.experimental.pallas import tpu as pltpu
from jax.sharding import PartitionSpec as P

NORM_EPSILON = 1e-06
ROPE_THETA = 1000000.0
MASKED_LOGIT = -1e30
F32 = jnp.float32
BF16 = jnp.bfloat16


def exchange(values, axis, size, mask):
    return lax.ppermute(values, axis, [(i, i ^ mask) for i in range(size)])


def lines(count):
    return [list(range(0, count, 2)), list(range(1, count, 2))]


def gather_line(shard, count):
    return lax.all_gather(shard, "fsdp", axis=0, tiled=True, axis_index_groups=lines(count))


def gather_pair(near, count, *before):
    far = exchange(near, "fsdp", count, 1)
    if before:
        far = hold(far, *before)
    return jnp.concatenate([near, far], axis=0)


def scatter_line(total, count):
    return lax.psum_scatter(
        total, "fsdp", scatter_dimension=0, tiled=True, axis_index_groups=lines(count)
    )


def add_low(first, second):
    return (first.astype(F32) + second.astype(F32)).astype(BF16)


def hold(value, *others):
    return lax.optimization_barrier((value,) + others)[0]


def to_pairs(values, me, count):
    blocks = values.reshape(values.shape[:-1] + (count // 2, 2, values.shape[-1] // count))
    even = blocks[..., 0, :].reshape(values.shape[:-1] + (-1,))
    odd = blocks[..., 1, :].reshape(values.shape[:-1] + (-1,))
    first = me % 2 == 0
    return jnp.concatenate([jnp.where(first, even, odd), jnp.where(first, odd, even)], axis=-1)


def swap_pairs(values, me, count):
    blocks = values.reshape(values.shape[0], count // 2, 2, values.shape[1] // count)
    swapped = jnp.concatenate([blocks[:, :, 1:], blocks[:, :, :1]], axis=2)
    return jnp.where(me % 2 == 0, values, swapped.reshape(values.shape))


def to_index_order(values, me, count):
    width = values.shape[-1]
    shape = values.shape[:-1] + (count // 2, 1, width // count)
    near = values[..., : width // 2].reshape(shape)
    far = values[..., width // 2 :].reshape(shape)
    first = me % 2 == 0
    even, odd = jnp.where(first, near, far), jnp.where(first, far, near)
    return jnp.concatenate([even, odd], axis=-2).reshape(values.shape)


def row_masks(count):
    half = count // 2
    return [((p % half) << 1) | (p // half) for p in range(count)]


def place_of(mask, count):
    return (mask & 1) * (count // 2) + (mask >> 1)


def rows_in(values, count, *before):
    half = count // 2
    moved = [exchange(values, "tensor", count, step << 1) for step in range(1, half)]
    if before:
        moved = [hold(piece, *before) for piece in moved]
    near = [values] + moved
    far = [exchange(piece, "tensor", count, 1) for piece in near]
    return jnp.concatenate(near + far, axis=0)


def rows_out(near, far, count, *before):
    half = count // 2
    rows = near.shape[0] // half
    arrived = exchange(far.astype(BF16), "tensor", count, 1)

    def block(step):
        piece = slice(step * rows, (step + 1) * rows)
        return near[piece].astype(F32) + arrived[piece].astype(F32)

    moved = [
        exchange(block(step).astype(BF16), "tensor", count, step << 1) for step in range(1, half)
    ]
    result = block(0)
    for piece in moved:
        result = result + (hold(piece, *before) if before else piece).astype(F32)
    return result


def sum_everywhere(values, axes):
    for axis, count in axes:
        mask = 1
        while mask < count:
            values = values + exchange(values, axis, count, mask)
            mask <<= 1
    return values


def matmul(first_op, second_op):
    return jnp.dot(first_op, second_op, preferred_element_type=F32)


def matmul_tn(first_op, second_op):
    return lax.dot_general(
        first_op, second_op, (((0,), (0,)), ((), ())), preferred_element_type=F32
    )


def matmul_nt(first_op, second_op):
    return lax.dot_general(
        first_op, second_op, (((1,), (1,)), ((), ())), preferred_element_type=F32
    )


def normalize(values):
    inv_root = lax.rsqrt(jnp.mean(values * values, axis=-1, keepdims=True) + NORM_EPSILON)
    return (values * inv_root, inv_root)


def norm_back(gradient, unit_rows, inv_root, gain_vec):
    scaled = gradient * gain_vec
    return inv_root * (scaled - unit_rows * jnp.mean(scaled * unit_rows, axis=-1, keepdims=True))


def rope_tables(slot_count, head_size):
    half_width = head_size // 2
    inverse = ROPE_THETA ** (-(jnp.arange(half_width, dtype=F32) * 2.0 / head_size))
    angles = jnp.arange(slot_count, dtype=F32)[:, None] * inverse[None, :]
    cosine = jnp.concatenate([jnp.cos(angles), jnp.cos(angles)], axis=-1)
    signed_sine = jnp.concatenate([-jnp.sin(angles), jnp.sin(angles)], axis=-1)
    return (cosine, signed_sine)


def allowed_block(block, rows, width, length):
    row_slot = block * rows + lax.broadcasted_iota(jnp.int32, (rows, width), 0)
    col_slot = lax.broadcasted_iota(jnp.int32, (rows, width), 1)
    return (col_slot <= row_slot) & (col_slot < length)


def turn(unit_rows, gain_vec, cosine, signed_sine):
    normed = unit_rows * gain_vec
    half = normed.shape[-1] // 2
    return normed * cosine + pltpu.roll(normed, half, 1) * signed_sine


def turn_back(gradient, cosine, signed_sine):
    half = gradient.shape[-1] // 2
    return gradient * cosine - pltpu.roll(gradient, half, 1) * signed_sine


def attend_forward_kernel(
    masks,
    head_size,
    score_scale,
    share_ref,
    length_ref,
    query_ref,
    key_ref,
    value_ref,
    query_gain_ref,
    key_gain_ref,
    cosine_ref,
    sine_ref,
    attended_ref,
    log_ref,
    query_rot_ref,
    key_rot_ref,
    value_low_ref,
):
    blocks = len(masks)
    rows = query_ref.shape[0] // blocks
    group = query_ref.shape[1] // head_size
    share, length = share_ref[0], length_ref[0]
    for place, mask in enumerate(masks):
        here = pl.ds(place * rows, rows)
        there = pl.ds(pl.multiple_of((share ^ mask) * rows, rows), rows)
        cosine, signed_sine = cosine_ref[there, :], sine_ref[there, :]
        for head in range(group):
            cols = pl.ds(head * head_size, head_size)
            unit_rows, _ = normalize(query_ref[here, cols])
            turned = turn(unit_rows, query_gain_ref[...], cosine, signed_sine)
            query_rot_ref[there, cols] = turned.astype(BF16)
        unit_rows, _ = normalize(key_ref[here, :])
        turned = turn(unit_rows, key_gain_ref[...], cosine, signed_sine)
        key_rot_ref[there, :] = turned.astype(BF16)
        value_low_ref[there, :] = value_ref[here, :].astype(BF16)

    for block in range(blocks):
        width = (block + 1) * rows
        here = pl.ds(block * rows, rows)
        allowed = allowed_block(block, rows, width, length)
        back = pl.ds(pl.multiple_of(place_of(share ^ block, blocks) * rows, rows), rows)

        def one_head(head, carry, width=width, here=here, allowed=allowed, back=back):
            cols = pl.ds(pl.multiple_of(head * head_size, head_size), head_size)
            scores = matmul_nt(query_rot_ref[here, cols], key_rot_ref[:width, :])
            logits = jnp.where(allowed, scores * score_scale, MASKED_LOGIT)
            highest = jnp.max(logits, axis=-1, keepdims=True)
            weights_raw = jnp.exp(logits - highest)
            row_total = jnp.sum(weights_raw, axis=-1, keepdims=True)
            probabilities = (weights_raw * (1.0 / row_total)).astype(BF16)
            attended_ref[back, cols] = matmul(probabilities, value_low_ref[:width, :])
            log_ref[here, cols] = jnp.broadcast_to(highest + jnp.log(row_total), (rows, head_size))
            return carry

        lax.fori_loop(0, group, one_head, 0)


def attend_backward_kernel(
    masks,
    head_size,
    score_scale,
    share_ref,
    length_ref,
    grad_ref,
    query_ref,
    key_ref,
    query_rot_ref,
    key_rot_ref,
    value_low_ref,
    log_ref,
    query_gain_ref,
    key_gain_ref,
    cosine_ref,
    sine_ref,
    send_ref,
    gain_ref,
    query_grad_ref,
    key_grad_ref,
    value_grad_ref,
):
    blocks = len(masks)
    rows = query_ref.shape[0] // blocks
    group = query_ref.shape[1] // head_size
    kv_heads = pl.num_programs(0)
    kv_head = pl.program_id(0)
    share, length = share_ref[0], length_ref[0]
    key_grad_ref[...] = jnp.zeros_like(key_grad_ref)
    value_grad_ref[...] = jnp.zeros_like(value_grad_ref)

    @pl.when(kv_head == 0)
    def _():
        gain_ref[...] = jnp.zeros_like(gain_ref)

    for block in range(blocks):
        width = (block + 1) * rows
        here = pl.ds(block * rows, rows)
        allowed = allowed_block(block, rows, width, length)
        back = pl.ds(pl.multiple_of(place_of(share ^ block, blocks) * rows, rows), rows)

        def one_head(head, carry, width=width, here=here, allowed=allowed, back=back):
            cols = pl.ds(pl.multiple_of(head * head_size, head_size), head_size)
            queries, grads = query_rot_ref[here, cols], grad_ref[back, cols]
            scores = matmul_nt(queries, key_rot_ref[:width, :])
            logits = jnp.where(allowed, scores * score_scale, MASKED_LOGIT)
            soft = jnp.where(allowed, jnp.exp(logits - log_ref[here, cols][:, :1]), 0.0)
            prob_grad = matmul_nt(grads, value_low_ref[:width, :])
            centre = jnp.sum(soft * prob_grad, axis=-1, keepdims=True)
            score_grad = (score_scale * soft * (prob_grad - centre)).astype(BF16)
            query_grad_ref[here, cols] = matmul(score_grad, key_rot_ref[:width, :])
            key_grad_ref[:width, :] += matmul_tn(score_grad, queries)
            value_grad_ref[:width, :] += matmul_tn(soft.astype(BF16), grads)
            return carry

        lax.fori_loop(0, group, one_head, 0)

    key_base, value_base = kv_heads * group * head_size, kv_heads * (group + 1) * head_size
    for place, mask in enumerate(masks):
        here = pl.ds(place * rows, rows)
        there = pl.ds(pl.multiple_of((share ^ mask) * rows, rows), rows)
        cosine, signed_sine = cosine_ref[there, :], sine_ref[there, :]

        def through_norm(gradient, raw, gain_vec):
            normed_grad = turn_back(gradient, cosine, signed_sine)
            unit_rows, inv_root = normalize(raw)
            gain_part = jnp.sum(normed_grad * unit_rows, axis=0, keepdims=True)
            return norm_back(normed_grad, unit_rows, inv_root, gain_vec).astype(BF16), gain_part

        for head in range(group):
            cols = pl.ds(head * head_size, head_size)
            sent, gain_part = through_norm(
                query_grad_ref[there, cols], query_ref[here, cols], query_gain_ref[...]
            )
            offset = pl.multiple_of((kv_head * group + head) * head_size, head_size)
            send_ref[here, pl.ds(offset, head_size)] = sent
            gain_ref[0:1, :] += gain_part
        sent, gain_part = through_norm(key_grad_ref[there, :], key_ref[here, :], key_gain_ref[...])
        offset = pl.multiple_of(key_base + kv_head * head_size, head_size)
        send_ref[here, pl.ds(offset, head_size)] = sent
        gain_ref[1:2, :] += gain_part
        offset = pl.multiple_of(value_base + kv_head * head_size, head_size)
        send_ref[here, pl.ds(offset, head_size)] = value_grad_ref[there, :].astype(BF16)


def head_specs(seq_len, group, kv_heads, head_size):
    query_spec = pl.BlockSpec((seq_len, group * head_size), lambda c: (0, c))
    key_spec = pl.BlockSpec((seq_len, head_size), lambda c: (0, kv_heads * group + c))
    value_spec = pl.BlockSpec((seq_len, head_size), lambda c: (0, kv_heads * (group + 1) + c))
    one_spec = pl.BlockSpec((seq_len, head_size), lambda c: (0, c))
    gain_spec = pl.BlockSpec((1, head_size), lambda c: (0, 0))
    table_spec = pl.BlockSpec((seq_len, head_size), lambda c: (0, 0))
    scalar_spec = pl.BlockSpec(memory_space=pltpu.SMEM)
    return query_spec, key_spec, value_spec, one_spec, gain_spec, table_spec, scalar_spec


def attend_forward(qkv_raw, share, length, gains, tables, masks, sizes):
    kv_heads, group, head_size = sizes
    seq_len = qkv_raw.shape[0]
    query, key, value, one, gain, table, scalar = head_specs(seq_len, group, kv_heads, head_size)
    wide, narrow = kv_heads * group * head_size, kv_heads * head_size
    return pl.pallas_call(
        functools.partial(attend_forward_kernel, masks, head_size, head_size ** (-0.5)),
        grid=(kv_heads,),
        in_specs=[scalar, scalar, query, key, value, gain, gain, table, table],
        out_specs=[query, query, query, one, one],
        out_shape=[
            jax.ShapeDtypeStruct((seq_len, wide), F32),
            jax.ShapeDtypeStruct((seq_len, wide), F32),
            jax.ShapeDtypeStruct((seq_len, wide), BF16),
            jax.ShapeDtypeStruct((seq_len, narrow), BF16),
            jax.ShapeDtypeStruct((seq_len, narrow), BF16),
        ],
        cost_estimate=pl.CostEstimate(
            flops=seq_len,
            bytes_accessed=seq_len,
            transcendentals=0,
        ),
        name="attend_forward",
    )(share, length, qkv_raw, qkv_raw, qkv_raw, *gains, *tables)


def attend_backward(grads, qkv_raw, kept, share, length, gains, tables, masks, sizes):
    kv_heads, group, head_size = sizes
    seq_len = qkv_raw.shape[0]
    query, key, value, one, gain, table, scalar = head_specs(seq_len, group, kv_heads, head_size)
    wide = kv_heads * group * head_size
    log_total, query_rot, key_rot, value_low = kept
    return pl.pallas_call(
        functools.partial(attend_backward_kernel, masks, head_size, head_size ** (-0.5)),
        grid=(kv_heads,),
        in_specs=[scalar, scalar, query, query, key, query, one, one, query]
        + [gain, gain, table, table],
        out_specs=[
            pl.BlockSpec(qkv_raw.shape, lambda c: (0, 0)),
            pl.BlockSpec((8, head_size), lambda c: (0, 0)),
        ],
        out_shape=[
            jax.ShapeDtypeStruct(qkv_raw.shape, BF16),
            jax.ShapeDtypeStruct((8, head_size), F32),
        ],
        scratch_shapes=[
            pltpu.VMEM((seq_len, group * head_size), F32),
            pltpu.VMEM((seq_len, head_size), F32),
            pltpu.VMEM((seq_len, head_size), F32),
        ],
        cost_estimate=pl.CostEstimate(
            flops=seq_len,
            bytes_accessed=seq_len,
            transcendentals=0,
        ),
        name="attend_backward",
    )(
        share,
        length,
        grads,
        qkv_raw,
        qkv_raw,
        query_rot,
        key_rot,
        value_low,
        log_total,
        *gains,
        *tables,
    )


def body(
    members,
    shares,
    hidden_in,
    lengths,
    attn_gain,
    query_weight,
    key_weight,
    value_weight,
    output_gate,
    query_gain,
    key_gain,
    out_weight,
    mlp_gain,
    gate_weight,
    up_weight,
    down_weight,
    cotangent,
):
    me = lax.axis_index("fsdp")
    share = lax.axis_index("tensor")
    local_rows = hidden_in.shape[0]
    length = lengths[0]
    head_size = query_gain.shape[0]
    query_width = query_weight.shape[1]
    key_width = key_weight.shape[1]
    sizes = (key_width // head_size, query_width // key_width, head_size)
    masks = row_masks(shares)
    slots = share * local_rows + jnp.arange(local_rows)
    valid_rows = (slots < length).astype(F32)[:, None]
    seq_len = local_rows * shares
    share_at, length_at = share.astype(jnp.int32)[None], lengths
    gains = (query_gain[None, :], key_gain[None, :])

    def relative(values):
        return to_pairs(values, me, members)

    def absolute(values):
        return to_index_order(values, me, members)

    attn_gain, mlp_gain = relative(attn_gain), relative(mlp_gain)

    qkv_near = gather_line(
        jnp.concatenate([query_weight, key_weight, value_weight], axis=1), members
    )
    gate_out_near = gather_line(
        jnp.concatenate([output_gate, out_weight.T], axis=1), members
    )
    down_own = down_weight.T
    down_pair = exchange(down_own, "fsdp", members, 1)
    gate_near = gather_line(hold(gate_weight, qkv_near, down_pair), members)
    up_near = gather_line(hold(up_weight, gate_out_near), members)
    down_both = jnp.concatenate([down_own, down_pair], axis=0)
    down_weights = gather_line(hold(down_both, gate_near), members)

    residual = relative(hidden_in).astype(F32)
    unit_one, root_one = normalize(residual)
    normed_one = rows_in((unit_one * attn_gain).astype(BF16), shares)
    grad_rows = relative(cotangent).astype(F32) * valid_rows
    tables = rope_tables(seq_len, head_size)
    qkv_full = gather_pair(qkv_near, members)
    qkv_raw = matmul(normed_one, qkv_full)
    qkv_raw = hold(qkv_raw, gate_out_near)
    attended, *kept = attend_forward(qkv_raw, share_at, length_at, gains, tables, masks, sizes)
    branch_rows = swap_pairs(cotangent.astype(F32) * valid_rows, me, members).astype(BF16)
    branch_full = rows_in(hold(branch_rows, qkv_full), shares, attended)
    gate_out_full = gather_pair(gate_out_near, members, attended)
    gate_full, out_full = gate_out_full[:, :query_width], gate_out_full[:, query_width:]
    gate_pre = matmul(hold(normed_one, attended, branch_full), gate_full)
    gate_sig = jax.nn.sigmoid(gate_pre)
    gated_out = (attended * gate_sig).astype(BF16)
    half_rows = seq_len // 2
    attn_far = matmul_nt(gated_out[half_rows:], out_full).astype(BF16)
    attn_near = matmul_nt(gated_out[:half_rows], out_full).astype(BF16)
    attn_near = hold(attn_near, gate_near)
    gate_weights = gather_pair(gate_near, members)
    middle = residual + rows_out(attn_near, attn_far, shares)
    unit_two, root_two = normalize(middle)
    normed_two = rows_in((unit_two * mlp_gain).astype(BF16), shares)
    normed_two = hold(normed_two, up_near)
    half_width = normed_two.shape[1] // 2
    up_far = exchange(up_near, "fsdp", members, 1)
    ffn_gate = matmul(normed_two, gate_weights)
    up_part = matmul(normed_two[:, :half_width], up_near)
    up_far = hold(up_far, up_part, ffn_gate)
    up_weights = jnp.concatenate([up_near, up_far], axis=0)
    ffn_up = up_part + matmul(normed_two[:, half_width:], up_far)
    ffn_sig = jax.nn.sigmoid(ffn_gate)
    ffn_act = ffn_gate * ffn_sig
    ffn_mid = (ffn_act * ffn_up).astype(BF16)

    def weight_grads(acts, grads):
        half = acts.shape[1] // 2
        far = matmul_tn(acts[:, half:], grads).astype(BF16)
        near = matmul_tn(acts[:, :half], grads).astype(BF16)
        return near, far

    down_part = matmul_tn(branch_full, ffn_mid).astype(BF16)
    down_sum = scatter_line(down_part, members)
    own_rows = down_sum.shape[0] // 2
    down_arrived = exchange(down_sum[own_rows:], "fsdp", members, 1)
    down_shard = (down_sum[:own_rows].astype(F32) + down_arrived.astype(F32)).T

    mid_grad = matmul(branch_full, hold(down_weights, down_part))
    gate_grad = (mid_grad * ffn_up * ffn_sig * (1.0 + ffn_gate * (1.0 - ffn_sig))).astype(BF16)
    up_grad = (mid_grad * ffn_act).astype(BF16)

    gate_near_sum, gate_far_sum = weight_grads(normed_two, gate_grad)
    gate_arrived = exchange(gate_far_sum, "fsdp", members, 1)

    gate_back, up_back = hold((gate_grad, up_grad), gate_far_sum)

    def ffn_back(rows):
        return matmul_nt(rows(gate_back), gate_weights) + matmul_nt(rows(up_back), up_weights)

    back_far = ffn_back(lambda g: g[half_rows:]).astype(BF16)
    back_near = ffn_back(lambda g: g[:half_rows]).astype(BF16)
    up_near_sum, up_far_sum = weight_grads(normed_two, up_grad)
    gate_total = add_low(gate_near_sum, gate_arrived)
    norm_two_grad = rows_out(back_near, back_far, shares, up_far_sum, gate_total)
    up_arrived = exchange(up_far_sum, "fsdp", members, 1)

    mlp_gain_part = jnp.sum(norm_two_grad * unit_two, axis=0)
    middle_grad = grad_rows + norm_back(norm_two_grad, unit_two, root_two, mlp_gain)
    mid_late = hold(ffn_mid, norm_two_grad)
    branch_far = matmul_nt(mid_late[half_rows:], down_weights).astype(BF16)
    branch_near = matmul_nt(mid_late[:half_rows], down_weights).astype(BF16)
    attn_full_grad = rows_in(middle_grad.astype(BF16), shares, branch_near, branch_far)
    gate_shard = scatter_line(gate_total, members)

    gated_grad = matmul(attn_full_grad, out_full)
    attended_grad = hold((gated_grad * gate_sig).astype(BF16), down_sum)
    gate_pre_grad = (gated_grad * attended * gate_sig * (1.0 - gate_sig)).astype(BF16)
    gate_attn_near_sum, gate_attn_far_sum = weight_grads(normed_one, gate_pre_grad)
    out_near_sum, out_far_sum = weight_grads(attn_full_grad, gated_out)
    gate_out_near_sum = jnp.concatenate([gate_attn_near_sum, out_near_sum], axis=1)
    gate_out_far_sum = jnp.concatenate([gate_attn_far_sum, out_far_sum], axis=1)
    gate_out_arrived = exchange(gate_out_far_sum, "fsdp", members, 1)
    ffn_branch = rows_out(branch_near, hold(branch_far, attn_full_grad), shares)
    ffn_branch = swap_pairs(ffn_branch, me, members)
    output = ((absolute(middle) + ffn_branch) * valid_rows).astype(BF16)
    qkv_send, gain_parts = attend_backward(
        attended_grad, qkv_raw, kept, share_at, length_at, gains, tables, masks, sizes
    )
    up_total = add_low(up_near_sum, hold(up_arrived, qkv_send))
    up_shard = scatter_line(up_total, members)
    qkv_near_sum, qkv_far_sum = weight_grads(normed_one, hold(qkv_send, up_total))
    qkv_arrived = exchange(qkv_far_sum, "fsdp", members, 1)
    one_send, one_gate = hold((qkv_send, gate_pre_grad), qkv_far_sum)

    def attn_back(rows):
        return matmul_nt(rows(one_send), qkv_full) + matmul_nt(rows(one_gate), gate_full)

    one_far = attn_back(lambda g: g[half_rows:]).astype(BF16)
    one_near = attn_back(lambda g: g[:half_rows]).astype(BF16)
    gate_out_total = add_low(
        gate_out_near_sum, hold(gate_out_arrived, gate_shard, one_near, one_far)
    )
    gate_out_shard = scatter_line(gate_out_total, members)
    norm_one_grad = rows_out(one_near, one_far, shares, gate_out_total)
    attn_gain_part = jnp.sum(norm_one_grad * unit_one, axis=0)
    grad_hidden = absolute(
        middle_grad + norm_back(norm_one_grad, unit_one, root_one, attn_gain)
    )
    gain_totals = sum_everywhere(
        jnp.concatenate(
            [absolute(attn_gain_part), absolute(mlp_gain_part), gain_parts[0], gain_parts[1]]
        ),
        (("tensor", shares), ("fsdp", members)),
    )
    qkv_total = add_low(qkv_near_sum, hold(qkv_arrived, up_shard, grad_hidden, ffn_branch))
    qkv_shard = scatter_line(qkv_total, members)
    gate_shard = gate_shard.astype(F32)
    up_shard = up_shard.astype(F32)
    gate_out_shard = gate_out_shard.astype(F32)
    qkv_shard = hold(
        qkv_shard, gain_totals, grad_hidden, output, gate_shard, up_shard, gate_out_shard, down_shard
    ).astype(F32)
    width = hidden_in.shape[1]
    return (
        output,
        grad_hidden,
        gain_totals[:width],
        qkv_shard[:, :query_width],
        qkv_shard[:, query_width : query_width + key_width],
        qkv_shard[:, query_width + key_width :],
        gate_out_shard[:, :query_width],
        gain_totals[2 * width : 2 * width + head_size],
        gain_totals[2 * width + head_size :],
        gate_out_shard[:, query_width:].T,
        gain_totals[width : 2 * width],
        gate_shard,
        up_shard,
        down_shard,
    )


def solution(mesh):
    members, shares = mesh.shape["fsdp"], mesh.shape["tensor"]

    def layer(*operands):
        return body(members, shares, *operands)

    tokens = P(("fsdp", "tensor"), None)
    return jax.shard_map(
        layer,
        mesh=mesh,
        in_specs=(
            tokens,
            P("fsdp"),
            P(),
            P("fsdp", "tensor"),
            P("fsdp", "tensor"),
            P("fsdp", "tensor"),
            P("fsdp", "tensor"),
            P(),
            P(),
            P("tensor", "fsdp"),
            P(),
            P("fsdp", "tensor"),
            P("fsdp", "tensor"),
            P("tensor", "fsdp"),
            tokens,
        ),
        out_specs=(
            tokens,
            tokens,
            P(),
            P("fsdp", "tensor"),
            P("fsdp", "tensor"),
            P("fsdp", "tensor"),
            P("fsdp", "tensor"),
            P(),
            P(),
            P("tensor", "fsdp"),
            P(),
            P("fsdp", "tensor"),
            P("fsdp", "tensor"),
            P("tensor", "fsdp"),
        ),
        check_vma=False,
    )
```

```python
import functools

import jax
import jax.numpy as jnp
from jax import lax
from jax.experimental import pallas as pl
from jax.experimental.pallas import tpu as pltpu
from jax.sharding import PartitionSpec as P

NORM_EPSILON = 1e-06
ROPE_THETA = 1000000.0
MASKED_LOGIT = -1e30
F32 = jnp.float32
BF16 = jnp.bfloat16


def exchange(values, axis, size, mask):
    return lax.ppermute(values, axis, [(i, i ^ mask) for i in range(size)])


def lines(count):
    return [list(range(0, count, 2)), list(range(1, count, 2))]


def to_partner(values, count):
    return exchange(values, "fsdp", count, 1)


def halves(values, odd):
    width = values.shape[-1] // 2
    left, right = values[..., :width], values[..., width:]
    return jnp.where(odd, right, left), jnp.where(odd, left, right)


def in_order(own, other, odd, axis):
    first, second = jnp.where(odd, other, own), jnp.where(odd, own, other)
    return jnp.concatenate([first, second], axis=axis)


def pair_rows(shards, odd, count, *before):
    split = [halves(shard, odd) for shard in shards]
    own = jnp.concatenate([piece[0] for piece in split], axis=1)
    other = jnp.concatenate([piece[1] for piece in split], axis=1)
    arrived = to_partner(other, count)
    if before:
        arrived = hold(arrived, *before)
    return in_order(own, arrived, odd, 0)


def gather_line(rows, count):
    return lax.all_gather(rows, "fsdp", axis=0, tiled=True, axis_index_groups=lines(count))


def scatter_line(total, count):
    return lax.psum_scatter(
        total, "fsdp", scatter_dimension=0, tiled=True, axis_index_groups=lines(count)
    )


def swap_rows(rows, odd, count):
    height = rows.shape[0] // 2
    top, bottom = rows[:height], rows[height:]
    return jnp.where(odd, bottom, top), to_partner(jnp.where(odd, top, bottom), count)


def own_shard(own, other, odd, widths):
    shards, start = [], 0
    for width in widths:
        piece = slice(start, start + width)
        shards.append(in_order(own[:, piece], other[:, piece], odd, 1).astype(F32))
        start += width
    return shards


def hold(value, *others):
    return lax.optimization_barrier((value,) + others)[0]


def row_masks(count):
    half = count // 2
    return [((p % half) << 1) | (p // half) for p in range(count)]


def across(values, count):
    return exchange(values, "tensor", count, 2)


def core(values, count):
    return exchange(values, "tensor", count, 1)


def rows_in(values, members, shares, *before):
    half = values.shape[0] // 2
    side = across(values, shares)
    partner = to_partner(values, members)
    if before and before[0] is not None:
        side, partner = hold((side, partner), before[0])
    upper = to_partner(side[:half], members)
    lower = across(partner[half:], shares)
    if before[1:]:
        upper, lower = hold((upper, lower), *before[1:])
    near = [values, side, partner, upper, lower]
    return stack_rows(near + [core(piece, shares) for piece in near])


def stack_kernel(count, *refs):
    pieces, out, held, in_sems, out_sems = refs[:count], *refs[count:]
    incoming, outgoing, start = [], [], 0
    for i, piece in enumerate(pieces):
        place = pl.ds(start, piece.shape[0])
        incoming.append(pltpu.make_async_copy(piece, held.at[place], in_sems.at[i]))
        outgoing.append(pltpu.make_async_copy(held.at[place], out.at[place], out_sems.at[i]))
        incoming[-1].start()
        start += piece.shape[0]
    for arrive, leave in zip(incoming, outgoing):
        arrive.wait()
        leave.start()
    for leave in outgoing:
        leave.wait()


def stack_rows(pieces):
    count, (_, width), kind = len(pieces), pieces[0].shape, pieces[0].dtype
    rows = sum(piece.shape[0] for piece in pieces)
    anywhere = pl.BlockSpec(memory_space=pl.ANY)
    return pl.pallas_call(
        functools.partial(stack_kernel, count),
        in_specs=[anywhere] * count,
        out_specs=anywhere,
        out_shape=jax.ShapeDtypeStruct((rows, width), kind),
        scratch_shapes=[
            pltpu.VMEM((rows, width), kind),
            pltpu.SemaphoreType.DMA((count,)),
            pltpu.SemaphoreType.DMA((count,)),
        ],
        compiler_params=pltpu.CompilerParams(vmem_limit_bytes=(rows * width * 2) + (1 << 20)),
        cost_estimate=light_cost(),
        name="stack_rows",
    )(*pieces)


def light_cost():
    return pl.CostEstimate(flops=1024, bytes_accessed=1024, transcendentals=0)


def corner_kernel(near_ref, arrived_ref, upper_ref, lower_ref):
    half = upper_ref.shape[0]
    total = (near_ref[...].astype(F32) + arrived_ref[...].astype(F32)).astype(BF16)
    upper_ref[...] = total[:half]
    lower_ref[...] = total[half:]


def add_corner(near, arrived):
    rows, width = arrived.shape
    tile = width // 2
    half = pl.BlockSpec((rows // 2, tile), lambda i: (0, i))
    return pl.pallas_call(
        corner_kernel,
        grid=(2,),
        in_specs=[
            pl.BlockSpec((rows, tile), lambda i: (3, i)),
            pl.BlockSpec((rows, tile), lambda i: (0, i)),
        ],
        out_specs=[half, half],
        out_shape=[jax.ShapeDtypeStruct((rows // 2, width), BF16)] * 2,
        compiler_params=pltpu.CompilerParams(vmem_limit_bytes=16 << 20),
        cost_estimate=light_cost(),
        name="add_corner",
    )(near, arrived)


def main_kernel(near_ref, arrived_ref, own_ref, side_a, side_b, partner_a, partner_b):
    rows = own_ref.shape[0]
    half = rows // 2

    def total(start, size):
        piece = pl.ds(start, size)
        return near_ref[piece, :].astype(F32) + arrived_ref[piece, :].astype(F32)

    own_ref[...] = total(0, rows)
    side_a[...] = total(rows, half).astype(BF16)
    side_b[...] = total(rows + half, half)
    partner_a[...] = total(2 * rows, half)
    partner_b[...] = total(2 * rows + half, half).astype(BF16)


def add_main(near, arrived):
    rows, width = arrived.shape[0] // 3, arrived.shape[1]
    tile = width // 4
    whole = pl.BlockSpec((rows, tile), lambda i: (0, i))
    half = pl.BlockSpec((rows // 2, tile), lambda i: (0, i))
    three = pl.BlockSpec((3 * rows, tile), lambda i: (0, i))

    def shape(kind):
        return jax.ShapeDtypeStruct((rows // 2, width), kind)

    return pl.pallas_call(
        main_kernel,
        grid=(4,),
        in_specs=[three, three],
        out_specs=[whole, half, half, half, half],
        out_shape=[
            jax.ShapeDtypeStruct((rows, width), F32),
            shape(BF16),
            shape(F32),
            shape(F32),
            shape(BF16),
        ],
        compiler_params=pltpu.CompilerParams(vmem_limit_bytes=24 << 20),
        cost_estimate=light_cost(),
        name="add_main",
    )(near, arrived)


def open_sum(parts, members, shares, *before):
    near, far, far_corner = parts
    arrived_corner, arrived = core(far_corner, shares), core(far, shares)
    if before:
        arrived_corner, arrived = hold((arrived_corner, arrived), *before)
    upper, lower = add_corner(near, arrived_corner)
    corners = across(upper, shares), to_partner(lower, members)
    own, side_a, side_b, partner_a, partner_b = add_main(near, arrived)
    return corners, (own, side_b, partner_a, across(side_a, shares), to_partner(partner_b, members))


def close_sum(corners, opened, members, shares, *before):
    corner_side, corner_partner = corners
    own, side, partner, side_first, partner_first = opened
    side_second = across((side + corner_partner.astype(F32)).astype(BF16), shares)
    partner_second = to_partner((partner + corner_side.astype(F32)).astype(BF16), members)
    if before:
        side_second, partner_second = hold((side_second, partner_second), *before)
    from_side = jnp.concatenate([side_first, side_second], axis=0).astype(F32)
    from_partner = jnp.concatenate([partner_second, partner_first], axis=0).astype(F32)
    return own + from_side + from_partner


def sum_everywhere(values, axes):
    for axis, count in axes:
        mask = 1
        while mask < count:
            values = values + exchange(values, axis, count, mask)
            mask <<= 1
    return values


def matmul(first_op, second_op):
    return jnp.dot(first_op, second_op, preferred_element_type=F32)


def matmul_tn(first_op, second_op):
    return lax.dot_general(
        first_op, second_op, (((0,), (0,)), ((), ())), preferred_element_type=F32
    )


def matmul_nt(first_op, second_op):
    return lax.dot_general(
        first_op, second_op, (((1,), (1,)), ((), ())), preferred_element_type=F32
    )


def normalize(values):
    inv_root = lax.rsqrt(jnp.mean(values * values, axis=-1, keepdims=True) + NORM_EPSILON)
    return (values * inv_root, inv_root)


def norm_back(gradient, unit_rows, inv_root, gain_vec):
    scaled = gradient * gain_vec
    return inv_root * (scaled - unit_rows * jnp.mean(scaled * unit_rows, axis=-1, keepdims=True))


def rope_tables(slot_count, head_size):
    half_width = head_size // 2
    inverse = ROPE_THETA ** (-(jnp.arange(half_width, dtype=F32) * 2.0 / head_size))
    angles = jnp.arange(slot_count, dtype=F32)[:, None] * inverse[None, :]
    cosine = jnp.concatenate([jnp.cos(angles), jnp.cos(angles)], axis=-1)
    signed_sine = jnp.concatenate([-jnp.sin(angles), jnp.sin(angles)], axis=-1)
    return (cosine, signed_sine)


def piece_of(mask, rows):
    return mask & 1, pl.ds(pl.multiple_of((mask >> 1) * rows, rows), rows)


def allowed_block(block, rows, width, length):
    row_slot = block * rows + lax.broadcasted_iota(jnp.int32, (rows, width), 0)
    col_slot = lax.broadcasted_iota(jnp.int32, (rows, width), 1)
    return (col_slot <= row_slot) & (col_slot < length)


def turn(unit_rows, gain_vec, cosine, signed_sine):
    normed = unit_rows * gain_vec
    half = normed.shape[-1] // 2
    return normed * cosine + pltpu.roll(normed, half, 1) * signed_sine


def turn_back(gradient, cosine, signed_sine):
    half = gradient.shape[-1] // 2
    return gradient * cosine - pltpu.roll(gradient, half, 1) * signed_sine


def attend_forward_kernel(
    masks,
    head_size,
    score_scale,
    share_ref,
    length_ref,
    query_ref,
    key_ref,
    value_ref,
    query_gain_ref,
    key_gain_ref,
    cosine_ref,
    sine_ref,
    attended_ref,
    log_ref,
    query_rot_ref,
    key_rot_ref,
    value_low_ref,
):
    blocks = len(masks)
    rows = 2 * query_ref.shape[1] // blocks
    group = query_ref.shape[2] // head_size
    share, length = share_ref[0], length_ref[pl.program_id(0)]
    for mask in masks:
        side, here = mask & 1, pl.ds((mask >> 1) * rows, rows)
        there = pl.ds(pl.multiple_of((share ^ mask) * rows, rows), rows)
        cosine, signed_sine = cosine_ref[there, :], sine_ref[there, :]
        for head in range(group):
            cols = pl.ds(head * head_size, head_size)
            unit_rows, _ = normalize(query_ref[side, here, cols])
            turned = turn(unit_rows, query_gain_ref[...], cosine, signed_sine)
            query_rot_ref[there, cols] = turned.astype(BF16)
        unit_rows, _ = normalize(key_ref[side, here, :])
        turned = turn(unit_rows, key_gain_ref[...], cosine, signed_sine)
        key_rot_ref[there, :] = turned.astype(BF16)
        value_low_ref[there, :] = value_ref[side, here, :].astype(BF16)

    for block in range(blocks):
        width = (block + 1) * rows
        here = pl.ds(block * rows, rows)
        allowed = allowed_block(block, rows, width, length)
        side, back = piece_of(share ^ block, rows)

        def one_head(head, carry, width=width, here=here, allowed=allowed, side=side, back=back):
            cols = pl.ds(pl.multiple_of(head * head_size, head_size), head_size)
            scores = matmul_nt(query_rot_ref[here, cols], key_rot_ref[:width, :])
            logits = jnp.where(allowed, scores * score_scale, MASKED_LOGIT)
            highest = jnp.max(logits, axis=-1, keepdims=True)
            weights_raw = jnp.exp(logits - highest)
            row_total = jnp.sum(weights_raw, axis=-1, keepdims=True)
            probabilities = (weights_raw * (1.0 / row_total)).astype(BF16)
            attended_ref[side, back, cols] = matmul(probabilities, value_low_ref[:width, :])
            log_ref[here, cols] = jnp.broadcast_to(highest + jnp.log(row_total), (rows, head_size))
            return carry

        lax.fori_loop(0, group, one_head, 0)


def attend_backward_kernel(
    masks,
    head_size,
    score_scale,
    share_ref,
    length_ref,
    grad_ref,
    gate_grad_ref,
    query_ref,
    key_ref,
    query_rot_ref,
    key_rot_ref,
    value_low_ref,
    log_ref,
    query_gain_ref,
    key_gain_ref,
    cosine_ref,
    sine_ref,
    send_ref,
    gain_ref,
    query_grad_ref,
    key_grad_ref,
    value_grad_ref,
):
    blocks = len(masks)
    rows = 2 * query_ref.shape[1] // blocks
    group = query_ref.shape[2] // head_size
    kv_heads = pl.num_programs(1)
    kv_head = pl.program_id(1)
    share, length = share_ref[0], length_ref[pl.program_id(0)]
    key_grad_ref[...] = jnp.zeros_like(key_grad_ref)
    value_grad_ref[...] = jnp.zeros_like(value_grad_ref)

    @pl.when((pl.program_id(0) == 0) & (kv_head == 0))
    def _():
        gain_ref[...] = jnp.zeros_like(gain_ref)

    for block in range(blocks):
        width = (block + 1) * rows
        here = pl.ds(block * rows, rows)
        allowed = allowed_block(block, rows, width, length)
        side, back = piece_of(share ^ block, rows)

        def one_head(head, carry, width=width, here=here, allowed=allowed, side=side, back=back):
            cols = pl.ds(pl.multiple_of(head * head_size, head_size), head_size)
            queries, grads = query_rot_ref[here, cols], grad_ref[side, back, cols]
            scores = matmul_nt(queries, key_rot_ref[:width, :])
            logits = jnp.where(allowed, scores * score_scale, MASKED_LOGIT)
            soft = jnp.where(allowed, jnp.exp(logits - log_ref[here, cols][:, :1]), 0.0)
            prob_grad = matmul_nt(grads, value_low_ref[:width, :])
            centre = jnp.sum(soft * prob_grad, axis=-1, keepdims=True)
            score_grad = (score_scale * soft * (prob_grad - centre)).astype(BF16)
            query_grad_ref[here, cols] = matmul(score_grad, key_rot_ref[:width, :])
            key_grad_ref[:width, :] += matmul_tn(score_grad, queries)
            value_grad_ref[:width, :] += matmul_tn(soft.astype(BF16), grads)
            return carry

        lax.fori_loop(0, group, one_head, 0)

    key_base, value_base = kv_heads * group * head_size, kv_heads * (group + 1) * head_size
    gate_base = kv_heads * (group + 2) * head_size
    for mask in masks:
        side, here = mask & 1, pl.ds((mask >> 1) * rows, rows)
        there = pl.ds(pl.multiple_of((share ^ mask) * rows, rows), rows)
        cosine, signed_sine = cosine_ref[there, :], sine_ref[there, :]

        def through_norm(gradient, raw, gain_vec):
            normed_grad = turn_back(gradient, cosine, signed_sine)
            unit_rows, inv_root = normalize(raw)
            gain_part = jnp.sum(normed_grad * unit_rows, axis=0, keepdims=True)
            return norm_back(normed_grad, unit_rows, inv_root, gain_vec).astype(BF16), gain_part

        for head in range(group):
            cols = pl.ds(head * head_size, head_size)
            sent, gain_part = through_norm(
                query_grad_ref[there, cols], query_ref[side, here, cols], query_gain_ref[...]
            )
            offset = pl.multiple_of((kv_head * group + head) * head_size, head_size)
            send_ref[side, here, pl.ds(offset, head_size)] = sent
            gain_ref[0:1, :] += gain_part
        sent, gain_part = through_norm(
            key_grad_ref[there, :], key_ref[side, here, :], key_gain_ref[...]
        )
        offset = pl.multiple_of(key_base + kv_head * head_size, head_size)
        send_ref[side, here, pl.ds(offset, head_size)] = sent
        gain_ref[1:2, :] += gain_part
        offset = pl.multiple_of(value_base + kv_head * head_size, head_size)
        send_ref[side, here, pl.ds(offset, head_size)] = value_grad_ref[there, :].astype(BF16)
        offset = pl.multiple_of(gate_base + kv_head * group * head_size, head_size)
        send_ref[side, here, pl.ds(offset, group * head_size)] = gate_grad_ref[side, here, :]


def head_specs(slots, group, kv_heads, head_size):
    half = slots // 2
    wide = group * head_size

    def piece(width, base):
        return pl.BlockSpec((2, None, half, width), lambda s, c: (0, s, 0, base + c))

    def ordered(width):
        return pl.BlockSpec((None, slots, width), lambda s, c: (s, 0, c))

    raw = [piece(wide, 0), piece(head_size, kv_heads * group)]
    value = piece(head_size, kv_heads * (group + 1))
    gain = pl.BlockSpec((1, head_size), lambda s, c: (0, 0))
    table = pl.BlockSpec((slots, head_size), lambda s, c: (0, 0))
    scalar = pl.BlockSpec(memory_space=pltpu.SMEM)
    return raw, value, ordered(wide), ordered(head_size), gain, table, scalar


def attend_forward(qkv_raw, share, lengths, gains, tables, masks, sizes):
    kv_heads, group, head_size = sizes
    slots = qkv_raw.shape[0] // 2
    raw, value, wide, narrow, gain, table, scalar = head_specs(slots, group, kv_heads, head_size)
    split = qkv_raw.reshape(2, 2, slots // 2, qkv_raw.shape[1])
    width, key_width = kv_heads * group * head_size, kv_heads * head_size
    attended, *kept = pl.pallas_call(
        functools.partial(attend_forward_kernel, masks, head_size, head_size ** (-0.5)),
        grid=(2, kv_heads),
        in_specs=[scalar, scalar, *raw, value, gain, gain, table, table],
        out_specs=[raw[0], wide, wide, narrow, narrow],
        out_shape=[
            jax.ShapeDtypeStruct((2, 2, slots // 2, width), F32),
            jax.ShapeDtypeStruct((2, slots, width), F32),
            jax.ShapeDtypeStruct((2, slots, width), BF16),
            jax.ShapeDtypeStruct((2, slots, key_width), BF16),
            jax.ShapeDtypeStruct((2, slots, key_width), BF16),
        ],
        cost_estimate=light_cost(),
        name="attend_forward",
    )(share, lengths, split, split, split, *gains, *tables)
    return attended.reshape(2 * slots, width), kept


def attend_backward(grads, gate_grads, qkv_raw, kept, share, lengths, gains, tables, masks, sizes):
    kv_heads, group, head_size = sizes
    slots = qkv_raw.shape[0] // 2
    raw, value, wide, narrow, gain, table, scalar = head_specs(slots, group, kv_heads, head_size)
    split = qkv_raw.reshape(2, 2, slots // 2, qkv_raw.shape[1])
    log_total, query_rot, key_rot, value_low = kept
    width = qkv_raw.shape[1] + gate_grads.shape[1]
    sent, gain_parts = pl.pallas_call(
        functools.partial(attend_backward_kernel, masks, head_size, head_size ** (-0.5)),
        grid=(2, kv_heads),
        in_specs=[scalar, scalar, raw[0], raw[0], *raw, wide, narrow, narrow, wide]
        + [gain, gain, table, table],
        out_specs=[
            pl.BlockSpec((2, None, slots // 2, width), lambda s, c: (0, s, 0, 0)),
            pl.BlockSpec((8, head_size), lambda s, c: (0, 0)),
        ],
        out_shape=[
            jax.ShapeDtypeStruct((2, 2, slots // 2, width), BF16),
            jax.ShapeDtypeStruct((8, head_size), F32),
        ],
        scratch_shapes=[
            pltpu.VMEM((slots, group * head_size), F32),
            pltpu.VMEM((slots, head_size), F32),
            pltpu.VMEM((slots, head_size), F32),
        ],
        cost_estimate=light_cost(),
        name="attend_backward",
    )(
        share,
        lengths,
        grads.reshape(2, 2, slots // 2, grads.shape[1]),
        gate_grads.reshape(2, 2, slots // 2, grads.shape[1]),
        split,
        split,
        query_rot,
        key_rot,
        value_low,
        log_total,
        *gains,
        *tables,
    )
    return sent.reshape(2 * slots, width), gain_parts


def body(
    members,
    shares,
    hidden_in,
    lengths,
    attn_gain,
    query_weight,
    key_weight,
    value_weight,
    output_gate,
    query_gain,
    key_gain,
    out_weight,
    mlp_gain,
    gate_weight,
    up_weight,
    down_weight,
    cotangent,
):
    odd = lax.axis_index("fsdp") % 2 == 1
    share = lax.axis_index("tensor")
    local_rows = hidden_in.shape[0]
    head_size = query_gain.shape[0]
    query_width = query_weight.shape[1] // 2
    key_width = key_weight.shape[1] // 2
    sizes = (key_width // head_size, query_width // key_width, head_size)
    masks = row_masks(shares)
    slots = share * local_rows + jnp.arange(local_rows)
    valid_rows = (slots < lengths[0]).astype(F32)[:, None]
    share_at = share.astype(jnp.int32)[None]
    both_lengths = jnp.concatenate([lengths, to_partner(lengths, members)])
    gains = (query_gain[None, :], key_gain[None, :])
    half_rows = local_rows * shares

    def gather_rows(values, *before):
        return rows_in(values, members, shares, *before)

    def sum_rows(parts, first, last):
        opened = open_sum(parts, members, shares, *first)
        return close_sum(*opened, members, shares, *last)

    def in_parts(function):
        corner = function(slice(2 * half_rows - local_rows, 2 * half_rows)).astype(BF16)
        far = function(slice(half_rows, 2 * half_rows - local_rows)).astype(BF16)
        near = function(slice(0, half_rows)).astype(BF16)
        return near, far, corner

    qkv_rows = pair_rows([query_weight, key_weight, value_weight], odd, members)
    qkv_full = gather_line(qkv_rows, members)
    gate_out_rows = pair_rows([output_gate, out_weight.T], odd, members)
    gate_out_full = gather_line(hold(gate_out_rows, qkv_rows), members)

    residual = hidden_in.astype(F32)
    unit_one, root_one = normalize(residual)
    gate_rows = pair_rows([hold(gate_weight, gate_out_rows)], odd, members)
    normed_one = gather_rows(hold((unit_one * attn_gain).astype(BF16), gate_rows))
    qkv_raw = matmul(normed_one, qkv_full)
    grad_rows = cotangent.astype(F32) * valid_rows
    tables = rope_tables(half_rows, head_size)
    attended, kept = attend_forward(
        qkv_raw, share_at, both_lengths, gains, tables, masks, sizes
    )
    up_in, down_in = hold((up_weight, down_weight), normed_one)
    up_rows = pair_rows([up_in], odd, members, attended)
    down_rows = pair_rows([down_in.T], odd, members, attended)
    gate_weights = gather_line(hold(gate_rows, qkv_full), members)
    up_weights = gather_line(hold(up_rows, gate_out_full), members)
    down_weights = gather_line(hold(down_rows, gate_weights), members)
    gate_full, out_full = gate_out_full[:, :query_width], gate_out_full[:, query_width:]
    gate_pre = matmul(hold(normed_one, attended, up_rows, down_rows), gate_full)
    gate_sig = jax.nn.sigmoid(gate_pre)
    gated_out = (attended * gate_sig).astype(BF16)
    attn_parts = in_parts(lambda rows: matmul_nt(gated_out[rows], out_full))
    middle = residual + sum_rows(attn_parts, (), ())
    unit_two, root_two = normalize(middle)
    normed_two = gather_rows((unit_two * mlp_gain).astype(BF16))
    one_weights = jnp.concatenate([qkv_full, gate_full], axis=1)
    ffn_gate = matmul(normed_two, gate_weights)
    branch_full = gather_rows(hold(grad_rows.astype(BF16), normed_two), ffn_gate, one_weights)
    ffn_up = matmul(normed_two, up_weights)
    ffn_sig = jax.nn.sigmoid(ffn_gate)
    ffn_act = ffn_gate * ffn_sig
    ffn_mid = (ffn_act * ffn_up).astype(BF16)

    down_part = matmul_tn(branch_full, ffn_mid).astype(BF16)
    down_sum = scatter_line(down_part, members)

    mid_grad = matmul(branch_full, hold(down_weights, down_part))
    gate_grad = (mid_grad * ffn_up * ffn_sig * (1.0 + ffn_gate * (1.0 - ffn_sig))).astype(BF16)
    up_grad = (mid_grad * ffn_act).astype(BF16)
    back_parts = in_parts(
        lambda rows: matmul_nt(gate_grad[rows], gate_weights)
        + matmul_nt(up_grad[rows], up_weights)
    )
    gate_part = matmul_tn(normed_two, hold(gate_grad, back_parts)).astype(BF16)
    gate_sum = scatter_line(gate_part, members)
    up_part = matmul_tn(normed_two, hold(up_grad, gate_part)).astype(BF16)
    up_sum = scatter_line(up_part, members)
    norm_two_grad = sum_rows(back_parts, (gate_part,), (down_sum, up_part))

    mlp_gain_part = jnp.sum(norm_two_grad * unit_two, axis=0)
    middle_grad = grad_rows + norm_back(norm_two_grad, unit_two, root_two, mlp_gain)
    mid_late = hold(ffn_mid, norm_two_grad)
    branch_parts = in_parts(lambda rows: matmul_nt(mid_late[rows], down_weights))
    attn_full_grad = gather_rows(middle_grad.astype(BF16), None, branch_parts, gate_sum)
    down_swap = swap_rows(hold(down_sum, attn_full_grad), odd, members)
    gate_swap = swap_rows(hold(gate_sum, attn_full_grad), odd, members)

    gated_grad = matmul(attn_full_grad, out_full)
    attended_grad = (gated_grad * gate_sig).astype(BF16)
    gate_pre_grad = (gated_grad * attended * gate_sig * (1.0 - gate_sig)).astype(BF16)
    gate_out_part = jnp.concatenate(
        [
            matmul_tn(normed_one, gate_pre_grad).astype(BF16),
            matmul_tn(attn_full_grad, gated_out).astype(BF16),
        ],
        axis=1,
    )
    gate_out_sum = scatter_line(gate_out_part, members)
    corners, opened = open_sum(hold(branch_parts, attn_full_grad), members, shares)
    one_send, gain_parts = attend_backward(
        hold(attended_grad, gate_out_part, down_swap, gate_swap),
        gate_pre_grad,
        qkv_raw,
        kept,
        share_at,
        both_lengths,
        gains,
        tables,
        masks,
        sizes,
    )
    ffn_branch = close_sum(corners, opened, members, shares, one_send)
    output = ((middle + ffn_branch) * valid_rows).astype(BF16)
    units = up_sum.shape[1]
    (down_shard,) = own_shard(*down_swap, odd, (units,))
    (gate_shard,) = own_shard(*gate_swap, odd, (units,))
    one_parts = in_parts(lambda rows: matmul_nt(one_send[rows], one_weights))
    qkv_send = hold(one_send, up_sum, one_parts)[:, : qkv_raw.shape[1]]
    qkv_part = matmul_tn(normed_one, qkv_send).astype(BF16)
    qkv_sum = scatter_line(qkv_part, members)
    norm_one_grad = sum_rows(one_parts, (qkv_part, ffn_branch), (gate_out_sum, output, down_shard, gate_shard))
    attn_gain_part = jnp.sum(norm_one_grad * unit_one, axis=0)
    grad_hidden = middle_grad + norm_back(norm_one_grad, unit_one, root_one, attn_gain)
    gain_totals = sum_everywhere(
        jnp.concatenate([attn_gain_part, mlp_gain_part, gain_parts[0], gain_parts[1]]),
        (("tensor", shares), ("fsdp", members)),
    )
    up_swap = swap_rows(hold(up_sum, norm_one_grad), odd, members)
    gate_out_swap = swap_rows(hold(gate_out_sum, norm_one_grad), odd, members)
    (up_shard,) = own_shard(*up_swap, odd, (units,))
    gate_attn_shard, out_shard = own_shard(*gate_out_swap, odd, (query_width,) * 2)
    qkv_sum = hold(
        qkv_sum,
        norm_one_grad,
        output,
        down_shard,
        gate_shard,
        up_shard,
        gate_attn_shard,
        out_shard,
    )
    query_shard, key_shard, value_shard = own_shard(
        *swap_rows(qkv_sum, odd, members), odd, (query_width, key_width, key_width)
    )
    width = hidden_in.shape[1]
    return (
        output,
        grad_hidden,
        gain_totals[:width],
        query_shard,
        key_shard,
        value_shard,
        gate_attn_shard,
        gain_totals[2 * width : 2 * width + head_size],
        gain_totals[2 * width + head_size :],
        out_shard.T,
        gain_totals[width : 2 * width],
        gate_shard,
        up_shard,
        down_shard.T,
    )


def solution(mesh):
    members, shares = mesh.shape["fsdp"], mesh.shape["tensor"]

    def layer(*operands):
        return body(members, shares, *operands)

    tokens = P(("fsdp", "tensor"), None)
    return jax.shard_map(
        layer,
        mesh=mesh,
        in_specs=(
            tokens,
            P("fsdp"),
            P(),
            P("fsdp", "tensor"),
            P("fsdp", "tensor"),
            P("fsdp", "tensor"),
            P("fsdp", "tensor"),
            P(),
            P(),
            P("tensor", "fsdp"),
            P(),
            P("fsdp", "tensor"),
            P("fsdp", "tensor"),
            P("tensor", "fsdp"),
            tokens,
        ),
        out_specs=(
            tokens,
            tokens,
            P(),
            P("fsdp", "tensor"),
            P("fsdp", "tensor"),
            P("fsdp", "tensor"),
            P("fsdp", "tensor"),
            P(),
            P(),
            P("tensor", "fsdp"),
            P(),
            P("fsdp", "tensor"),
            P("fsdp", "tensor"),
            P("tensor", "fsdp"),
        ),
        check_vma=False,
    )
```

```python
import functools

import jax
import jax.numpy as jnp
from jax import lax
from jax.experimental import pallas as pl
from jax.experimental.pallas import tpu as pltpu
from jax.sharding import PartitionSpec as P

NORM_EPSILON = 1e-06
ROPE_THETA = 1000000.0
MASKED_LOGIT = -1e30
F32 = jnp.float32
BF16 = jnp.bfloat16


def exchange(values, axis, size, mask):
    return lax.ppermute(values, axis, [(i, i ^ mask) for i in range(size)])


def lines(count):
    return [list(range(0, count, 2)), list(range(1, count, 2))]


def to_partner(values, count):
    return exchange(values, "fsdp", count, 1)


def halves(values, odd):
    width = values.shape[-1] // 2
    left, right = values[..., :width], values[..., width:]
    return jnp.where(odd, right, left), jnp.where(odd, left, right)


def in_order(own, other, odd, axis):
    first, second = jnp.where(odd, other, own), jnp.where(odd, own, other)
    return jnp.concatenate([first, second], axis=axis)


def pair_rows(shards, odd, count, *before):
    split = [halves(shard, odd) for shard in shards]
    own = jnp.concatenate([piece[0] for piece in split], axis=1)
    other = jnp.concatenate([piece[1] for piece in split], axis=1)
    arrived = to_partner(other, count)
    if before:
        arrived = hold(arrived, *before)
    return in_order(own, arrived, odd, 0)


def gather_line(rows, count):
    return lax.all_gather(rows, "fsdp", axis=0, tiled=True, axis_index_groups=lines(count))


def scatter_line(total, count):
    return lax.psum_scatter(
        total, "fsdp", scatter_dimension=0, tiled=True, axis_index_groups=lines(count)
    )


def swap_rows(rows, odd, count):
    height = rows.shape[0] // 2
    top, bottom = rows[:height], rows[height:]
    return jnp.where(odd, bottom, top), to_partner(jnp.where(odd, top, bottom), count)


def own_shard(own, other, odd, widths):
    shards, start = [], 0
    for width in widths:
        piece = slice(start, start + width)
        shards.append(in_order(own[:, piece], other[:, piece], odd, 1).astype(F32))
        start += width
    return shards


def dot_rows(first, second):
    return jnp.sum(first.astype(F32) * second.astype(F32), axis=1)


def hold(value, *others):
    return lax.optimization_barrier((value,) + others)[0]


def row_masks(count):
    half = count // 2
    return [((p % half) << 1) | (p // half) for p in range(count)]


def across(values, count):
    return exchange(values, "tensor", count, 2)


def core(values, count):
    return exchange(values, "tensor", count, 1)


def rows_in(values, members, shares, *before):
    half = values.shape[0] // 2
    side = across(values, shares)
    partner = to_partner(values, members)
    if before and before[0] is not None:
        side, partner = hold((side, partner), before[0])
    upper = to_partner(side[:half], members)
    lower = across(partner[half:], shares)
    if before[1:]:
        upper, lower = hold((upper, lower), *before[1:])
    near = [values, side, partner, upper, lower]
    return stack_rows(near + [core(piece, shares) for piece in near])


def stack_kernel(count, *refs):
    pieces, out, held, in_sems, out_sems = refs[:count], *refs[count:]
    incoming, outgoing, start = [], [], 0
    for i, piece in enumerate(pieces):
        place = pl.ds(start, piece.shape[0])
        incoming.append(pltpu.make_async_copy(piece, held.at[place], in_sems.at[i]))
        outgoing.append(pltpu.make_async_copy(held.at[place], out.at[place], out_sems.at[i]))
        incoming[-1].start()
        start += piece.shape[0]
    for arrive, leave in zip(incoming, outgoing):
        arrive.wait()
        leave.start()
    for leave in outgoing:
        leave.wait()


def stack_rows(pieces):
    count, (_, width), kind = len(pieces), pieces[0].shape, pieces[0].dtype
    rows = sum(piece.shape[0] for piece in pieces)
    anywhere = pl.BlockSpec(memory_space=pl.ANY)
    return pl.pallas_call(
        functools.partial(stack_kernel, count),
        in_specs=[anywhere] * count,
        out_specs=anywhere,
        out_shape=jax.ShapeDtypeStruct((rows, width), kind),
        scratch_shapes=[
            pltpu.VMEM((rows, width), kind),
            pltpu.SemaphoreType.DMA((count,)),
            pltpu.SemaphoreType.DMA((count,)),
        ],
        compiler_params=pltpu.CompilerParams(vmem_limit_bytes=(rows * width * 2) + (1 << 20)),
        cost_estimate=light_cost(),
        name="stack_rows",
    )(*pieces)


def light_cost():
    return pl.CostEstimate(flops=1024, bytes_accessed=1024, transcendentals=0)


def corner_kernel(near_ref, arrived_ref, upper_ref, lower_ref):
    half = upper_ref.shape[0]
    total = (near_ref[...].astype(F32) + arrived_ref[...].astype(F32)).astype(BF16)
    upper_ref[...] = total[:half]
    lower_ref[...] = total[half:]


def add_corner(near, arrived):
    rows, width = arrived.shape
    tile = width // 2
    half = pl.BlockSpec((rows // 2, tile), lambda i: (0, i))
    return pl.pallas_call(
        corner_kernel,
        grid=(2,),
        in_specs=[
            pl.BlockSpec((rows, tile), lambda i: (3, i)),
            pl.BlockSpec((rows, tile), lambda i: (0, i)),
        ],
        out_specs=[half, half],
        out_shape=[jax.ShapeDtypeStruct((rows // 2, width), BF16)] * 2,
        compiler_params=pltpu.CompilerParams(vmem_limit_bytes=16 << 20),
        cost_estimate=light_cost(),
        name="add_corner",
    )(near, arrived)


def main_kernel(near_ref, arrived_ref, own_ref, side_a, side_b, partner_a, partner_b):
    rows = own_ref.shape[0]
    half = rows // 2

    def total(start, size):
        piece = pl.ds(start, size)
        return near_ref[piece, :].astype(F32) + arrived_ref[piece, :].astype(F32)

    own_ref[...] = total(0, rows)
    side_a[...] = total(rows, half).astype(BF16)
    side_b[...] = total(rows + half, half)
    partner_a[...] = total(2 * rows, half)
    partner_b[...] = total(2 * rows + half, half).astype(BF16)


def add_main(near, arrived):
    rows, width = arrived.shape[0] // 3, arrived.shape[1]
    tile = width // 4
    whole = pl.BlockSpec((rows, tile), lambda i: (0, i))
    half = pl.BlockSpec((rows // 2, tile), lambda i: (0, i))
    three = pl.BlockSpec((3 * rows, tile), lambda i: (0, i))

    def shape(kind):
        return jax.ShapeDtypeStruct((rows // 2, width), kind)

    return pl.pallas_call(
        main_kernel,
        grid=(4,),
        in_specs=[three, three],
        out_specs=[whole, half, half, half, half],
        out_shape=[
            jax.ShapeDtypeStruct((rows, width), F32),
            shape(BF16),
            shape(F32),
            shape(F32),
            shape(BF16),
        ],
        compiler_params=pltpu.CompilerParams(vmem_limit_bytes=24 << 20),
        cost_estimate=light_cost(),
        name="add_main",
    )(near, arrived)


def open_sum(parts, members, shares, *before):
    near, far, far_corner = parts
    arrived_corner, arrived = core(far_corner, shares), core(far, shares)
    if before:
        arrived_corner, arrived = hold((arrived_corner, arrived), *before)
    return add_corner(near, arrived_corner), add_main(near, arrived)


def send_sum(added, members, shares):
    (upper, lower), (own, side_a, side_b, partner_a, partner_b) = added
    corners = across(upper, shares), to_partner(lower, members)
    return corners, (own, side_b, partner_a, across(side_a, shares), to_partner(partner_b, members))


def close_sum(corners, opened, members, shares, *before):
    corner_side, corner_partner = corners
    own, side, partner, side_first, partner_first = opened
    side_second = across((side + corner_partner.astype(F32)).astype(BF16), shares)
    partner_second = to_partner((partner + corner_side.astype(F32)).astype(BF16), members)
    if before:
        side_second, partner_second = hold((side_second, partner_second), *before)
    from_side = jnp.concatenate([side_first, side_second], axis=0).astype(F32)
    from_partner = jnp.concatenate([partner_second, partner_first], axis=0).astype(F32)
    return own + from_side + from_partner


def sum_everywhere(values, axis, mask, stop):
    count = lax.axis_size(axis)
    while mask < stop:
        values = values + exchange(values, axis, count, mask)
        mask <<= 1
    return values


def matmul(first_op, second_op):
    return jnp.dot(first_op, second_op, preferred_element_type=F32)


def matmul_tn(first_op, second_op):
    return lax.dot_general(
        first_op, second_op, (((0,), (0,)), ((), ())), preferred_element_type=F32
    )


def matmul_nt(first_op, second_op):
    return lax.dot_general(
        first_op, second_op, (((1,), (1,)), ((), ())), preferred_element_type=F32
    )


def normalize(values):
    inv_root = lax.rsqrt(jnp.mean(values * values, axis=-1, keepdims=True) + NORM_EPSILON)
    return (values * inv_root, inv_root)


def norm_back(gradient, unit_rows, inv_root, gain_vec):
    scaled = gradient * gain_vec
    return inv_root * (scaled - unit_rows * jnp.mean(scaled * unit_rows, axis=-1, keepdims=True))


def rope_tables(slot_count, head_size):
    half_width = head_size // 2
    inverse = ROPE_THETA ** (-(jnp.arange(half_width, dtype=F32) * 2.0 / head_size))
    angles = jnp.arange(slot_count, dtype=F32)[:, None] * inverse[None, :]
    cosine = jnp.concatenate([jnp.cos(angles), jnp.cos(angles)], axis=-1)
    signed_sine = jnp.concatenate([-jnp.sin(angles), jnp.sin(angles)], axis=-1)
    return (cosine, signed_sine)


def piece_of(mask, rows):
    return mask & 1, pl.ds(pl.multiple_of((mask >> 1) * rows, rows), rows)


def allowed_block(block, rows, width, length):
    row_slot = block * rows + lax.broadcasted_iota(jnp.int32, (rows, width), 0)
    col_slot = lax.broadcasted_iota(jnp.int32, (rows, width), 1)
    return (col_slot <= row_slot) & (col_slot < length)


def turn(unit_rows, gain_vec, cosine, signed_sine):
    normed = unit_rows * gain_vec
    half = normed.shape[-1] // 2
    return normed * cosine + pltpu.roll(normed, half, 1) * signed_sine


def turn_back(gradient, cosine, signed_sine):
    half = gradient.shape[-1] // 2
    return gradient * cosine - pltpu.roll(gradient, half, 1) * signed_sine


def attend_forward_kernel(
    masks,
    head_size,
    score_scale,
    share_ref,
    length_ref,
    query_ref,
    key_ref,
    value_ref,
    query_gain_ref,
    key_gain_ref,
    cosine_ref,
    sine_ref,
    attended_ref,
    log_ref,
    query_rot_ref,
    key_rot_ref,
    value_low_ref,
):
    blocks = len(masks)
    rows = 2 * query_ref.shape[1] // blocks
    group = query_ref.shape[2] // head_size
    share, length = share_ref[0], length_ref[pl.program_id(0)]
    for mask in masks:
        side, here = mask & 1, pl.ds((mask >> 1) * rows, rows)
        there = pl.ds(pl.multiple_of((share ^ mask) * rows, rows), rows)
        cosine, signed_sine = cosine_ref[there, :], sine_ref[there, :]
        for head in range(group):
            cols = pl.ds(head * head_size, head_size)
            unit_rows, _ = normalize(query_ref[side, here, cols])
            turned = turn(unit_rows, query_gain_ref[...], cosine, signed_sine)
            query_rot_ref[there, cols] = turned.astype(BF16)
        unit_rows, _ = normalize(key_ref[side, here, :])
        turned = turn(unit_rows, key_gain_ref[...], cosine, signed_sine)
        key_rot_ref[there, :] = turned.astype(BF16)
        value_low_ref[there, :] = value_ref[side, here, :].astype(BF16)

    for block in range(blocks):
        width = (block + 1) * rows
        here = pl.ds(block * rows, rows)
        allowed = allowed_block(block, rows, width, length)
        side, back = piece_of(share ^ block, rows)

        def one_head(head, carry, width=width, here=here, allowed=allowed, side=side, back=back):
            cols = pl.ds(pl.multiple_of(head * head_size, head_size), head_size)
            scores = matmul_nt(query_rot_ref[here, cols], key_rot_ref[:width, :])
            logits = jnp.where(allowed, scores * score_scale, MASKED_LOGIT)
            highest = jnp.max(logits, axis=-1, keepdims=True)
            weights_raw = jnp.exp(logits - highest)
            row_total = jnp.sum(weights_raw, axis=-1, keepdims=True)
            probabilities = (weights_raw * (1.0 / row_total)).astype(BF16)
            attended_ref[side, back, cols] = matmul(probabilities, value_low_ref[:width, :])
            log_ref[here, cols] = jnp.broadcast_to(highest + jnp.log(row_total), (rows, head_size))
            return carry

        lax.fori_loop(0, group, one_head, 0)


def attend_backward_kernel(
    masks,
    head_size,
    score_scale,
    share_ref,
    length_ref,
    grad_ref,
    gate_grad_ref,
    query_ref,
    key_ref,
    query_rot_ref,
    key_rot_ref,
    value_low_ref,
    log_ref,
    query_gain_ref,
    key_gain_ref,
    cosine_ref,
    sine_ref,
    send_ref,
    gain_ref,
    query_grad_ref,
    key_grad_ref,
    value_grad_ref,
):
    blocks = len(masks)
    rows = 2 * query_ref.shape[1] // blocks
    group = query_ref.shape[2] // head_size
    kv_heads = pl.num_programs(1)
    kv_head = pl.program_id(1)
    share, length = share_ref[0], length_ref[pl.program_id(0)]
    key_grad_ref[...] = jnp.zeros_like(key_grad_ref)
    value_grad_ref[...] = jnp.zeros_like(value_grad_ref)

    @pl.when((pl.program_id(0) == 0) & (kv_head == 0))
    def _():
        gain_ref[...] = jnp.zeros_like(gain_ref)

    for block in range(blocks):
        width = (block + 1) * rows
        here = pl.ds(block * rows, rows)
        allowed = allowed_block(block, rows, width, length)
        side, back = piece_of(share ^ block, rows)

        def one_head(head, carry, width=width, here=here, allowed=allowed, side=side, back=back):
            cols = pl.ds(pl.multiple_of(head * head_size, head_size), head_size)
            queries, grads = query_rot_ref[here, cols], grad_ref[side, back, cols]
            scores = matmul_nt(queries, key_rot_ref[:width, :])
            logits = jnp.where(allowed, scores * score_scale, MASKED_LOGIT)
            soft = jnp.where(allowed, jnp.exp(logits - log_ref[here, cols][:, :1]), 0.0)
            prob_grad = matmul_nt(grads, value_low_ref[:width, :])
            centre = jnp.sum(soft * prob_grad, axis=-1, keepdims=True)
            score_grad = (score_scale * soft * (prob_grad - centre)).astype(BF16)
            query_grad_ref[here, cols] = matmul(score_grad, key_rot_ref[:width, :])
            key_grad_ref[:width, :] += matmul_tn(score_grad, queries)
            value_grad_ref[:width, :] += matmul_tn(soft.astype(BF16), grads)
            return carry

        lax.fori_loop(0, group, one_head, 0)

    key_base, value_base = kv_heads * group * head_size, kv_heads * (group + 1) * head_size
    gate_base = kv_heads * (group + 2) * head_size
    for mask in masks:
        side, here = mask & 1, pl.ds((mask >> 1) * rows, rows)
        there = pl.ds(pl.multiple_of((share ^ mask) * rows, rows), rows)
        cosine, signed_sine = cosine_ref[there, :], sine_ref[there, :]

        def through_norm(gradient, raw, gain_vec):
            normed_grad = turn_back(gradient, cosine, signed_sine)
            unit_rows, inv_root = normalize(raw)
            gain_part = jnp.sum(normed_grad * unit_rows, axis=0, keepdims=True)
            return norm_back(normed_grad, unit_rows, inv_root, gain_vec).astype(BF16), gain_part

        for head in range(group):
            cols = pl.ds(head * head_size, head_size)
            sent, gain_part = through_norm(
                query_grad_ref[there, cols], query_ref[side, here, cols], query_gain_ref[...]
            )
            offset = pl.multiple_of((kv_head * group + head) * head_size, head_size)
            send_ref[side, here, pl.ds(offset, head_size)] = sent
            gain_ref[0:1, :] += gain_part
        sent, gain_part = through_norm(
            key_grad_ref[there, :], key_ref[side, here, :], key_gain_ref[...]
        )
        offset = pl.multiple_of(key_base + kv_head * head_size, head_size)
        send_ref[side, here, pl.ds(offset, head_size)] = sent
        gain_ref[1:2, :] += gain_part
        offset = pl.multiple_of(value_base + kv_head * head_size, head_size)
        send_ref[side, here, pl.ds(offset, head_size)] = value_grad_ref[there, :].astype(BF16)
        offset = pl.multiple_of(gate_base + kv_head * group * head_size, head_size)
        send_ref[side, here, pl.ds(offset, group * head_size)] = gate_grad_ref[side, here, :]


def units_kernel(rows_ref, gate_weights_ref, up_weights_ref, gate_ref, up_ref, mid_ref):
    rows = rows_ref[...]
    gate = matmul(rows, gate_weights_ref[...])
    gate_ref[...] = gate
    up = matmul(rows, up_weights_ref[...])
    up_ref[...] = up
    mid_ref[...] = (gate * jax.nn.sigmoid(gate) * up).astype(BF16)


def hidden_units(normed, gate_weights, up_weights):
    rows, width = normed.shape
    units = gate_weights.shape[1]
    tile = rows // 8
    tokens = pl.BlockSpec((tile, width), lambda i: (i, 0))
    hidden = pl.BlockSpec((tile, units), lambda i: (i, 0))
    weight = pl.BlockSpec((width, units), lambda i: (0, 0), pipeline_mode=pl.Buffered(1))
    return pl.pallas_call(
        units_kernel,
        grid=(8,),
        in_specs=[tokens, weight, weight],
        out_specs=[hidden, hidden, hidden],
        out_shape=[jax.ShapeDtypeStruct((rows, units), kind) for kind in (F32, F32, BF16)],
        compiler_params=pltpu.CompilerParams(vmem_limit_bytes=32 << 20),
        cost_estimate=light_cost(),
        name="hidden_units",
    )(normed, gate_weights, up_weights)


def unit_grads_kernel(
    near_steps,
    far_steps,
    branch_ref,
    gate_ref,
    up_ref,
    down_weights_ref,
    gate_weights_ref,
    up_weights_ref,
    gate_grad_ref,
    up_grad_ref,
    near_ref,
    far_ref,
    corner_ref,
):
    step = pl.program_id(0)
    mid_grad = matmul(branch_ref[...], down_weights_ref[...])
    gate, up = gate_ref[...], up_ref[...]
    sig = jax.nn.sigmoid(gate)
    gate_grad = (mid_grad * up * sig * (1.0 + gate * (1.0 - sig))).astype(BF16)
    up_grad = (mid_grad * (gate * sig)).astype(BF16)
    gate_grad_ref[...] = gate_grad
    up_grad_ref[...] = up_grad
    back = matmul_nt(gate_grad, gate_weights_ref[...]) + matmul_nt(up_grad, up_weights_ref[...])
    back = back.astype(BF16)

    @pl.when(step < near_steps)
    def _():
        near_ref[...] = back

    @pl.when((step >= near_steps) & (step < near_steps + far_steps))
    def _():
        far_ref[...] = back

    @pl.when(step == near_steps + far_steps)
    def _():
        corner_ref[...] = back


def unit_grads(branch, ffn_gate, ffn_up, down_weights, gate_weights, up_weights):
    rows, width = branch.shape
    units = ffn_gate.shape[1]
    tile = rows // 8
    tokens = pl.BlockSpec((tile, width), lambda i: (i, 0))
    hidden = pl.BlockSpec((tile, units), lambda i: (i, 0))
    weight = pl.BlockSpec((width, units), lambda i: (0, 0), pipeline_mode=pl.Buffered(1))
    gate_grad, up_grad, *parts = pl.pallas_call(
        functools.partial(unit_grads_kernel, 4, 3),
        grid=(8,),
        in_specs=[tokens, hidden, hidden, weight, weight, weight],
        out_specs=[
            hidden,
            hidden,
            pl.BlockSpec((tile, width), lambda i: (jnp.minimum(i, 3), 0)),
            pl.BlockSpec((tile, width), lambda i: (jnp.clip(i - 4, 0, 2), 0)),
            pl.BlockSpec((tile, width), lambda i: (0, 0)),
        ],
        out_shape=[
            jax.ShapeDtypeStruct((rows, units), BF16),
            jax.ShapeDtypeStruct((rows, units), BF16),
            jax.ShapeDtypeStruct((4 * tile, width), BF16),
            jax.ShapeDtypeStruct((3 * tile, width), BF16),
            jax.ShapeDtypeStruct((tile, width), BF16),
        ],
        compiler_params=pltpu.CompilerParams(vmem_limit_bytes=44 << 20),
        cost_estimate=light_cost(),
        name="unit_grads",
    )(branch, ffn_gate, ffn_up, down_weights, gate_weights, up_weights)
    return gate_grad, up_grad, parts


def head_specs(slots, group, kv_heads, head_size):
    half = slots // 2
    wide = group * head_size

    def piece(width, base):
        return pl.BlockSpec((2, None, half, width), lambda s, c: (0, s, 0, base + c))

    def ordered(width):
        return pl.BlockSpec((None, slots, width), lambda s, c: (s, 0, c))

    raw = [piece(wide, 0), piece(head_size, kv_heads * group)]
    value = piece(head_size, kv_heads * (group + 1))
    gain = pl.BlockSpec((1, head_size), lambda s, c: (0, 0))
    table = pl.BlockSpec((slots, head_size), lambda s, c: (0, 0))
    scalar = pl.BlockSpec(memory_space=pltpu.SMEM)
    return raw, value, ordered(wide), ordered(head_size), gain, table, scalar


def attend_forward(qkv_raw, share, lengths, gains, tables, masks, sizes):
    kv_heads, group, head_size = sizes
    slots = qkv_raw.shape[0] // 2
    raw, value, wide, narrow, gain, table, scalar = head_specs(slots, group, kv_heads, head_size)
    split = qkv_raw.reshape(2, 2, slots // 2, qkv_raw.shape[1])
    width, key_width = kv_heads * group * head_size, kv_heads * head_size
    attended, *kept = pl.pallas_call(
        functools.partial(attend_forward_kernel, masks, head_size, head_size ** (-0.5)),
        grid=(2, kv_heads),
        in_specs=[scalar, scalar, *raw, value, gain, gain, table, table],
        out_specs=[raw[0], wide, wide, narrow, narrow],
        out_shape=[
            jax.ShapeDtypeStruct((2, 2, slots // 2, width), F32),
            jax.ShapeDtypeStruct((2, slots, width), F32),
            jax.ShapeDtypeStruct((2, slots, width), BF16),
            jax.ShapeDtypeStruct((2, slots, key_width), BF16),
            jax.ShapeDtypeStruct((2, slots, key_width), BF16),
        ],
        cost_estimate=light_cost(),
        name="attend_forward",
    )(share, lengths, split, split, split, *gains, *tables)
    return attended.reshape(2 * slots, width), kept


def attend_backward(grads, gate_grads, qkv_raw, kept, share, lengths, gains, tables, masks, sizes):
    kv_heads, group, head_size = sizes
    slots = qkv_raw.shape[0] // 2
    raw, value, wide, narrow, gain, table, scalar = head_specs(slots, group, kv_heads, head_size)
    split = qkv_raw.reshape(2, 2, slots // 2, qkv_raw.shape[1])
    log_total, query_rot, key_rot, value_low = kept
    width = qkv_raw.shape[1] + gate_grads.shape[1]
    sent, gain_parts = pl.pallas_call(
        functools.partial(attend_backward_kernel, masks, head_size, head_size ** (-0.5)),
        grid=(2, kv_heads),
        in_specs=[scalar, scalar, raw[0], raw[0], *raw, wide, narrow, narrow, wide]
        + [gain, gain, table, table],
        out_specs=[
            pl.BlockSpec((2, None, slots // 2, width), lambda s, c: (0, s, 0, 0)),
            pl.BlockSpec((8, head_size), lambda s, c: (0, 0)),
        ],
        out_shape=[
            jax.ShapeDtypeStruct((2, 2, slots // 2, width), BF16),
            jax.ShapeDtypeStruct((8, head_size), F32),
        ],
        scratch_shapes=[
            pltpu.VMEM((slots, group * head_size), F32),
            pltpu.VMEM((slots, head_size), F32),
            pltpu.VMEM((slots, head_size), F32),
        ],
        cost_estimate=light_cost(),
        name="attend_backward",
    )(
        share,
        lengths,
        grads.reshape(2, 2, slots // 2, grads.shape[1]),
        gate_grads.reshape(2, 2, slots // 2, grads.shape[1]),
        split,
        split,
        query_rot,
        key_rot,
        value_low,
        log_total,
        *gains,
        *tables,
    )
    return sent.reshape(2 * slots, width), gain_parts


def body(
    members,
    shares,
    hidden_in,
    lengths,
    attn_gain,
    query_weight,
    key_weight,
    value_weight,
    output_gate,
    query_gain,
    key_gain,
    out_weight,
    mlp_gain,
    gate_weight,
    up_weight,
    down_weight,
    cotangent,
):
    odd = lax.axis_index("fsdp") % 2 == 1
    share = lax.axis_index("tensor")
    local_rows = hidden_in.shape[0]
    head_size = query_gain.shape[0]
    query_width = query_weight.shape[1] // 2
    key_width = key_weight.shape[1] // 2
    sizes = (key_width // head_size, query_width // key_width, head_size)
    masks = row_masks(shares)
    slots = share * local_rows + jnp.arange(local_rows)
    valid_rows = (slots < lengths[0]).astype(F32)[:, None]
    share_at = share.astype(jnp.int32)[None]
    both_lengths = jnp.concatenate([lengths, to_partner(lengths, members)])
    gains = (query_gain[None, :], key_gain[None, :])
    half_rows = local_rows * shares

    def gather_rows(values, *before):
        return rows_in(values, members, shares, *before)

    def sum_rows(parts, first, last):
        added = open_sum(parts, members, shares, *first)
        return close_sum(*send_sum(added, members, shares), members, shares, *last)

    def in_parts(function):
        corner = function(slice(2 * half_rows - local_rows, 2 * half_rows)).astype(BF16)
        far = function(slice(half_rows, 2 * half_rows - local_rows)).astype(BF16)
        near = function(slice(0, half_rows)).astype(BF16)
        return near, far, corner

    qkv_rows = pair_rows([query_weight, key_weight, value_weight], odd, members)
    qkv_full = gather_line(qkv_rows, members)
    gate_out_rows = pair_rows([output_gate, out_weight.T], odd, members)
    gate_out_full = gather_line(hold(gate_out_rows, qkv_rows), members)

    residual = hidden_in.astype(F32)
    unit_one, root_one = normalize(residual)
    gate_rows = pair_rows([hold(gate_weight, gate_out_rows)], odd, members)
    normed_one = gather_rows(hold((unit_one * attn_gain).astype(BF16), gate_rows))
    qkv_raw = matmul(normed_one, qkv_full)
    grad_rows = cotangent.astype(F32) * valid_rows
    tables = rope_tables(half_rows, head_size)
    attended, kept = attend_forward(
        qkv_raw, share_at, both_lengths, gains, tables, masks, sizes
    )
    up_in, down_in = hold((up_weight, down_weight), normed_one)
    up_rows = pair_rows([up_in], odd, members, attended)
    down_rows = pair_rows([down_in.T], odd, members, attended)
    gate_weights = gather_line(hold(gate_rows, qkv_full), members)
    up_weights = gather_line(hold(up_rows, gate_out_full), members)
    down_weights = gather_line(hold(down_rows, gate_weights), members)
    gate_full, out_full = gate_out_full[:, :query_width], gate_out_full[:, query_width:]
    gate_pre = matmul(hold(normed_one, attended, up_rows, down_rows), gate_full)
    gate_sig = jax.nn.sigmoid(gate_pre)
    gated_out = (attended * gate_sig).astype(BF16)
    attn_parts = in_parts(lambda rows: matmul_nt(gated_out[rows], out_full))
    middle = residual + sum_rows(attn_parts, (), (gate_weights,))
    unit_two, root_two = normalize(middle)
    normed_two = gather_rows((unit_two * mlp_gain).astype(BF16))
    one_weights = jnp.concatenate([qkv_full, gate_full], axis=1)
    ffn_gate, ffn_up, ffn_mid = hidden_units(normed_two, gate_weights, up_weights)
    branch_full = gather_rows(
        hold(grad_rows.astype(BF16), normed_two), None, one_weights, ffn_mid
    )

    down_part = matmul_tn(branch_full, ffn_mid).astype(BF16)
    down_sum = scatter_line(down_part, members)

    gate_grad, up_grad, back_parts = unit_grads(
        branch_full, ffn_gate, ffn_up, hold(down_weights, down_part), gate_weights, up_weights
    )
    gate_part = matmul_tn(normed_two, hold(gate_grad, back_parts)).astype(BF16)
    gate_sum = scatter_line(gate_part, members)
    up_part = matmul_tn(normed_two, hold(up_grad, gate_part)).astype(BF16)
    up_sum = scatter_line(up_part, members)
    norm_two_grad = sum_rows(back_parts, (gate_part,), (down_sum, up_part))

    mlp_gain_part = jnp.sum(norm_two_grad * unit_two, axis=0)
    middle_grad = grad_rows + norm_back(norm_two_grad, unit_two, root_two, mlp_gain)
    mid_late = hold(ffn_mid, norm_two_grad)
    branch_parts = in_parts(lambda rows: matmul_nt(mid_late[rows], down_weights))
    attn_full_grad = gather_rows(middle_grad.astype(BF16), None, branch_parts, gate_sum)
    branch_added = open_sum(branch_parts, members, shares)
    down_swap = swap_rows(hold(down_sum, attn_full_grad), odd, members)
    gate_swap = swap_rows(hold(gate_sum, attn_full_grad), odd, members)
    attn_full_grad = hold(attn_full_grad, branch_added)
    corners, opened = send_sum(hold(branch_added, attn_full_grad), members, shares)
    gated_grad = matmul(attn_full_grad, out_full)
    attended_grad = (gated_grad * gate_sig).astype(BF16)
    gate_pre_grad = (gated_grad * attended * gate_sig * (1.0 - gate_sig)).astype(BF16)
    gate_attn_part = matmul_tn(normed_one, gate_pre_grad).astype(BF16)
    gate_out_part = jnp.concatenate(
        [
            gate_attn_part,
            matmul_tn(attn_full_grad, gated_out).astype(BF16),
        ],
        axis=1,
    )
    gate_out_sum = scatter_line(gate_out_part, members)
    one_send, gain_parts = attend_backward(
        hold(attended_grad, gate_out_part),
        gate_pre_grad,
        qkv_raw,
        kept,
        share_at,
        both_lengths,
        gains,
        tables,
        masks,
        sizes,
    )
    one_send = hold(one_send, corners, opened, down_swap, gate_swap)
    ffn_branch = close_sum(corners, opened, members, shares, one_send)
    output = ((middle + ffn_branch) * valid_rows).astype(BF16)
    units = up_sum.shape[1]
    one_parts = in_parts(lambda rows: matmul_nt(one_send[rows], one_weights))
    qkv_send = hold(one_send, up_sum, one_parts)[:, : qkv_raw.shape[1]]
    qkv_part = matmul_tn(normed_one, qkv_send).astype(BF16)
    qkv_sum = scatter_line(qkv_part, members)
    attn_gain_part = (
        dot_rows(qkv_part, qkv_full) + dot_rows(gate_attn_part, gate_full)
    ) / attn_gain
    up_swap = swap_rows(hold(up_sum, one_send), odd, members)
    added_one = open_sum(one_parts, members, shares, qkv_part, ffn_branch)
    gain_parts = hold(
        jnp.concatenate([attn_gain_part, mlp_gain_part, gain_parts[0], gain_parts[1]]), added_one
    )
    gain_parts = sum_everywhere(gain_parts, "fsdp", 2, members)
    gain_parts = sum_everywhere(gain_parts, "tensor", 1, 2)
    norm_one_grad = close_sum(
        *send_sum(added_one, members, shares), members, shares, gate_out_sum, gain_parts, up_swap
    )
    gain_totals = hold(gain_parts, norm_one_grad)
    gain_totals = sum_everywhere(gain_totals, "tensor", 2, shares)
    gain_totals = sum_everywhere(gain_totals, "fsdp", 1, 2)
    grad_hidden = middle_grad + norm_back(norm_one_grad, unit_one, root_one, attn_gain)
    (down_shard,) = own_shard(*down_swap, odd, (units,))
    (gate_shard,) = own_shard(*gate_swap, odd, (units,))
    gate_out_swap = swap_rows(hold(gate_out_sum, norm_one_grad, qkv_sum), odd, members)
    (up_shard,) = own_shard(*up_swap, odd, (units,))
    gate_attn_shard, out_shard = own_shard(*gate_out_swap, odd, (query_width,) * 2)
    qkv_sum = hold(
        qkv_sum,
        norm_one_grad,
        gain_totals,
        output,
        down_shard,
        gate_shard,
        up_shard,
        gate_attn_shard,
        out_shard,
    )
    query_shard, key_shard, value_shard = own_shard(
        *swap_rows(qkv_sum, odd, members), odd, (query_width, key_width, key_width)
    )
    width = hidden_in.shape[1]
    return (
        output,
        grad_hidden,
        gain_totals[:width],
        query_shard,
        key_shard,
        value_shard,
        gate_attn_shard,
        gain_totals[2 * width : 2 * width + head_size],
        gain_totals[2 * width + head_size :],
        out_shard.T,
        gain_totals[width : 2 * width],
        gate_shard,
        up_shard,
        down_shard.T,
    )


def solution(mesh):
    members, shares = mesh.shape["fsdp"], mesh.shape["tensor"]

    def layer(*operands):
        return body(members, shares, *operands)

    tokens = P(("fsdp", "tensor"), None)
    return jax.shard_map(
        layer,
        mesh=mesh,
        in_specs=(
            tokens,
            P("fsdp"),
            P(),
            P("fsdp", "tensor"),
            P("fsdp", "tensor"),
            P("fsdp", "tensor"),
            P("fsdp", "tensor"),
            P(),
            P(),
            P("tensor", "fsdp"),
            P(),
            P("fsdp", "tensor"),
            P("fsdp", "tensor"),
            P("tensor", "fsdp"),
            tokens,
        ),
        out_specs=(
            tokens,
            tokens,
            P(),
            P("fsdp", "tensor"),
            P("fsdp", "tensor"),
            P("fsdp", "tensor"),
            P("fsdp", "tensor"),
            P(),
            P(),
            P("tensor", "fsdp"),
            P(),
            P("fsdp", "tensor"),
            P("fsdp", "tensor"),
            P("tensor", "fsdp"),
        ),
        check_vma=False,
    )
```

```python
import functools

import jax
import jax.numpy as jnp
from jax import lax
from jax.experimental import pallas as pl
from jax.experimental.pallas import tpu as pltpu
from jax.sharding import PartitionSpec as P

NORM_EPSILON = 1e-06
ROPE_THETA = 1000000.0
MASKED_LOGIT = -1e30
F32 = jnp.float32
BF16 = jnp.bfloat16


def exchange(values, axis, size, mask):
    return lax.ppermute(values, axis, [(i, i ^ mask) for i in range(size)])


def lines(count):
    return [list(range(0, count, 2)), list(range(1, count, 2))]


def to_partner(values, count):
    return exchange(values, "fsdp", count, 1)


def halves(values, odd):
    width = values.shape[-1] // 2
    left, right = values[..., :width], values[..., width:]
    return jnp.where(odd, right, left), jnp.where(odd, left, right)


def in_order(own, other, odd, axis):
    first, second = jnp.where(odd, other, own), jnp.where(odd, own, other)
    return jnp.concatenate([first, second], axis=axis)


def pair_rows(shards, odd, count, *before):
    split = [halves(shard, odd) for shard in shards]
    own = jnp.concatenate([piece[0] for piece in split], axis=1)
    other = jnp.concatenate([piece[1] for piece in split], axis=1)
    arrived = to_partner(other, count)
    if before:
        arrived = hold(arrived, *before)
    return in_order(own, arrived, odd, 0)


def gather_line(rows, count):
    return lax.all_gather(rows, "fsdp", axis=0, tiled=True, axis_index_groups=lines(count))


def scatter_line(total, count):
    return lax.psum_scatter(
        total, "fsdp", scatter_dimension=0, tiled=True, axis_index_groups=lines(count)
    )


def swap_rows(rows, odd, count):
    height = rows.shape[0] // 2
    top, bottom = rows[:height], rows[height:]
    return jnp.where(odd, bottom, top), to_partner(jnp.where(odd, top, bottom), count)


def own_shard(own, other, odd, widths):
    shards, start = [], 0
    for width in widths:
        piece = slice(start, start + width)
        shards.append(in_order(own[:, piece], other[:, piece], odd, 1).astype(F32))
        start += width
    return shards


def dot_rows(first, second):
    return jnp.sum(first.astype(F32) * second.astype(F32), axis=1)


def hold(value, *others):
    return lax.optimization_barrier((value,) + others)[0]


def row_masks(count):
    half = count // 2
    return [((p % half) << 1) | (p // half) for p in range(count)]


def across(values, count):
    return exchange(values, "tensor", count, 2)


def core(values, count):
    return exchange(values, "tensor", count, 1)


def rows_in(values, members, shares, *before):
    half = values.shape[0] // 2
    side = across(values, shares)
    partner = to_partner(values, members)
    if before and before[0] is not None:
        side, partner = hold((side, partner), before[0])
    upper = to_partner(side[:half], members)
    lower = across(partner[half:], shares)
    if before[1:]:
        upper, lower = hold((upper, lower), *before[1:])
    near = [values, side, partner, upper, lower]
    return stack_rows(near + [core(piece, shares) for piece in near])


def stack_kernel(count, *refs):
    pieces, out, held, in_sems, out_sems = refs[:count], *refs[count:]
    incoming, outgoing, start = [], [], 0
    for i, piece in enumerate(pieces):
        place = pl.ds(start, piece.shape[0])
        incoming.append(pltpu.make_async_copy(piece, held.at[place], in_sems.at[i]))
        outgoing.append(pltpu.make_async_copy(held.at[place], out.at[place], out_sems.at[i]))
        incoming[-1].start()
        start += piece.shape[0]
    for arrive, leave in zip(incoming, outgoing):
        arrive.wait()
        leave.start()
    for leave in outgoing:
        leave.wait()


def stack_rows(pieces):
    count, (_, width), kind = len(pieces), pieces[0].shape, pieces[0].dtype
    rows = sum(piece.shape[0] for piece in pieces)
    anywhere = pl.BlockSpec(memory_space=pl.ANY)
    return pl.pallas_call(
        functools.partial(stack_kernel, count),
        in_specs=[anywhere] * count,
        out_specs=anywhere,
        out_shape=jax.ShapeDtypeStruct((rows, width), kind),
        scratch_shapes=[
            pltpu.VMEM((rows, width), kind),
            pltpu.SemaphoreType.DMA((count,)),
            pltpu.SemaphoreType.DMA((count,)),
        ],
        compiler_params=pltpu.CompilerParams(vmem_limit_bytes=(rows * width * 2) + (1 << 20)),
        cost_estimate=light_cost(),
        name="stack_rows",
    )(*pieces)


def light_cost():
    return pl.CostEstimate(flops=1024, bytes_accessed=1024, transcendentals=0)


def corner_kernel(near_ref, arrived_ref, upper_ref, lower_ref):
    half = upper_ref.shape[0]
    total = (near_ref[...].astype(F32) + arrived_ref[...].astype(F32)).astype(BF16)
    upper_ref[...] = total[:half]
    lower_ref[...] = total[half:]


def add_corner(near, arrived):
    rows, width = arrived.shape
    tile = width // 2
    half = pl.BlockSpec((rows // 2, tile), lambda i: (0, i))
    return pl.pallas_call(
        corner_kernel,
        grid=(2,),
        in_specs=[
            pl.BlockSpec((rows, tile), lambda i: (3, i)),
            pl.BlockSpec((rows, tile), lambda i: (0, i)),
        ],
        out_specs=[half, half],
        out_shape=[jax.ShapeDtypeStruct((rows // 2, width), BF16)] * 2,
        compiler_params=pltpu.CompilerParams(vmem_limit_bytes=16 << 20),
        cost_estimate=light_cost(),
        name="add_corner",
    )(near, arrived)


def main_kernel(near_ref, arrived_ref, own_ref, side_a, side_b, partner_a, partner_b):
    rows = own_ref.shape[0]
    half = rows // 2

    def total(start, size):
        piece = pl.ds(start, size)
        return near_ref[piece, :].astype(F32) + arrived_ref[piece, :].astype(F32)

    own_ref[...] = total(0, rows)
    side_a[...] = total(rows, half).astype(BF16)
    side_b[...] = total(rows + half, half)
    partner_a[...] = total(2 * rows, half)
    partner_b[...] = total(2 * rows + half, half).astype(BF16)


def add_main(near, arrived):
    rows, width = arrived.shape[0] // 3, arrived.shape[1]
    tile = width // 4
    whole = pl.BlockSpec((rows, tile), lambda i: (0, i))
    half = pl.BlockSpec((rows // 2, tile), lambda i: (0, i))
    three = pl.BlockSpec((3 * rows, tile), lambda i: (0, i))

    def shape(kind):
        return jax.ShapeDtypeStruct((rows // 2, width), kind)

    return pl.pallas_call(
        main_kernel,
        grid=(4,),
        in_specs=[three, three],
        out_specs=[whole, half, half, half, half],
        out_shape=[
            jax.ShapeDtypeStruct((rows, width), F32),
            shape(BF16),
            shape(F32),
            shape(F32),
            shape(BF16),
        ],
        compiler_params=pltpu.CompilerParams(vmem_limit_bytes=24 << 20),
        cost_estimate=light_cost(),
        name="add_main",
    )(near, arrived)


def open_sum(parts, members, shares, *before):
    near, far, far_corner = parts
    arrived_corner, arrived = core(far_corner, shares), core(far, shares)
    if before:
        arrived_corner, arrived = hold((arrived_corner, arrived), *before)
    return add_corner(near, arrived_corner), add_main(near, arrived)


def send_sum(added, members, shares):
    (upper, lower), (own, side_a, side_b, partner_a, partner_b) = added
    corners = across(upper, shares), to_partner(lower, members)
    return corners, (own, side_b, partner_a, across(side_a, shares), to_partner(partner_b, members))


def close_sum(corners, opened, members, shares, *before):
    corner_side, corner_partner = corners
    own, side, partner, side_first, partner_first = opened
    side_second = across((side + corner_partner.astype(F32)).astype(BF16), shares)
    partner_second = to_partner((partner + corner_side.astype(F32)).astype(BF16), members)
    if before:
        side_second, partner_second = hold((side_second, partner_second), *before)
    from_side = jnp.concatenate([side_first, side_second], axis=0).astype(F32)
    from_partner = jnp.concatenate([partner_second, partner_first], axis=0).astype(F32)
    return own + from_side + from_partner


def sum_everywhere(values, axis, mask, stop):
    count = lax.axis_size(axis)
    while mask < stop:
        values = values + exchange(values, axis, count, mask)
        mask <<= 1
    return values


def matmul(first_op, second_op):
    return jnp.dot(first_op, second_op, preferred_element_type=F32)


def matmul_tn(first_op, second_op):
    return lax.dot_general(
        first_op, second_op, (((0,), (0,)), ((), ())), preferred_element_type=F32
    )


def matmul_nt(first_op, second_op):
    return lax.dot_general(
        first_op, second_op, (((1,), (1,)), ((), ())), preferred_element_type=F32
    )


def normalize(values):
    inv_root = lax.rsqrt(jnp.mean(values * values, axis=-1, keepdims=True) + NORM_EPSILON)
    return (values * inv_root, inv_root)


def norm_back(gradient, unit_rows, inv_root, gain_vec):
    scaled = gradient * gain_vec
    return inv_root * (scaled - unit_rows * jnp.mean(scaled * unit_rows, axis=-1, keepdims=True))


def rope_tables(slot_count, head_size):
    half_width = head_size // 2
    inverse = ROPE_THETA ** (-(jnp.arange(half_width, dtype=F32) * 2.0 / head_size))
    angles = jnp.arange(slot_count, dtype=F32)[:, None] * inverse[None, :]
    cosine = jnp.concatenate([jnp.cos(angles), jnp.cos(angles)], axis=-1)
    signed_sine = jnp.concatenate([-jnp.sin(angles), jnp.sin(angles)], axis=-1)
    return (cosine, signed_sine)


def piece_of(mask, rows):
    return mask & 1, pl.ds(pl.multiple_of((mask >> 1) * rows, rows), rows)


def allowed_block(block, rows, width, length):
    row_slot = block * rows + lax.broadcasted_iota(jnp.int32, (rows, width), 0)
    col_slot = lax.broadcasted_iota(jnp.int32, (rows, width), 1)
    return (col_slot <= row_slot) & (col_slot < length)


def turn(unit_rows, gain_vec, cosine, signed_sine):
    normed = unit_rows * gain_vec
    half = normed.shape[-1] // 2
    return normed * cosine + pltpu.roll(normed, half, 1) * signed_sine


def turn_back(gradient, cosine, signed_sine):
    half = gradient.shape[-1] // 2
    return gradient * cosine - pltpu.roll(gradient, half, 1) * signed_sine


def attend_forward_kernel(
    masks,
    head_size,
    score_scale,
    share_ref,
    length_ref,
    query_ref,
    key_ref,
    value_ref,
    query_gain_ref,
    key_gain_ref,
    cosine_ref,
    sine_ref,
    attended_ref,
    log_ref,
    query_rot_ref,
    key_rot_ref,
    value_low_ref,
):
    blocks = len(masks)
    rows = 2 * query_ref.shape[1] // blocks
    group = query_ref.shape[2] // head_size
    share, length = share_ref[0], length_ref[pl.program_id(0)]
    for mask in masks:
        side, here = mask & 1, pl.ds((mask >> 1) * rows, rows)
        there = pl.ds(pl.multiple_of((share ^ mask) * rows, rows), rows)
        cosine, signed_sine = cosine_ref[there, :], sine_ref[there, :]
        for head in range(group):
            cols = pl.ds(head * head_size, head_size)
            unit_rows, _ = normalize(query_ref[side, here, cols])
            turned = turn(unit_rows, query_gain_ref[...], cosine, signed_sine)
            query_rot_ref[there, cols] = turned.astype(BF16)
        unit_rows, _ = normalize(key_ref[side, here, :])
        turned = turn(unit_rows, key_gain_ref[...], cosine, signed_sine)
        key_rot_ref[there, :] = turned.astype(BF16)
        value_low_ref[there, :] = value_ref[side, here, :].astype(BF16)

    for block in range(blocks):
        width = (block + 1) * rows
        here = pl.ds(block * rows, rows)
        allowed = allowed_block(block, rows, width, length)
        side, back = piece_of(share ^ block, rows)

        def one_head(head, carry, width=width, here=here, allowed=allowed, side=side, back=back):
            cols = pl.ds(pl.multiple_of(head * head_size, head_size), head_size)
            scores = matmul_nt(query_rot_ref[here, cols], key_rot_ref[:width, :])
            logits = jnp.where(allowed, scores * score_scale, MASKED_LOGIT)
            highest = jnp.max(logits, axis=-1, keepdims=True)
            weights_raw = jnp.exp(logits - highest)
            row_total = jnp.sum(weights_raw, axis=-1, keepdims=True)
            probabilities = (weights_raw * (1.0 / row_total)).astype(BF16)
            attended_ref[side, back, cols] = matmul(probabilities, value_low_ref[:width, :])
            log_ref[here, cols] = jnp.broadcast_to(highest + jnp.log(row_total), (rows, head_size))
            return carry

        lax.fori_loop(0, group, one_head, 0)


def attend_backward_kernel(
    masks,
    head_size,
    score_scale,
    share_ref,
    length_ref,
    grad_ref,
    gate_grad_ref,
    query_ref,
    key_ref,
    query_rot_ref,
    key_rot_ref,
    value_low_ref,
    log_ref,
    query_gain_ref,
    key_gain_ref,
    cosine_ref,
    sine_ref,
    send_ref,
    gain_ref,
    query_grad_ref,
    key_grad_ref,
    value_grad_ref,
):
    blocks = len(masks)
    rows = 2 * query_ref.shape[1] // blocks
    group = query_ref.shape[2] // head_size
    kv_heads = pl.num_programs(1)
    kv_head = pl.program_id(1)
    share, length = share_ref[0], length_ref[pl.program_id(0)]
    key_grad_ref[...] = jnp.zeros_like(key_grad_ref)
    value_grad_ref[...] = jnp.zeros_like(value_grad_ref)

    @pl.when((pl.program_id(0) == 0) & (kv_head == 0))
    def _():
        gain_ref[...] = jnp.zeros_like(gain_ref)

    for block in range(blocks):
        width = (block + 1) * rows
        here = pl.ds(block * rows, rows)
        allowed = allowed_block(block, rows, width, length)
        side, back = piece_of(share ^ block, rows)

        def one_head(head, carry, width=width, here=here, allowed=allowed, side=side, back=back):
            cols = pl.ds(pl.multiple_of(head * head_size, head_size), head_size)
            queries, grads = query_rot_ref[here, cols], grad_ref[side, back, cols]
            scores = matmul_nt(queries, key_rot_ref[:width, :])
            logits = jnp.where(allowed, scores * score_scale, MASKED_LOGIT)
            soft = jnp.where(allowed, jnp.exp(logits - log_ref[here, cols][:, :1]), 0.0)
            prob_grad = matmul_nt(grads, value_low_ref[:width, :])
            centre = jnp.sum(soft * prob_grad, axis=-1, keepdims=True)
            score_grad = (score_scale * soft * (prob_grad - centre)).astype(BF16)
            query_grad_ref[here, cols] = matmul(score_grad, key_rot_ref[:width, :])
            key_grad_ref[:width, :] += matmul_tn(score_grad, queries)
            value_grad_ref[:width, :] += matmul_tn(soft.astype(BF16), grads)
            return carry

        lax.fori_loop(0, group, one_head, 0)

    key_base, value_base = kv_heads * group * head_size, kv_heads * (group + 1) * head_size
    gate_base = kv_heads * (group + 2) * head_size
    for mask in masks:
        side, here = mask & 1, pl.ds((mask >> 1) * rows, rows)
        there = pl.ds(pl.multiple_of((share ^ mask) * rows, rows), rows)
        cosine, signed_sine = cosine_ref[there, :], sine_ref[there, :]

        def through_norm(gradient, raw, gain_vec):
            normed_grad = turn_back(gradient, cosine, signed_sine)
            unit_rows, inv_root = normalize(raw)
            gain_part = jnp.sum(normed_grad * unit_rows, axis=0, keepdims=True)
            return norm_back(normed_grad, unit_rows, inv_root, gain_vec).astype(BF16), gain_part

        for head in range(group):
            cols = pl.ds(head * head_size, head_size)
            sent, gain_part = through_norm(
                query_grad_ref[there, cols], query_ref[side, here, cols], query_gain_ref[...]
            )
            offset = pl.multiple_of((kv_head * group + head) * head_size, head_size)
            send_ref[side, here, pl.ds(offset, head_size)] = sent
            gain_ref[0:1, :] += gain_part
        sent, gain_part = through_norm(
            key_grad_ref[there, :], key_ref[side, here, :], key_gain_ref[...]
        )
        offset = pl.multiple_of(key_base + kv_head * head_size, head_size)
        send_ref[side, here, pl.ds(offset, head_size)] = sent
        gain_ref[1:2, :] += gain_part
        offset = pl.multiple_of(value_base + kv_head * head_size, head_size)
        send_ref[side, here, pl.ds(offset, head_size)] = value_grad_ref[there, :].astype(BF16)
        offset = pl.multiple_of(gate_base + kv_head * group * head_size, head_size)
        send_ref[side, here, pl.ds(offset, group * head_size)] = gate_grad_ref[side, here, :]


def units_kernel(rows_ref, gate_weights_ref, up_weights_ref, gate_ref, up_ref, mid_ref):
    rows = rows_ref[...]
    gate = matmul(rows, gate_weights_ref[...])
    gate_ref[...] = gate
    up = matmul(rows, up_weights_ref[...])
    up_ref[...] = up
    mid_ref[...] = (gate * jax.nn.sigmoid(gate) * up).astype(BF16)


def hidden_units(normed, gate_weights, up_weights):
    rows, width = normed.shape
    units = gate_weights.shape[1]
    tile = rows // 8
    tokens = pl.BlockSpec((tile, width), lambda i: (i, 0))
    hidden = pl.BlockSpec((tile, units), lambda i: (i, 0))
    weight = pl.BlockSpec((width, units), lambda i: (0, 0), pipeline_mode=pl.Buffered(1))
    return pl.pallas_call(
        units_kernel,
        grid=(8,),
        in_specs=[tokens, weight, weight],
        out_specs=[hidden, hidden, hidden],
        out_shape=[jax.ShapeDtypeStruct((rows, units), kind) for kind in (F32, F32, BF16)],
        compiler_params=pltpu.CompilerParams(vmem_limit_bytes=32 << 20),
        cost_estimate=light_cost(),
        name="hidden_units",
    )(normed, gate_weights, up_weights)


def unit_grads_kernel(
    near_steps,
    far_steps,
    branch_ref,
    gate_ref,
    up_ref,
    down_weights_ref,
    gate_weights_ref,
    up_weights_ref,
    gate_grad_ref,
    up_grad_ref,
    near_ref,
    far_ref,
    corner_ref,
):
    step = pl.program_id(0)
    mid_grad = matmul(branch_ref[...], down_weights_ref[...])
    gate, up = gate_ref[...], up_ref[...]
    sig = jax.nn.sigmoid(gate)
    gate_grad = (mid_grad * up * sig * (1.0 + gate * (1.0 - sig))).astype(BF16)
    up_grad = (mid_grad * (gate * sig)).astype(BF16)
    gate_grad_ref[...] = gate_grad
    up_grad_ref[...] = up_grad
    back = matmul_nt(gate_grad, gate_weights_ref[...]) + matmul_nt(up_grad, up_weights_ref[...])
    back = back.astype(BF16)

    @pl.when(step < near_steps)
    def _():
        near_ref[...] = back

    @pl.when((step >= near_steps) & (step < near_steps + far_steps))
    def _():
        far_ref[...] = back

    @pl.when(step == near_steps + far_steps)
    def _():
        corner_ref[...] = back


def unit_grads(branch, ffn_gate, ffn_up, down_weights, gate_weights, up_weights):
    rows, width = branch.shape
    units = ffn_gate.shape[1]
    tile = rows // 8
    tokens = pl.BlockSpec((tile, width), lambda i: (i, 0))
    hidden = pl.BlockSpec((tile, units), lambda i: (i, 0))
    weight = pl.BlockSpec((width, units), lambda i: (0, 0), pipeline_mode=pl.Buffered(1))
    gate_grad, up_grad, *parts = pl.pallas_call(
        functools.partial(unit_grads_kernel, 4, 3),
        grid=(8,),
        in_specs=[tokens, hidden, hidden, weight, weight, weight],
        out_specs=[
            hidden,
            hidden,
            pl.BlockSpec((tile, width), lambda i: (jnp.minimum(i, 3), 0)),
            pl.BlockSpec((tile, width), lambda i: (jnp.clip(i - 4, 0, 2), 0)),
            pl.BlockSpec((tile, width), lambda i: (0, 0)),
        ],
        out_shape=[
            jax.ShapeDtypeStruct((rows, units), BF16),
            jax.ShapeDtypeStruct((rows, units), BF16),
            jax.ShapeDtypeStruct((4 * tile, width), BF16),
            jax.ShapeDtypeStruct((3 * tile, width), BF16),
            jax.ShapeDtypeStruct((tile, width), BF16),
        ],
        compiler_params=pltpu.CompilerParams(vmem_limit_bytes=44 << 20),
        cost_estimate=light_cost(),
        name="unit_grads",
    )(branch, ffn_gate, ffn_up, down_weights, gate_weights, up_weights)
    return gate_grad, up_grad, parts


def head_specs(slots, group, kv_heads, head_size):
    half = slots // 2
    wide = group * head_size

    def piece(width, base):
        return pl.BlockSpec((2, None, half, width), lambda s, c: (0, s, 0, base + c))

    def ordered(width):
        return pl.BlockSpec((None, slots, width), lambda s, c: (s, 0, c))

    raw = [piece(wide, 0), piece(head_size, kv_heads * group)]
    value = piece(head_size, kv_heads * (group + 1))
    gain = pl.BlockSpec((1, head_size), lambda s, c: (0, 0))
    table = pl.BlockSpec((slots, head_size), lambda s, c: (0, 0))
    scalar = pl.BlockSpec(memory_space=pltpu.SMEM)
    return raw, value, ordered(wide), ordered(head_size), gain, table, scalar


def attend_forward(qkv_raw, share, lengths, gains, tables, masks, sizes):
    kv_heads, group, head_size = sizes
    slots = qkv_raw.shape[0] // 2
    raw, value, wide, narrow, gain, table, scalar = head_specs(slots, group, kv_heads, head_size)
    split = qkv_raw.reshape(2, 2, slots // 2, qkv_raw.shape[1])
    width, key_width = kv_heads * group * head_size, kv_heads * head_size
    attended, *kept = pl.pallas_call(
        functools.partial(attend_forward_kernel, masks, head_size, head_size ** (-0.5)),
        grid=(2, kv_heads),
        in_specs=[scalar, scalar, *raw, value, gain, gain, table, table],
        out_specs=[raw[0], wide, wide, narrow, narrow],
        out_shape=[
            jax.ShapeDtypeStruct((2, 2, slots // 2, width), F32),
            jax.ShapeDtypeStruct((2, slots, width), F32),
            jax.ShapeDtypeStruct((2, slots, width), BF16),
            jax.ShapeDtypeStruct((2, slots, key_width), BF16),
            jax.ShapeDtypeStruct((2, slots, key_width), BF16),
        ],
        cost_estimate=light_cost(),
        name="attend_forward",
    )(share, lengths, split, split, split, *gains, *tables)
    return attended.reshape(2 * slots, width), kept


def attend_backward(grads, gate_grads, qkv_raw, kept, share, lengths, gains, tables, masks, sizes):
    kv_heads, group, head_size = sizes
    slots = qkv_raw.shape[0] // 2
    raw, value, wide, narrow, gain, table, scalar = head_specs(slots, group, kv_heads, head_size)
    split = qkv_raw.reshape(2, 2, slots // 2, qkv_raw.shape[1])
    log_total, query_rot, key_rot, value_low = kept
    width = qkv_raw.shape[1] + gate_grads.shape[1]
    sent, gain_parts = pl.pallas_call(
        functools.partial(attend_backward_kernel, masks, head_size, head_size ** (-0.5)),
        grid=(2, kv_heads),
        in_specs=[scalar, scalar, raw[0], raw[0], *raw, wide, narrow, narrow, wide]
        + [gain, gain, table, table],
        out_specs=[
            pl.BlockSpec((2, None, slots // 2, width), lambda s, c: (0, s, 0, 0)),
            pl.BlockSpec((8, head_size), lambda s, c: (0, 0)),
        ],
        out_shape=[
            jax.ShapeDtypeStruct((2, 2, slots // 2, width), BF16),
            jax.ShapeDtypeStruct((8, head_size), F32),
        ],
        scratch_shapes=[
            pltpu.VMEM((slots, group * head_size), F32),
            pltpu.VMEM((slots, head_size), F32),
            pltpu.VMEM((slots, head_size), F32),
        ],
        cost_estimate=light_cost(),
        name="attend_backward",
    )(
        share,
        lengths,
        grads.reshape(2, 2, slots // 2, grads.shape[1]),
        gate_grads.reshape(2, 2, slots // 2, grads.shape[1]),
        split,
        split,
        query_rot,
        key_rot,
        value_low,
        log_total,
        *gains,
        *tables,
    )
    return sent.reshape(2 * slots, width), gain_parts


def body(
    members,
    shares,
    hidden_in,
    lengths,
    attn_gain,
    query_weight,
    key_weight,
    value_weight,
    output_gate,
    query_gain,
    key_gain,
    out_weight,
    mlp_gain,
    gate_weight,
    up_weight,
    down_weight,
    cotangent,
):
    odd = lax.axis_index("fsdp") % 2 == 1
    share = lax.axis_index("tensor")
    local_rows = hidden_in.shape[0]
    head_size = query_gain.shape[0]
    query_width = query_weight.shape[1] // 2
    key_width = key_weight.shape[1] // 2
    sizes = (key_width // head_size, query_width // key_width, head_size)
    masks = row_masks(shares)
    slots = share * local_rows + jnp.arange(local_rows)
    valid_rows = (slots < lengths[0]).astype(F32)[:, None]
    share_at = share.astype(jnp.int32)[None]
    both_lengths = jnp.concatenate([lengths, to_partner(lengths, members)])
    gains = (query_gain[None, :], key_gain[None, :])
    half_rows = local_rows * shares

    def gather_rows(values, *before):
        return rows_in(values, members, shares, *before)

    def sum_rows(parts, first, last):
        added = open_sum(parts, members, shares, *first)
        return close_sum(*send_sum(added, members, shares), members, shares, *last)

    def in_parts(function):
        corner = function(slice(2 * half_rows - local_rows, 2 * half_rows)).astype(BF16)
        far = function(slice(half_rows, 2 * half_rows - local_rows)).astype(BF16)
        near = function(slice(0, half_rows)).astype(BF16)
        return near, far, corner

    qkv_rows = pair_rows([query_weight, key_weight, value_weight], odd, members)
    qkv_full = gather_line(qkv_rows, members)
    gate_out_rows = pair_rows([output_gate, out_weight.T], odd, members)
    gate_out_full = gather_line(hold(gate_out_rows, qkv_rows), members)

    residual = hidden_in.astype(F32)
    unit_one, root_one = normalize(residual)
    gate_rows = pair_rows([hold(gate_weight, gate_out_rows)], odd, members)
    normed_one = gather_rows(hold((unit_one * attn_gain).astype(BF16), gate_rows))
    qkv_raw = matmul(normed_one, qkv_full)
    grad_rows = cotangent.astype(F32) * valid_rows
    tables = rope_tables(half_rows, head_size)
    attended, kept = attend_forward(
        qkv_raw, share_at, both_lengths, gains, tables, masks, sizes
    )
    up_in, down_in = hold((up_weight, down_weight), normed_one)
    up_rows = pair_rows([up_in], odd, members, attended)
    down_rows = pair_rows([down_in.T], odd, members, attended)
    gate_weights = gather_line(hold(gate_rows, qkv_full), members)
    up_weights = gather_line(hold(up_rows, gate_out_full), members)
    down_weights = gather_line(hold(down_rows, gate_weights), members)
    gate_full, out_full = gate_out_full[:, :query_width], gate_out_full[:, query_width:]
    gate_pre = matmul(hold(normed_one, attended, up_rows, down_rows), gate_full)
    gate_sig = jax.nn.sigmoid(gate_pre)
    gated_out = (attended * gate_sig).astype(BF16)
    attn_parts = in_parts(lambda rows: matmul_nt(gated_out[rows], out_full))
    middle = residual + sum_rows(attn_parts, (), (gate_weights,))
    unit_two, root_two = normalize(middle)
    normed_two = gather_rows((unit_two * mlp_gain).astype(BF16))
    one_weights = jnp.concatenate([qkv_full, gate_full], axis=1)
    ffn_gate, ffn_up, ffn_mid = hidden_units(normed_two, gate_weights, up_weights)
    branch_full = gather_rows(
        hold(grad_rows.astype(BF16), normed_two), None, one_weights, ffn_mid
    )

    down_part = matmul_tn(branch_full, ffn_mid).astype(BF16)
    down_sum = scatter_line(down_part, members)

    gate_grad, up_grad, back_parts = unit_grads(
        branch_full, ffn_gate, ffn_up, hold(down_weights, down_part), gate_weights, up_weights
    )
    gate_part = matmul_tn(normed_two, hold(gate_grad, back_parts)).astype(BF16)
    gate_sum = scatter_line(gate_part, members)
    up_part = matmul_tn(normed_two, hold(up_grad, gate_part)).astype(BF16)
    up_sum = scatter_line(up_part, members)
    norm_two_grad = sum_rows(back_parts, (gate_part,), (down_sum, up_part))

    mlp_gain_part = jnp.sum(norm_two_grad * unit_two, axis=0)
    middle_grad = grad_rows + norm_back(norm_two_grad, unit_two, root_two, mlp_gain)
    mid_late = hold(ffn_mid, norm_two_grad)
    branch_parts = in_parts(lambda rows: matmul_nt(mid_late[rows], down_weights))
    attn_full_grad = gather_rows(middle_grad.astype(BF16), None, branch_parts, gate_sum)
    branch_added = open_sum(branch_parts, members, shares)
    down_swap = swap_rows(hold(down_sum, attn_full_grad), odd, members)
    gate_swap = swap_rows(hold(gate_sum, attn_full_grad), odd, members)
    attn_full_grad = hold(attn_full_grad, branch_added)
    corners, opened = send_sum(hold(branch_added, attn_full_grad), members, shares)
    gated_grad = matmul(attn_full_grad, out_full)
    attended_grad = (gated_grad * gate_sig).astype(BF16)
    gate_pre_grad = (gated_grad * attended * gate_sig * (1.0 - gate_sig)).astype(BF16)
    gate_attn_part = matmul_tn(normed_one, gate_pre_grad).astype(BF16)
    gate_out_part = jnp.concatenate(
        [
            gate_attn_part,
            matmul_tn(attn_full_grad, gated_out).astype(BF16),
        ],
        axis=1,
    )
    gate_out_sum = scatter_line(gate_out_part, members)
    one_send, gain_parts = attend_backward(
        hold(attended_grad, gate_out_part),
        gate_pre_grad,
        qkv_raw,
        kept,
        share_at,
        both_lengths,
        gains,
        tables,
        masks,
        sizes,
    )
    one_send = hold(one_send, corners, opened, down_swap, gate_swap)
    ffn_branch = close_sum(corners, opened, members, shares, one_send)
    output = ((middle + ffn_branch) * valid_rows).astype(BF16)
    units = up_sum.shape[1]
    one_parts = in_parts(lambda rows: matmul_nt(one_send[rows], one_weights))
    qkv_send = hold(one_send, up_sum, one_parts)[:, : qkv_raw.shape[1]]
    qkv_part = matmul_tn(normed_one, qkv_send).astype(BF16)
    qkv_sum = scatter_line(qkv_part, members)
    attn_gain_part = (
        dot_rows(qkv_part, qkv_full) + dot_rows(gate_attn_part, gate_full)
    ) / attn_gain
    up_swap = swap_rows(hold(up_sum, one_send), odd, members)
    added_one = open_sum(one_parts, members, shares, qkv_part)
    gain_parts = hold(
        jnp.concatenate([attn_gain_part, mlp_gain_part, gain_parts[0], gain_parts[1]]), added_one
    )
    gain_parts = sum_everywhere(gain_parts, "fsdp", 2, members)
    gain_parts = sum_everywhere(gain_parts, "tensor", 1, 2)
    norm_one_grad = close_sum(
        *send_sum(added_one, members, shares), members, shares, gate_out_sum, gain_parts, up_swap, output
    )
    gain_totals = hold(gain_parts, norm_one_grad)
    gain_totals = sum_everywhere(gain_totals, "tensor", 2, shares)
    gain_totals = sum_everywhere(gain_totals, "fsdp", 1, 2)
    grad_hidden = middle_grad + norm_back(norm_one_grad, unit_one, root_one, attn_gain)
    (down_shard,) = own_shard(*down_swap, odd, (units,))
    (gate_shard,) = own_shard(*gate_swap, odd, (units,))
    gate_out_swap = swap_rows(hold(gate_out_sum, norm_one_grad, qkv_sum), odd, members)
    (up_shard,) = own_shard(*up_swap, odd, (units,))
    gate_attn_shard, out_shard = own_shard(*gate_out_swap, odd, (query_width,) * 2)
    qkv_sum = hold(qkv_sum, norm_one_grad)
    query_shard, key_shard, value_shard = own_shard(
        *swap_rows(qkv_sum, odd, members), odd, (query_width, key_width, key_width)
    )
    width = hidden_in.shape[1]
    return (
        output,
        grad_hidden,
        gain_totals[:width],
        query_shard,
        key_shard,
        value_shard,
        gate_attn_shard,
        gain_totals[2 * width : 2 * width + head_size],
        gain_totals[2 * width + head_size :],
        out_shard.T,
        gain_totals[width : 2 * width],
        gate_shard,
        up_shard,
        down_shard.T,
    )


def solution(mesh):
    members, shares = mesh.shape["fsdp"], mesh.shape["tensor"]

    def layer(*operands):
        return body(members, shares, *operands)

    tokens = P(("fsdp", "tensor"), None)
    return jax.shard_map(
        layer,
        mesh=mesh,
        in_specs=(
            tokens,
            P("fsdp"),
            P(),
            P("fsdp", "tensor"),
            P("fsdp", "tensor"),
            P("fsdp", "tensor"),
            P("fsdp", "tensor"),
            P(),
            P(),
            P("tensor", "fsdp"),
            P(),
            P("fsdp", "tensor"),
            P("fsdp", "tensor"),
            P("tensor", "fsdp"),
            tokens,
        ),
        out_specs=(
            tokens,
            tokens,
            P(),
            P("fsdp", "tensor"),
            P("fsdp", "tensor"),
            P("fsdp", "tensor"),
            P("fsdp", "tensor"),
            P(),
            P(),
            P("tensor", "fsdp"),
            P(),
            P("fsdp", "tensor"),
            P("fsdp", "tensor"),
            P("tensor", "fsdp"),
        ),
        check_vma=False,
    )
```

```python
import functools

import jax
import jax.numpy as jnp
from jax import lax
from jax.experimental import pallas as pl
from jax.experimental.pallas import tpu as pltpu
from jax.sharding import PartitionSpec as P

NORM_EPSILON = 1e-06
ROPE_THETA = 1000000.0
MASKED_LOGIT = -1e30
F32 = jnp.float32
BF16 = jnp.bfloat16


def exchange(values, axis, size, mask):
    return lax.ppermute(values, axis, [(i, i ^ mask) for i in range(size)])


def lines(count):
    return [list(range(0, count, 2)), list(range(1, count, 2))]


def to_partner(values, count):
    return exchange(values, "fsdp", count, 1)


def halves(values, odd):
    width = values.shape[-1] // 2
    left, right = values[..., :width], values[..., width:]
    return jnp.where(odd, right, left), jnp.where(odd, left, right)


def in_order(own, other, odd, axis):
    first, second = jnp.where(odd, other, own), jnp.where(odd, own, other)
    return jnp.concatenate([first, second], axis=axis)


def pair_rows(shards, odd, count, *before):
    split = [halves(shard, odd) for shard in shards]
    own = jnp.concatenate([piece[0] for piece in split], axis=1)
    other = jnp.concatenate([piece[1] for piece in split], axis=1)
    arrived = to_partner(other, count)
    if before:
        arrived = hold(arrived, *before)
    return in_order(own, arrived, odd, 0)


def gather_line(rows, count):
    return lax.all_gather(rows, "fsdp", axis=0, tiled=True, axis_index_groups=lines(count))


def scatter_line(total, count):
    return lax.psum_scatter(
        total, "fsdp", scatter_dimension=0, tiled=True, axis_index_groups=lines(count)
    )


def swap_rows(rows, odd, count):
    height = rows.shape[0] // 2
    top, bottom = rows[:height], rows[height:]
    return jnp.where(odd, bottom, top), to_partner(jnp.where(odd, top, bottom), count)


def own_shard(own, other, odd, widths):
    shards, start = [], 0
    for width in widths:
        piece = slice(start, start + width)
        shards.append(in_order(own[:, piece], other[:, piece], odd, 1).astype(F32))
        start += width
    return shards


def dot_rows(first, second):
    return jnp.sum(first.astype(F32) * second.astype(F32), axis=1)


def hold(value, *others):
    return lax.optimization_barrier((value,) + others)[0]


def row_masks(count):
    half = count // 2
    return [((p % half) << 1) | (p // half) for p in range(count)]


def across(values, count):
    return exchange(values, "tensor", count, 2)


def core(values, count):
    return exchange(values, "tensor", count, 1)


def rows_in(values, members, shares, *before):
    half = values.shape[0] // 2
    side = across(values, shares)
    partner = to_partner(values, members)
    if before and before[0] is not None:
        side, partner = hold((side, partner), before[0])
    upper = to_partner(side[:half], members)
    lower = across(partner[half:], shares)
    if before[1:]:
        upper, lower = hold((upper, lower), *before[1:])
    near = [values, side, partner, upper, lower]
    return stack_rows(near + [core(piece, shares) for piece in near])


def stack_kernel(count, *refs):
    pieces, out, held, in_sems, out_sems = refs[:count], *refs[count:]
    incoming, outgoing, start = [], [], 0
    for i, piece in enumerate(pieces):
        place = pl.ds(start, piece.shape[0])
        incoming.append(pltpu.make_async_copy(piece, held.at[place], in_sems.at[i]))
        outgoing.append(pltpu.make_async_copy(held.at[place], out.at[place], out_sems.at[i]))
        incoming[-1].start()
        start += piece.shape[0]
    for arrive, leave in zip(incoming, outgoing):
        arrive.wait()
        leave.start()
    for leave in outgoing:
        leave.wait()


def stack_rows(pieces):
    count, (_, width), kind = len(pieces), pieces[0].shape, pieces[0].dtype
    rows = sum(piece.shape[0] for piece in pieces)
    anywhere = pl.BlockSpec(memory_space=pl.ANY)
    return pl.pallas_call(
        functools.partial(stack_kernel, count),
        in_specs=[anywhere] * count,
        out_specs=anywhere,
        out_shape=jax.ShapeDtypeStruct((rows, width), kind),
        scratch_shapes=[
            pltpu.VMEM((rows, width), kind),
            pltpu.SemaphoreType.DMA((count,)),
            pltpu.SemaphoreType.DMA((count,)),
        ],
        compiler_params=pltpu.CompilerParams(vmem_limit_bytes=(rows * width * 2) + (1 << 20)),
        cost_estimate=light_cost(),
        name="stack_rows",
    )(*pieces)


def light_cost():
    return pl.CostEstimate(flops=1024, bytes_accessed=1024, transcendentals=0)


def corner_kernel(near_ref, arrived_ref, upper_ref, lower_ref):
    half = upper_ref.shape[0]
    total = (near_ref[...].astype(F32) + arrived_ref[...].astype(F32)).astype(BF16)
    upper_ref[...] = total[:half]
    lower_ref[...] = total[half:]


def add_corner(near, arrived):
    rows, width = arrived.shape
    tile = width // 2
    half = pl.BlockSpec((rows // 2, tile), lambda i: (0, i))
    return pl.pallas_call(
        corner_kernel,
        grid=(2,),
        in_specs=[
            pl.BlockSpec((rows, tile), lambda i: (3, i)),
            pl.BlockSpec((rows, tile), lambda i: (0, i)),
        ],
        out_specs=[half, half],
        out_shape=[jax.ShapeDtypeStruct((rows // 2, width), BF16)] * 2,
        compiler_params=pltpu.CompilerParams(vmem_limit_bytes=16 << 20),
        cost_estimate=light_cost(),
        name="add_corner",
    )(near, arrived)


def main_kernel(near_ref, arrived_ref, own_ref, side_a, side_b, partner_a, partner_b):
    rows = own_ref.shape[0]
    half = rows // 2

    def total(start, size):
        piece = pl.ds(start, size)
        return near_ref[piece, :].astype(F32) + arrived_ref[piece, :].astype(F32)

    own_ref[...] = total(0, rows)
    side_a[...] = total(rows, half).astype(BF16)
    side_b[...] = total(rows + half, half)
    partner_a[...] = total(2 * rows, half)
    partner_b[...] = total(2 * rows + half, half).astype(BF16)


def add_main(near, arrived):
    rows, width = arrived.shape[0] // 3, arrived.shape[1]
    tile = width // 4
    whole = pl.BlockSpec((rows, tile), lambda i: (0, i))
    half = pl.BlockSpec((rows // 2, tile), lambda i: (0, i))
    three = pl.BlockSpec((3 * rows, tile), lambda i: (0, i))

    def shape(kind):
        return jax.ShapeDtypeStruct((rows // 2, width), kind)

    return pl.pallas_call(
        main_kernel,
        grid=(4,),
        in_specs=[three, three],
        out_specs=[whole, half, half, half, half],
        out_shape=[
            jax.ShapeDtypeStruct((rows, width), F32),
            shape(BF16),
            shape(F32),
            shape(F32),
            shape(BF16),
        ],
        compiler_params=pltpu.CompilerParams(vmem_limit_bytes=24 << 20),
        cost_estimate=light_cost(),
        name="add_main",
    )(near, arrived)


def open_sum(parts, members, shares, *before):
    near, far, far_corner = parts
    arrived_corner, arrived = core(far_corner, shares), core(far, shares)
    if before:
        arrived_corner, arrived = hold((arrived_corner, arrived), *before)
    return add_corner(near, arrived_corner), add_main(near, arrived)


def send_sum(added, members, shares):
    (upper, lower), (own, side_a, side_b, partner_a, partner_b) = added
    corners = across(upper, shares), to_partner(lower, members)
    return corners, (own, side_b, partner_a, across(side_a, shares), to_partner(partner_b, members))


def close_sum(corners, opened, members, shares, *before):
    corner_side, corner_partner = corners
    own, side, partner, side_first, partner_first = opened
    side_second = across((side + corner_partner.astype(F32)).astype(BF16), shares)
    partner_second = to_partner((partner + corner_side.astype(F32)).astype(BF16), members)
    if before:
        side_second, partner_second = hold((side_second, partner_second), *before)
    from_side = jnp.concatenate([side_first, side_second], axis=0).astype(F32)
    from_partner = jnp.concatenate([partner_second, partner_first], axis=0).astype(F32)
    return own + from_side + from_partner


def sum_everywhere(values, axis, mask, stop):
    count = lax.axis_size(axis)
    while mask < stop:
        values = values + exchange(values, axis, count, mask)
        mask <<= 1
    return values


def matmul(first_op, second_op):
    return jnp.dot(first_op, second_op, preferred_element_type=F32)


def matmul_tn(first_op, second_op):
    return lax.dot_general(
        first_op, second_op, (((0,), (0,)), ((), ())), preferred_element_type=F32
    )


def matmul_nt(first_op, second_op):
    return lax.dot_general(
        first_op, second_op, (((1,), (1,)), ((), ())), preferred_element_type=F32
    )


def normalize(values):
    inv_root = lax.rsqrt(jnp.mean(values * values, axis=-1, keepdims=True) + NORM_EPSILON)
    return (values * inv_root, inv_root)


def norm_back(gradient, unit_rows, inv_root, gain_vec):
    scaled = gradient * gain_vec
    return inv_root * (scaled - unit_rows * jnp.mean(scaled * unit_rows, axis=-1, keepdims=True))


def rope_tables(slot_count, head_size):
    half_width = head_size // 2
    inverse = ROPE_THETA ** (-(jnp.arange(half_width, dtype=F32) * 2.0 / head_size))
    angles = jnp.arange(slot_count, dtype=F32)[:, None] * inverse[None, :]
    cosine = jnp.concatenate([jnp.cos(angles), jnp.cos(angles)], axis=-1)
    signed_sine = jnp.concatenate([-jnp.sin(angles), jnp.sin(angles)], axis=-1)
    return (cosine, signed_sine)


def piece_of(mask, rows):
    return mask & 1, pl.ds(pl.multiple_of((mask >> 1) * rows, rows), rows)


def allowed_block(block, rows, width, length):
    row_slot = block * rows + lax.broadcasted_iota(jnp.int32, (rows, width), 0)
    col_slot = lax.broadcasted_iota(jnp.int32, (rows, width), 1)
    return (col_slot <= row_slot) & (col_slot < length)


def turn(unit_rows, gain_vec, cosine, signed_sine):
    normed = unit_rows * gain_vec
    half = normed.shape[-1] // 2
    return normed * cosine + pltpu.roll(normed, half, 1) * signed_sine


def turn_back(gradient, cosine, signed_sine):
    half = gradient.shape[-1] // 2
    return gradient * cosine - pltpu.roll(gradient, half, 1) * signed_sine


def attend_forward_kernel(
    masks,
    head_size,
    score_scale,
    share_ref,
    length_ref,
    query_ref,
    key_ref,
    value_ref,
    query_gain_ref,
    key_gain_ref,
    cosine_ref,
    sine_ref,
    attended_ref,
    log_ref,
    query_rot_ref,
    key_rot_ref,
    value_low_ref,
):
    blocks = len(masks)
    rows = 2 * query_ref.shape[1] // blocks
    group = query_ref.shape[2] // head_size
    share, length = share_ref[0], length_ref[pl.program_id(0)]
    for mask in masks:
        side, here = mask & 1, pl.ds((mask >> 1) * rows, rows)
        there = pl.ds(pl.multiple_of((share ^ mask) * rows, rows), rows)
        cosine, signed_sine = cosine_ref[there, :], sine_ref[there, :]
        for head in range(group):
            cols = pl.ds(head * head_size, head_size)
            unit_rows, _ = normalize(query_ref[side, here, cols])
            turned = turn(unit_rows, query_gain_ref[...], cosine, signed_sine)
            query_rot_ref[there, cols] = turned.astype(BF16)
        unit_rows, _ = normalize(key_ref[side, here, :])
        turned = turn(unit_rows, key_gain_ref[...], cosine, signed_sine)
        key_rot_ref[there, :] = turned.astype(BF16)
        value_low_ref[there, :] = value_ref[side, here, :].astype(BF16)

    for block in range(blocks):
        width = (block + 1) * rows
        here = pl.ds(block * rows, rows)
        allowed = allowed_block(block, rows, width, length)
        side, back = piece_of(share ^ block, rows)

        def one_head(head, carry, width=width, here=here, allowed=allowed, side=side, back=back):
            cols = pl.ds(pl.multiple_of(head * head_size, head_size), head_size)
            scores = matmul_nt(query_rot_ref[here, cols], key_rot_ref[:width, :])
            logits = jnp.where(allowed, scores * score_scale, MASKED_LOGIT)
            highest = jnp.max(logits, axis=-1, keepdims=True)
            weights_raw = jnp.exp(logits - highest)
            row_total = jnp.sum(weights_raw, axis=-1, keepdims=True)
            probabilities = (weights_raw * (1.0 / row_total)).astype(BF16)
            attended_ref[side, back, cols] = matmul(probabilities, value_low_ref[:width, :])
            log_ref[here, cols] = jnp.broadcast_to(highest + jnp.log(row_total), (rows, head_size))
            return carry

        lax.fori_loop(0, group, one_head, 0)


def attend_backward_kernel(
    masks,
    head_size,
    score_scale,
    share_ref,
    length_ref,
    grad_ref,
    gate_grad_ref,
    query_ref,
    key_ref,
    query_rot_ref,
    key_rot_ref,
    value_low_ref,
    log_ref,
    query_gain_ref,
    key_gain_ref,
    cosine_ref,
    sine_ref,
    send_ref,
    gain_ref,
    query_grad_ref,
    key_grad_ref,
    value_grad_ref,
):
    blocks = len(masks)
    rows = 2 * query_ref.shape[1] // blocks
    group = query_ref.shape[2] // head_size
    kv_heads = pl.num_programs(1)
    kv_head = pl.program_id(1)
    share, length = share_ref[0], length_ref[pl.program_id(0)]
    key_grad_ref[...] = jnp.zeros_like(key_grad_ref)
    value_grad_ref[...] = jnp.zeros_like(value_grad_ref)

    @pl.when((pl.program_id(0) == 0) & (kv_head == 0))
    def _():
        gain_ref[...] = jnp.zeros_like(gain_ref)

    for block in range(blocks):
        width = (block + 1) * rows
        here = pl.ds(block * rows, rows)
        allowed = allowed_block(block, rows, width, length)
        side, back = piece_of(share ^ block, rows)

        def one_head(head, carry, width=width, here=here, allowed=allowed, side=side, back=back):
            cols = pl.ds(pl.multiple_of(head * head_size, head_size), head_size)
            queries, grads = query_rot_ref[here, cols], grad_ref[side, back, cols]
            scores = matmul_nt(queries, key_rot_ref[:width, :])
            logits = jnp.where(allowed, scores * score_scale, MASKED_LOGIT)
            soft = jnp.where(allowed, jnp.exp(logits - log_ref[here, cols][:, :1]), 0.0)
            prob_grad = matmul_nt(grads, value_low_ref[:width, :])
            centre = jnp.sum(soft * prob_grad, axis=-1, keepdims=True)
            score_grad = (score_scale * soft * (prob_grad - centre)).astype(BF16)
            query_grad_ref[here, cols] = matmul(score_grad, key_rot_ref[:width, :])
            key_grad_ref[:width, :] += matmul_tn(score_grad, queries)
            value_grad_ref[:width, :] += matmul_tn(soft.astype(BF16), grads)
            return carry

        lax.fori_loop(0, group, one_head, 0)

    key_base, value_base = kv_heads * group * head_size, kv_heads * (group + 1) * head_size
    gate_base = kv_heads * (group + 2) * head_size
    for mask in masks:
        side, here = mask & 1, pl.ds((mask >> 1) * rows, rows)
        there = pl.ds(pl.multiple_of((share ^ mask) * rows, rows), rows)
        cosine, signed_sine = cosine_ref[there, :], sine_ref[there, :]

        def through_norm(gradient, raw, gain_vec):
            normed_grad = turn_back(gradient, cosine, signed_sine)
            unit_rows, inv_root = normalize(raw)
            gain_part = jnp.sum(normed_grad * unit_rows, axis=0, keepdims=True)
            return norm_back(normed_grad, unit_rows, inv_root, gain_vec).astype(BF16), gain_part

        for head in range(group):
            cols = pl.ds(head * head_size, head_size)
            sent, gain_part = through_norm(
                query_grad_ref[there, cols], query_ref[side, here, cols], query_gain_ref[...]
            )
            offset = pl.multiple_of((kv_head * group + head) * head_size, head_size)
            send_ref[side, here, pl.ds(offset, head_size)] = sent
            gain_ref[0:1, :] += gain_part
        sent, gain_part = through_norm(
            key_grad_ref[there, :], key_ref[side, here, :], key_gain_ref[...]
        )
        offset = pl.multiple_of(key_base + kv_head * head_size, head_size)
        send_ref[side, here, pl.ds(offset, head_size)] = sent
        gain_ref[1:2, :] += gain_part
        offset = pl.multiple_of(value_base + kv_head * head_size, head_size)
        send_ref[side, here, pl.ds(offset, head_size)] = value_grad_ref[there, :].astype(BF16)
        offset = pl.multiple_of(gate_base + kv_head * group * head_size, head_size)
        send_ref[side, here, pl.ds(offset, group * head_size)] = gate_grad_ref[side, here, :]


def units_kernel(rows_ref, gate_weights_ref, up_weights_ref, gate_ref, up_ref, mid_ref):
    rows = rows_ref[...]
    gate = matmul(rows, gate_weights_ref[...])
    gate_ref[...] = gate
    up = matmul(rows, up_weights_ref[...])
    up_ref[...] = up
    mid_ref[...] = (gate * jax.nn.sigmoid(gate) * up).astype(BF16)


def hidden_units(normed, gate_weights, up_weights):
    rows, width = normed.shape
    units = gate_weights.shape[1]
    tile = rows // 8
    tokens = pl.BlockSpec((tile, width), lambda i: (i, 0))
    hidden = pl.BlockSpec((tile, units), lambda i: (i, 0))
    weight = pl.BlockSpec((width, units), lambda i: (0, 0), pipeline_mode=pl.Buffered(1))
    return pl.pallas_call(
        units_kernel,
        grid=(8,),
        in_specs=[tokens, weight, weight],
        out_specs=[hidden, hidden, hidden],
        out_shape=[jax.ShapeDtypeStruct((rows, units), kind) for kind in (F32, F32, BF16)],
        compiler_params=pltpu.CompilerParams(vmem_limit_bytes=32 << 20),
        cost_estimate=light_cost(),
        name="hidden_units",
    )(normed, gate_weights, up_weights)


def unit_grads_kernel(
    near_steps,
    branch_ref,
    gate_ref,
    up_ref,
    down_weights_ref,
    gate_weights_ref,
    up_weights_ref,
    gate_grad_ref,
    up_grad_ref,
    near_ref,
    far_ref,
    corner_ref,
):
    step = pl.program_id(0)
    mid_grad = matmul(branch_ref[...], down_weights_ref[...])
    gate, up = gate_ref[...], up_ref[...]
    sig = jax.nn.sigmoid(gate)
    gate_grad = (mid_grad * up * sig * (1.0 + gate * (1.0 - sig))).astype(BF16)
    up_grad = (mid_grad * (gate * sig)).astype(BF16)
    gate_grad_ref[...] = gate_grad
    up_grad_ref[...] = up_grad
    back = matmul_nt(gate_grad, gate_weights_ref[...]) + matmul_nt(up_grad, up_weights_ref[...])
    back = back.astype(BF16)

    rows = back.shape[0]
    half = rows // 2

    @pl.when(step < near_steps)
    def _():
        near_ref[...] = back

    @pl.when(step == near_steps)
    def _():
        far_ref[:rows, :] = back

    @pl.when(step == near_steps + 1)
    def _():
        far_ref[rows:, :] = back[:half]
        corner_ref[...] = back[half:]


def unit_grads(branch, ffn_gate, ffn_up, down_weights, gate_weights, up_weights):
    rows, width = branch.shape
    units = ffn_gate.shape[1]
    tile = rows // 4
    tokens = pl.BlockSpec((tile, width), lambda i: (i, 0))
    hidden = pl.BlockSpec((tile, units), lambda i: (i, 0))
    weight = pl.BlockSpec((width, units), lambda i: (0, 0), pipeline_mode=pl.Buffered(1))
    gate_grad, up_grad, *parts = pl.pallas_call(
        functools.partial(unit_grads_kernel, 2),
        grid=(4,),
        in_specs=[tokens, hidden, hidden, weight, weight, weight],
        out_specs=[
            hidden,
            hidden,
            pl.BlockSpec((tile, width), lambda i: (jnp.minimum(i, 1), 0)),
            pl.BlockSpec((3 * tile // 2, width), lambda i: (0, 0)),
            pl.BlockSpec((tile // 2, width), lambda i: (0, 0)),
        ],
        out_shape=[
            jax.ShapeDtypeStruct((rows, units), BF16),
            jax.ShapeDtypeStruct((rows, units), BF16),
            jax.ShapeDtypeStruct((2 * tile, width), BF16),
            jax.ShapeDtypeStruct((3 * tile // 2, width), BF16),
            jax.ShapeDtypeStruct((tile // 2, width), BF16),
        ],
        compiler_params=pltpu.CompilerParams(vmem_limit_bytes=58 << 20),
        cost_estimate=light_cost(),
        name="unit_grads",
    )(branch, ffn_gate, ffn_up, down_weights, gate_weights, up_weights)
    return gate_grad, up_grad, parts


def head_specs(slots, group, kv_heads, head_size):
    half = slots // 2
    wide = group * head_size

    def piece(width, base):
        return pl.BlockSpec((2, None, half, width), lambda s, c: (0, s, 0, base + c))

    def ordered(width):
        return pl.BlockSpec((None, slots, width), lambda s, c: (s, 0, c))

    raw = [piece(wide, 0), piece(head_size, kv_heads * group)]
    value = piece(head_size, kv_heads * (group + 1))
    gain = pl.BlockSpec((1, head_size), lambda s, c: (0, 0))
    table = pl.BlockSpec((slots, head_size), lambda s, c: (0, 0))
    scalar = pl.BlockSpec(memory_space=pltpu.SMEM)
    return raw, value, ordered(wide), ordered(head_size), gain, table, scalar


def attend_forward(qkv_raw, share, lengths, gains, tables, masks, sizes):
    kv_heads, group, head_size = sizes
    slots = qkv_raw.shape[0] // 2
    raw, value, wide, narrow, gain, table, scalar = head_specs(slots, group, kv_heads, head_size)
    split = qkv_raw.reshape(2, 2, slots // 2, qkv_raw.shape[1])
    width, key_width = kv_heads * group * head_size, kv_heads * head_size
    attended, *kept = pl.pallas_call(
        functools.partial(attend_forward_kernel, masks, head_size, head_size ** (-0.5)),
        grid=(2, kv_heads),
        in_specs=[scalar, scalar, *raw, value, gain, gain, table, table],
        out_specs=[raw[0], wide, wide, narrow, narrow],
        out_shape=[
            jax.ShapeDtypeStruct((2, 2, slots // 2, width), F32),
            jax.ShapeDtypeStruct((2, slots, width), F32),
            jax.ShapeDtypeStruct((2, slots, width), BF16),
            jax.ShapeDtypeStruct((2, slots, key_width), BF16),
            jax.ShapeDtypeStruct((2, slots, key_width), BF16),
        ],
        cost_estimate=light_cost(),
        name="attend_forward",
    )(share, lengths, split, split, split, *gains, *tables)
    return attended.reshape(2 * slots, width), kept


def attend_backward(grads, gate_grads, qkv_raw, kept, share, lengths, gains, tables, masks, sizes):
    kv_heads, group, head_size = sizes
    slots = qkv_raw.shape[0] // 2
    raw, value, wide, narrow, gain, table, scalar = head_specs(slots, group, kv_heads, head_size)
    split = qkv_raw.reshape(2, 2, slots // 2, qkv_raw.shape[1])
    log_total, query_rot, key_rot, value_low = kept
    width = qkv_raw.shape[1] + gate_grads.shape[1]
    sent, gain_parts = pl.pallas_call(
        functools.partial(attend_backward_kernel, masks, head_size, head_size ** (-0.5)),
        grid=(2, kv_heads),
        in_specs=[scalar, scalar, raw[0], raw[0], *raw, wide, narrow, narrow, wide]
        + [gain, gain, table, table],
        out_specs=[
            pl.BlockSpec((2, None, slots // 2, width), lambda s, c: (0, s, 0, 0)),
            pl.BlockSpec((8, head_size), lambda s, c: (0, 0)),
        ],
        out_shape=[
            jax.ShapeDtypeStruct((2, 2, slots // 2, width), BF16),
            jax.ShapeDtypeStruct((8, head_size), F32),
        ],
        scratch_shapes=[
            pltpu.VMEM((slots, group * head_size), F32),
            pltpu.VMEM((slots, head_size), F32),
            pltpu.VMEM((slots, head_size), F32),
        ],
        cost_estimate=light_cost(),
        name="attend_backward",
    )(
        share,
        lengths,
        grads.reshape(2, 2, slots // 2, grads.shape[1]),
        gate_grads.reshape(2, 2, slots // 2, grads.shape[1]),
        split,
        split,
        query_rot,
        key_rot,
        value_low,
        log_total,
        *gains,
        *tables,
    )
    return sent.reshape(2 * slots, width), gain_parts


def body(
    members,
    shares,
    hidden_in,
    lengths,
    attn_gain,
    query_weight,
    key_weight,
    value_weight,
    output_gate,
    query_gain,
    key_gain,
    out_weight,
    mlp_gain,
    gate_weight,
    up_weight,
    down_weight,
    cotangent,
):
    odd = lax.axis_index("fsdp") % 2 == 1
    share = lax.axis_index("tensor")
    local_rows = hidden_in.shape[0]
    head_size = query_gain.shape[0]
    query_width = query_weight.shape[1] // 2
    key_width = key_weight.shape[1] // 2
    sizes = (key_width // head_size, query_width // key_width, head_size)
    masks = row_masks(shares)
    slots = share * local_rows + jnp.arange(local_rows)
    valid_rows = (slots < lengths[0]).astype(F32)[:, None]
    share_at = share.astype(jnp.int32)[None]
    both_lengths = jnp.concatenate([lengths, to_partner(lengths, members)])
    gains = (query_gain[None, :], key_gain[None, :])
    half_rows = local_rows * shares

    def gather_rows(values, *before):
        return rows_in(values, members, shares, *before)

    def sum_rows(parts, first, last):
        added = open_sum(parts, members, shares, *first)
        return close_sum(*send_sum(added, members, shares), members, shares, *last)

    def in_parts(function):
        corner = function(slice(2 * half_rows - local_rows, 2 * half_rows)).astype(BF16)
        far = function(slice(half_rows, 2 * half_rows - local_rows)).astype(BF16)
        near = function(slice(0, half_rows)).astype(BF16)
        return near, far, corner

    qkv_rows = pair_rows([query_weight, key_weight, value_weight], odd, members)
    qkv_full = gather_line(qkv_rows, members)
    gate_out_rows = pair_rows([output_gate, out_weight.T], odd, members)
    gate_out_full = gather_line(hold(gate_out_rows, qkv_rows), members)

    residual = hidden_in.astype(F32)
    unit_one, root_one = normalize(residual)
    gate_rows = pair_rows([hold(gate_weight, gate_out_rows)], odd, members)
    normed_one = gather_rows(hold((unit_one * attn_gain).astype(BF16), gate_rows))
    qkv_raw = matmul(normed_one, qkv_full)
    grad_rows = cotangent.astype(F32) * valid_rows
    tables = rope_tables(half_rows, head_size)
    attended, kept = attend_forward(
        qkv_raw, share_at, both_lengths, gains, tables, masks, sizes
    )
    up_in, down_in = hold((up_weight, down_weight), normed_one)
    up_rows = pair_rows([up_in], odd, members, attended)
    down_rows = pair_rows([down_in.T], odd, members, attended)
    gate_weights = gather_line(hold(gate_rows, qkv_full), members)
    up_weights = gather_line(hold(up_rows, gate_out_full), members)
    down_weights = gather_line(hold(down_rows, gate_weights), members)
    gate_full, out_full = gate_out_full[:, :query_width], gate_out_full[:, query_width:]
    gate_pre = matmul(hold(normed_one, attended, up_rows, down_rows), gate_full)
    gate_sig = jax.nn.sigmoid(gate_pre)
    gated_out = (attended * gate_sig).astype(BF16)
    attn_parts = in_parts(lambda rows: matmul_nt(gated_out[rows], out_full))
    middle = residual + sum_rows(attn_parts, (), (gate_weights,))
    unit_two, root_two = normalize(middle)
    normed_two = gather_rows((unit_two * mlp_gain).astype(BF16))
    one_weights = jnp.concatenate([qkv_full, gate_full], axis=1)
    ffn_gate, ffn_up, ffn_mid = hidden_units(normed_two, gate_weights, up_weights)
    branch_full = gather_rows(
        hold(grad_rows.astype(BF16), normed_two), None, one_weights, ffn_mid
    )

    down_part = matmul_tn(branch_full, ffn_mid).astype(BF16)
    down_sum = scatter_line(down_part, members)

    gate_grad, up_grad, back_parts = unit_grads(
        branch_full, ffn_gate, ffn_up, hold(down_weights, down_part), gate_weights, up_weights
    )
    gate_part = matmul_tn(normed_two, hold(gate_grad, back_parts)).astype(BF16)
    gate_sum = scatter_line(gate_part, members)
    up_part = matmul_tn(normed_two, hold(up_grad, gate_part)).astype(BF16)
    up_sum = scatter_line(up_part, members)
    norm_two_grad = sum_rows(back_parts, (gate_part,), (down_sum, up_part))

    mlp_gain_part = jnp.sum(norm_two_grad * unit_two, axis=0)
    middle_grad = grad_rows + norm_back(norm_two_grad, unit_two, root_two, mlp_gain)
    mid_late = hold(ffn_mid, norm_two_grad)
    branch_parts = in_parts(lambda rows: matmul_nt(mid_late[rows], down_weights))
    attn_full_grad = gather_rows(middle_grad.astype(BF16), None, branch_parts, gate_sum)
    branch_added = open_sum(branch_parts, members, shares)
    down_swap = swap_rows(hold(down_sum, attn_full_grad), odd, members)
    gate_swap = swap_rows(hold(gate_sum, attn_full_grad), odd, members)
    attn_full_grad = hold(attn_full_grad, branch_added)
    corners, opened = send_sum(hold(branch_added, attn_full_grad), members, shares)
    gated_grad = matmul(attn_full_grad, out_full)
    attended_grad = (gated_grad * gate_sig).astype(BF16)
    gate_pre_grad = (gated_grad * attended * gate_sig * (1.0 - gate_sig)).astype(BF16)
    gate_attn_part = matmul_tn(normed_one, gate_pre_grad).astype(BF16)
    gate_out_part = jnp.concatenate(
        [
            gate_attn_part,
            matmul_tn(attn_full_grad, gated_out).astype(BF16),
        ],
        axis=1,
    )
    gate_out_sum = scatter_line(gate_out_part, members)
    one_send, gain_parts = attend_backward(
        hold(attended_grad, gate_out_part),
        gate_pre_grad,
        qkv_raw,
        kept,
        share_at,
        both_lengths,
        gains,
        tables,
        masks,
        sizes,
    )
    one_send = hold(one_send, corners, opened, down_swap, gate_swap)
    ffn_branch = close_sum(corners, opened, members, shares, one_send)
    output = ((middle + ffn_branch) * valid_rows).astype(BF16)
    units = up_sum.shape[1]
    one_parts = in_parts(lambda rows: matmul_nt(one_send[rows], one_weights))
    qkv_send = hold(one_send, up_sum, one_parts)[:, : qkv_raw.shape[1]]
    qkv_part = matmul_tn(normed_one, qkv_send).astype(BF16)
    qkv_sum = scatter_line(qkv_part, members)
    attn_gain_part = (
        dot_rows(qkv_part, qkv_full) + dot_rows(gate_attn_part, gate_full)
    ) / attn_gain
    up_swap = swap_rows(hold(up_sum, one_send), odd, members)
    added_one = open_sum(one_parts, members, shares, qkv_part)
    gain_parts = hold(
        jnp.concatenate([attn_gain_part, mlp_gain_part, gain_parts[0], gain_parts[1]]), added_one
    )
    gain_parts = sum_everywhere(gain_parts, "fsdp", 2, members)
    gain_parts = sum_everywhere(gain_parts, "tensor", 1, 2)
    norm_one_grad = close_sum(
        *send_sum(added_one, members, shares), members, shares, gate_out_sum, gain_parts, up_swap, output
    )
    gain_totals = hold(gain_parts, norm_one_grad)
    gain_totals = sum_everywhere(gain_totals, "tensor", 2, shares)
    gain_totals = sum_everywhere(gain_totals, "fsdp", 1, 2)
    grad_hidden = middle_grad + norm_back(norm_one_grad, unit_one, root_one, attn_gain)
    (down_shard,) = own_shard(*down_swap, odd, (units,))
    (gate_shard,) = own_shard(*gate_swap, odd, (units,))
    gate_out_swap = swap_rows(hold(gate_out_sum, norm_one_grad, qkv_sum), odd, members)
    (up_shard,) = own_shard(*up_swap, odd, (units,))
    gate_attn_shard, out_shard = own_shard(*gate_out_swap, odd, (query_width,) * 2)
    qkv_sum = hold(qkv_sum, norm_one_grad)
    query_shard, key_shard, value_shard = own_shard(
        *swap_rows(qkv_sum, odd, members), odd, (query_width, key_width, key_width)
    )
    width = hidden_in.shape[1]
    return (
        output,
        grad_hidden,
        gain_totals[:width],
        query_shard,
        key_shard,
        value_shard,
        gate_attn_shard,
        gain_totals[2 * width : 2 * width + head_size],
        gain_totals[2 * width + head_size :],
        out_shard.T,
        gain_totals[width : 2 * width],
        gate_shard,
        up_shard,
        down_shard.T,
    )


def solution(mesh):
    members, shares = mesh.shape["fsdp"], mesh.shape["tensor"]

    def layer(*operands):
        return body(members, shares, *operands)

    tokens = P(("fsdp", "tensor"), None)
    return jax.shard_map(
        layer,
        mesh=mesh,
        in_specs=(
            tokens,
            P("fsdp"),
            P(),
            P("fsdp", "tensor"),
            P("fsdp", "tensor"),
            P("fsdp", "tensor"),
            P("fsdp", "tensor"),
            P(),
            P(),
            P("tensor", "fsdp"),
            P(),
            P("fsdp", "tensor"),
            P("fsdp", "tensor"),
            P("tensor", "fsdp"),
            tokens,
        ),
        out_specs=(
            tokens,
            tokens,
            P(),
            P("fsdp", "tensor"),
            P("fsdp", "tensor"),
            P("fsdp", "tensor"),
            P("fsdp", "tensor"),
            P(),
            P(),
            P("tensor", "fsdp"),
            P(),
            P("fsdp", "tensor"),
            P("fsdp", "tensor"),
            P("tensor", "fsdp"),
        ),
        check_vma=False,
    )
```
